128 devices in a mesh: dp: 1, ing: 2 (over core), grp: 64 (over z, y, x).
Axes of the slice: x: 4, y: 4, z: 4, core: 2. Of those that a mesh axis runs over, the one named last changes fastest.
Arguments:
- x_first: bfloat16 [16384, 2048], P(('dp', 'grp', 'ing'))
- ids_first: int32 [16384, 8], P(('dp', 'grp', 'ing'))
- gates_first: float32 [16384, 8], P(('dp', 'grp', 'ing'))
- x_second: bfloat16 [16384, 2048], P(('dp', 'grp', 'ing'))
- ids_second: int32 [16384, 8], P(('dp', 'grp', 'ing'))
- gates_second: float32 [16384, 8], P(('dp', 'grp', 'ing'))
- w_one: bfloat16 [128, 2048, 768], P(('grp', 'ing'))
- w_three: bfloat16 [128, 2048, 768], P(('grp', 'ing'))
- w_two: bfloat16 [128, 768, 2048], P(('grp', 'ing'))
Outputs:
- output 1: bfloat16 [16384, 2048], P(('dp', 'grp', 'ing'))
- output 2: bfloat16 [16384, 2048], P(('dp', 'grp', 'ing'))
All inputs are finite; a program needn't handle non-finite values.
Results may differ from the reference program's by a relative error of at most 0.0108876.
Values are sent between devices in bfloat16 or wider.
A program may use at most 1 GiB of HBM per device.

```python
import jax
import jax.numpy as jnp
from jax import lax

HIDDEN = 2048
EXPERT_FF = 768
EXPERTS = 128
TOP_K = 8
GROUPS = 64
INNER_DEV = 2
TOKENS = 128

SOURCES = GROUPS * INNER_DEV
ROWS_ALL = SOURCES * TOKENS
PER_GROUP = EXPERTS // GROUPS
LIMIT_M = min(TOP_K, GROUPS // 2)
PER_SLOT = TOP_K // LIMIT_M
GROUP_STEP = GROUPS // LIMIT_M
CAP_EXPERT = LIMIT_M * ((TOKENS * PER_SLOT + EXPERTS - 1) // EXPERTS)
EXPERT_ROWS = SOURCES * CAP_EXPERT


def route_source(tok_perm, grp_perm, loc_perm, offset):
    position = tok_perm[:, None, None]
    slot_q = jnp.arange(LIMIT_M)[None, :, None]
    slot_u = jnp.arange(PER_SLOT)[None, None, :]
    grp_id = grp_perm[(position + slot_q * GROUP_STEP) % GROUPS]
    residue = ((position // GROUPS) * PER_SLOT + slot_u + offset) % PER_GROUP
    local_id = loc_perm[grp_id, residue]
    return (grp_id * PER_GROUP + local_id).reshape(TOKENS, TOP_K)


def draw_routing(key_in):
    key_tok, key_grp, key_loc, key_off = jax.random.split(key_in, 4)
    tok_perm = jax.vmap(lambda sub_key: jax.random.permutation(sub_key, TOKENS))(jax.random.split(key_tok, SOURCES))
    grp_perm = jax.vmap(lambda sub_key: jax.random.permutation(sub_key, GROUPS))(jax.random.split(key_grp, SOURCES))
    loc_keys = jax.random.split(key_loc, SOURCES * GROUPS)
    loc_perm = jax.vmap(lambda sub_key: jax.random.permutation(sub_key, PER_GROUP))(loc_keys).reshape(SOURCES, GROUPS, PER_GROUP)
    offset = jax.random.randint(key_off, (SOURCES,), 0, PER_GROUP)
    expert_ids = jax.vmap(route_source)(tok_perm, grp_perm, loc_perm, offset)
    return expert_ids.reshape(ROWS_ALL, TOP_K).astype(jnp.int32)


def draw_gates(key_in):
    return jax.random.uniform(key_in, (ROWS_ALL, TOP_K), jnp.float32, 0.2, 1.8) / TOP_K


def draw_weights(key_in, fan_in, fan_out):
    expert_keys = jax.random.split(key_in, EXPERTS)
    scale_in = fan_in ** -0.5
    return lax.map(lambda sub_key: (jax.random.normal(sub_key, (fan_in, fan_out), jnp.float32) * scale_in).astype(jnp.bfloat16), expert_keys)


def setup_inputs(seed: int = 0, part: int = 0) -> dict:
    root_key = jax.random.key(seed)
    key_data, key_weight = jax.random.split(root_key)
    key_part = jax.random.fold_in(key_data, part)
    data_keys = jax.random.split(key_part, 6)
    weight_keys = jax.random.split(key_weight, 3)
    return {
        'x_first': jax.random.normal(data_keys[0], (ROWS_ALL, HIDDEN), jnp.float32).astype(jnp.bfloat16),
        'ids_first': draw_routing(data_keys[1]),
        'gates_first': draw_gates(data_keys[2]),
        'x_second': jax.random.normal(data_keys[3], (ROWS_ALL, HIDDEN), jnp.float32).astype(jnp.bfloat16),
        'ids_second': draw_routing(data_keys[4]),
        'gates_second': draw_gates(data_keys[5]),
        'w_one': draw_weights(weight_keys[0], HIDDEN, EXPERT_FF),
        'w_three': draw_weights(weight_keys[1], HIDDEN, EXPERT_FF),
        'w_two': draw_weights(weight_keys[2], EXPERT_FF, HIDDEN),
    }


def moe_layer(tokens_in, expert_ids, gate_vals, w_one, w_three, w_two):
    w_stack = (w_one.reshape(GROUPS, PER_GROUP, HIDDEN, EXPERT_FF),
               w_three.reshape(GROUPS, PER_GROUP, HIDDEN, EXPERT_FF),
               w_two.reshape(GROUPS, PER_GROUP, EXPERT_FF, HIDDEN))
    row_range = jnp.arange(EXPERT_ROWS)

    def expert_step(acc_sum, expert_in):
        e_one, e_three, e_two, expert = expert_in
        expert_hit = expert_ids == expert
        member = jnp.any(expert_hit, axis=1)
        gate_col = jnp.sum(jnp.where(expert_hit, gate_vals, 0.0), axis=1)
        row_count = jnp.sum(member.astype(jnp.int32))
        row_ids = jnp.nonzero(member, size=EXPERT_ROWS, fill_value=0)[0]
        row_gate = jnp.where(row_range < row_count, gate_col[row_ids], 0.0)
        picked = tokens_in[row_ids]
        act_a = jnp.dot(picked, e_one, preferred_element_type=jnp.float32)
        act_b = jnp.dot(picked, e_three, preferred_element_type=jnp.float32)
        hidden_act = (jax.nn.silu(act_a) * act_b).astype(jnp.bfloat16)
        expert_out = jnp.dot(hidden_act, e_two, preferred_element_type=jnp.float32)
        scaled = (expert_out * row_gate[:, None]).astype(jnp.bfloat16)
        return acc_sum.at[row_ids].add(scaled.astype(jnp.float32)), None

    def group_step(y_acc, group_in):
        g_one, g_three, g_two, group_id = group_in
        expert_list = group_id * PER_GROUP + jnp.arange(PER_GROUP)
        zero_acc = jnp.zeros((ROWS_ALL, HIDDEN), jnp.float32)
        group_acc, _ = lax.scan(expert_step, zero_acc, (g_one, g_three, g_two, expert_list))
        return y_acc + group_acc.astype(jnp.bfloat16).astype(jnp.float32), None

    y_init = jnp.zeros((ROWS_ALL, HIDDEN), jnp.float32)
    y_acc, _ = lax.scan(group_step, y_init, w_stack + (jnp.arange(GROUPS),))
    return y_acc.astype(jnp.bfloat16)


def reference(x_first, ids_first, gates_first, x_second, ids_second, gates_second, w_one, w_three, w_two):
    y_first = moe_layer(x_first, ids_first, gates_first, w_one, w_three, w_two)
    y_second = moe_layer(x_second, ids_second, gates_second, w_one, w_three, w_two)
    return (y_first, y_second)
```

```python
import functools

import jax
import jax.numpy as jnp
from jax import lax
from jax.experimental import pallas as pl
from jax.experimental.pallas import tpu as pltpu
from jax.sharding import PartitionSpec as P

MESH = pl.DeviceIdType.MESH
CAP = 8
PAIR = 16
CHUNKS = 8


def moe_kernel(side, x1, x2, ids1, ids2, gt1, gt2, w1_hbm, w3_hbm, w2_hbm, y1, y2,
               xs, xr, zs, zr, gs, gr, w1, w3, w2, xall, val, yacc,
               wsem, sx, rx, sg, rg, sz, rz):
    tokens, hidden = x1.shape
    slots = xs.shape[0] // PAIR
    per = slots // CHUNKS
    rows = per * PAIR
    me_grp = lax.axis_index('grp')
    me_ing = lax.axis_index('ing')
    me = (me_grp // (side * side), (me_grp // side) % side, me_grp % side)

    def place(k, sign):
        j = k // 2
        a = j % side
        t = j // side
        p = t % side
        q = t // side
        dx = a
        dy = (a + p) % side
        dz = (a + q) % side
        if sign < 0:
            dx, dy, dz = side - dx, side - dy, side - dz
        nz = (me[0] + dz) % side
        ny = (me[1] + dy) % side
        nx = (me[2] + dx) % side
        return (nz * side + ny) * side + nx, (me_ing + k % 2) % 2

    copies = [pltpu.make_async_copy(src, dst, wsem.at[n])
              for n, (src, dst) in enumerate(((w1_hbm.at[0], w1), (w3_hbm.at[0], w3), (w2_hbm.at[0], w2)))]
    for copy in copies:
        copy.start()

    slot_lane = lax.broadcasted_iota(jnp.int32, (1, slots), 1)
    peer_grp, peer_ing = place(slot_lane, 1)
    peer_expert = peer_grp * 2 + peer_ing
    tri = (lax.broadcasted_iota(jnp.int32, (tokens, tokens), 0)
           > lax.broadcasted_iota(jnp.int32, (tokens, tokens), 1)).astype(jnp.float32).astype(jnp.bfloat16)
    gate_rows = []
    for b, (ids, gates) in enumerate(((ids1, gt1), (ids2, gt2))):
        ids_v = ids[...]
        gates_v = gates[...]
        member = jnp.zeros((tokens, slots), jnp.float32)
        gate = jnp.zeros((tokens, slots), jnp.float32)
        for j in range(ids_v.shape[1]):
            hit = ids_v[:, j:j + 1] == peer_expert
            member = jnp.where(hit, 1.0, member)
            gate = jnp.where(hit, gates_v[:, j:j + 1], gate)
        before = jnp.dot(tri, member.astype(jnp.bfloat16), preferred_element_type=jnp.float32)
        place_v = jnp.where(member > 0.0, before + 1.0, 0.0)
        val[b * tokens:(b + 1) * tokens, :] = place_v.astype(jnp.bfloat16)
        for s in range(CAP):
            gate_rows.append(jnp.sum(jnp.where(place_v == s + 1.0, gate, 0.0), axis=0, keepdims=True))
    xall[0:tokens, :] = x1[...]
    xall[tokens:2 * tokens, :] = x2[...]
    if slots > PAIR:
        gate_rows.append(jnp.zeros((slots - PAIR, slots), jnp.float32))
    gate_send = jnp.concatenate(gate_rows, axis=0).T
    gs[...] = gate_send[:, None, :]

    def select(c):
        r = lax.broadcasted_iota(jnp.int32, (rows, slots), 0)
        k = lax.broadcasted_iota(jnp.int32, (rows, slots), 1)
        expand = (r // PAIR + c * per == k).astype(jnp.float32).astype(jnp.bfloat16)
        v = lax.dot_general(expand, val[...], (((1,), (1,)), ((), ())), preferred_element_type=jnp.float32)
        r = lax.broadcasted_iota(jnp.int32, v.shape, 0)
        u = lax.broadcasted_iota(jnp.int32, v.shape, 1)
        hit = (v == (r % CAP + 1).astype(jnp.float32)) & ((r // CAP) % 2 == u // tokens)
        return hit.astype(jnp.float32).astype(jnp.bfloat16)

    def select_t(c):
        k = lax.broadcasted_iota(jnp.int32, (slots, rows), 0)
        r = lax.broadcasted_iota(jnp.int32, (slots, rows), 1)
        expand = (r // PAIR + c * per == k).astype(jnp.float32).astype(jnp.bfloat16)
        v = jnp.dot(val[...], expand, preferred_element_type=jnp.float32)
        u = lax.broadcasted_iota(jnp.int32, v.shape, 0)
        r = lax.broadcasted_iota(jnp.int32, v.shape, 1)
        hit = (v == (r % CAP + 1).astype(jnp.float32)) & ((r // CAP) % 2 == u // tokens)
        return hit.astype(jnp.float32).astype(jnp.bfloat16)

    def chunk_rows(c):
        return pl.ds(pl.multiple_of(c * rows, rows), rows)

    def pair_rows(k):
        return pl.ds(pl.multiple_of(k * PAIR, PAIR), PAIR)

    def remote(src, dst, send, recv, dev):
        return pltpu.make_async_remote_copy(src_ref=src, dst_ref=dst, send_sem=send, recv_sem=recv,
                                            device_id={'grp': dev[0], 'ing': dev[1]}, device_id_type=MESH)

    def all_of(src, dst, send, recv, c, size):
        def whole(part):
            return remote(src.at[part], dst.at[part], send.at[c], recv.at[c], (me_grp, me_ing))

        return whole(pl.ds(size, (per - 1) * size)), whole(pl.ds(pl.multiple_of(c * per * size, size), per * size))

    def wait_recv(src, dst, send, recv, c, size):
        first, other = all_of(src, dst, send, recv, c, size)
        pl.when(c == 0)(lambda: first.wait_recv())
        pl.when(c != 0)(lambda: other.wait_recv())

    def wait_send(src, dst, send, recv, c, size):
        first, other = all_of(src, dst, send, recv, c, size)
        pl.when(c == 0)(lambda: first.wait_send())
        pl.when(c != 0)(lambda: other.wait_send())

    all_x = (xs, xr, sx, rx)
    all_g = (gs, gr, sg, rg)
    all_z = (zs, zr, sz, rz)

    def first_slot(c):
        return jnp.where(c == 0, 1, 0)

    def dispatch(c, carry):
        picked = jnp.dot(select(c), xall[...], preferred_element_type=jnp.float32)
        xs[chunk_rows(c), :] = picked.astype(jnp.bfloat16)

        @pl.when(c == 0)
        def _():
            xr[0:PAIR, :] = picked[0:PAIR].astype(jnp.bfloat16)
            gr[0:1] = gs[0:1]

        def send(i, carry):
            k = c * per + i
            dev = place(k, 1)
            remote(xs.at[pair_rows(k)], xr.at[pair_rows(k)], sx.at[c], rx.at[c], dev).start()
            remote(gs.at[pl.ds(k, 1)], gr.at[pl.ds(k, 1)], sg.at[c], rg.at[c], dev).start()
            return carry

        return lax.fori_loop(first_slot(c), per, send, carry)

    lax.fori_loop(0, CHUNKS, dispatch, 0)
    yacc[...] = jnp.zeros_like(yacc)
    for copy in copies:
        copy.wait()

    def expert(c, carry):
        wait_recv(*all_x, c, PAIR)
        wait_recv(*all_g, c, 1)
        part = chunk_rows(c)
        rec = xr[part, :]
        act_a = jnp.dot(rec, w1[...], preferred_element_type=jnp.float32)
        act_b = jnp.dot(rec, w3[...], preferred_element_type=jnp.float32)
        mid = (act_a * jax.nn.sigmoid(act_a) * act_b).astype(jnp.bfloat16)
        g = gr[pl.ds(c * per, per)]
        g = jnp.broadcast_to(g, (per, PAIR, slots)).reshape(rows, slots)
        lane = lax.broadcasted_iota(jnp.int32, g.shape, 1)
        row = lax.broadcasted_iota(jnp.int32, g.shape, 0)
        g = jnp.sum(jnp.where(lane == row % PAIR, g, 0.0), axis=1, keepdims=True)
        out = jnp.dot(mid, w2[...], preferred_element_type=jnp.float32)
        scaled = (out * g).astype(jnp.bfloat16)
        zs[part, :] = scaled

        @pl.when(c == 0)
        def _():
            zr[0:PAIR, :] = scaled[0:PAIR]

        def send(i, carry):
            k = c * per + i
            dev = place(k, -1)
            remote(zs.at[pair_rows(k)], zr.at[pair_rows(k)], sz.at[c], rz.at[c], dev).start()
            return carry

        return lax.fori_loop(first_slot(c), per, send, carry)

    lax.fori_loop(0, CHUNKS, expert, 0)

    def combine(c, carry):
        sel = select(c)
        sel_t = select_t(c)
        same = jnp.dot(sel, sel_t, preferred_element_type=jnp.float32)
        i = lax.broadcasted_iota(jnp.int32, same.shape, 0)
        j = lax.broadcasted_iota(jnp.int32, same.shape, 1)
        same = jnp.where(i // (2 * PAIR) == j // (2 * PAIR), same, 0.0)
        earlier = jnp.sum(jnp.where(j < i, same, 0.0), axis=1, keepdims=True)
        fold = jnp.where(earlier > 0.0, 0.0, same).astype(jnp.bfloat16)
        wait_recv(*all_z, c, PAIR)
        part = jnp.dot(fold, zr[chunk_rows(c), :], preferred_element_type=jnp.float32).astype(jnp.bfloat16)
        yacc[...] += jnp.dot(sel_t, part, preferred_element_type=jnp.float32)
        return carry

    lax.fori_loop(0, CHUNKS, combine, 0)
    y1[...] = yacc[0:tokens, :].astype(jnp.bfloat16)
    y2[...] = yacc[tokens:2 * tokens, :].astype(jnp.bfloat16)

    def drain(c, carry):
        wait_send(*all_x, c, PAIR)
        wait_send(*all_g, c, 1)
        wait_send(*all_z, c, PAIR)
        return carry

    lax.fori_loop(0, CHUNKS, drain, 0)


def solution(mesh):
    n_grp = mesh.shape['grp']
    n_ing = mesh.shape['ing']
    slots = n_grp * n_ing
    side = round(n_grp ** (1 / 3))
    tok_spec = P(('dp', 'grp', 'ing'), None)
    w_spec = P(('grp', 'ing'), None, None)

    def body(x1, ids1, g1, x2, ids2, g2, w1, w3, w2):
        tokens, hidden = x1.shape
        ff = w1.shape[2]
        vmem = pl.BlockSpec(memory_space=pltpu.VMEM)
        hbm = pl.BlockSpec(memory_space=pl.ANY)
        big = pltpu.VMEM((slots * PAIR, hidden), jnp.bfloat16)
        gate = pltpu.VMEM((slots, 1, slots), jnp.float32)
        sem = pltpu.SemaphoreType.DMA((CHUNKS,))
        out = jax.ShapeDtypeStruct((tokens, hidden), jnp.bfloat16)
        return pl.pallas_call(
            functools.partial(moe_kernel, side),
            out_shape=(out, out),
            in_specs=[vmem] * 6 + [hbm] * 3,
            out_specs=(vmem, vmem),
            scratch_shapes=[big, big, big, big, gate, gate,
                            pltpu.VMEM((hidden, ff), jnp.bfloat16),
                            pltpu.VMEM((hidden, ff), jnp.bfloat16),
                            pltpu.VMEM((ff, hidden), jnp.bfloat16),
                            pltpu.VMEM((2 * tokens, hidden), jnp.bfloat16),
                            pltpu.VMEM((2 * tokens, slots), jnp.bfloat16),
                            pltpu.VMEM((2 * tokens, hidden), jnp.float32),
                            pltpu.SemaphoreType.DMA((3,)), sem, sem, sem, sem, sem, sem],
            compiler_params=pltpu.CompilerParams(has_side_effects=True, vmem_limit_bytes=66_000_000),
        )(x1, x2, ids1, ids2, g1, g2, w1, w3, w2)

    return jax.shard_map(body, mesh=mesh, in_specs=(tok_spec,) * 6 + (w_spec,) * 3,
                         out_specs=(tok_spec, tok_spec), check_vma=False)
```

```python
import functools

import jax
import jax.numpy as jnp
from jax import lax
from jax.experimental import pallas as pl
from jax.experimental.pallas import tpu as pltpu
from jax.sharding import PartitionSpec as P

MESH = pl.DeviceIdType.MESH
CAP = 8
LANES = 128


def lane_parts(hidden):
    tiles = hidden // LANES
    sizes = [(tiles // 3 + (1 if d < tiles % 3 else 0)) * LANES for d in range(3)]
    return [(sum(sizes[:d]), sizes[d]) for d in range(3)]


def moe_kernel(side, x1, x2, ids1, ids2, gt1, gt2, w1_hbm, w3_hbm, w2_hbm, y1, y2,
               ag, p2s, p2r, r2, zr, vt, vr, selt, fold, xr, gs, gr, w1, w3, w2, yacc,
               wsem, gsem, sems):
    xs, ys = (x1, x2), (y1, y2)
    tokens, hidden = x1.shape
    n = side ** 3 * 2
    plane = n // side
    rows = plane * CAP
    parts = lane_parts(hidden)
    grp = lax.axis_index('grp')
    ing = lax.axis_index('ing')
    me = (grp % side, (grp // side) % side, grp // (side * side))
    order = [(d, (d + 1) % 3, (d + 2) % 3) for d in range(3)]
    f32, bf16 = jnp.float32, jnp.bfloat16

    def at(off, core=0):
        x, y, z = ((m + o) % side for m, o in zip(me, off))
        return (z * side + y) * side + x, (ing + core) % 2

    def along(dim, step, core=0):
        off = [0, 0, 0]
        off[dim] = step % side
        return at(off, core)

    def remote(src, dst, send, recv, dev):
        return pltpu.make_async_remote_copy(src_ref=src, dst_ref=dst, send_sem=send, recv_sem=recv,
                                            device_id={'grp': dev[0], 'ing': dev[1]}, device_id_type=MESH)

    def iota(shape, dim):
        return lax.broadcasted_iota(jnp.int32, shape, dim)

    def split(q):
        return q // (side * side * 2), (q // (side * 2)) % side, (q // 2) % side, q % 2

    barrier = pltpu.get_barrier_semaphore()

    def knock(q, carry):
        ox, oy, oz, oc = split(q)
        dev = at((ox, oy, oz), oc)
        pl.semaphore_signal(barrier, inc=1, device_id={'grp': dev[0], 'ing': dev[1]}, device_id_type=MESH)
        return carry

    lax.fori_loop(1, n, knock, 0)
    weights = [pltpu.make_async_copy(src, dst, wsem.at[k])
               for k, (src, dst) in enumerate(((w1_hbm.at[0], w1), (w3_hbm.at[0], w3), (w2_hbm.at[0], w2)))]
    for copy in weights:
        copy.start()

    later = (iota((tokens, tokens), 0) < iota((tokens, tokens), 1)).astype(f32).astype(bf16)
    expert = iota((n, tokens), 0)
    gate_rows = jnp.zeros((n, LANES), f32)
    lane = iota((n, LANES), 1)
    for b, (ids, gates) in enumerate(((ids1, gt1), (ids2, gt2))):
        member = jnp.zeros((n, tokens), f32)
        gate = jnp.zeros((n, tokens), f32)
        for j in range(ids.shape[0]):
            hit = ids[j:j + 1, :] == expert
            member = jnp.where(hit, 1.0, member)
            gate = jnp.where(hit, gates[j:j + 1, :], gate)
        before = jnp.dot(member.astype(bf16), later, preferred_element_type=f32)
        table = jnp.where(member > 0.0, before + 1.0, 0.0)
        for d, (f, s, t) in enumerate(order):
            q = split(iota((n, n), 0))
            off = [None] * 3
            off[f], off[s], off[t] = q[0], q[1], q[2]
            to_grp, to_ing = at(off, q[3])
            perm = (to_grp * 2 + to_ing == iota((n, n), 1)).astype(f32).astype(bf16)
            vt[d][b] = jnp.dot(perm, table.astype(bf16), preferred_element_type=f32).astype(bf16)
            vr[d][b, 0] = vt[d][b, 0:plane, :]
        for k in range(CAP):
            col = jnp.sum(jnp.where(table == k + 1.0, gate, 0.0), axis=1, keepdims=True)
            gate_rows = jnp.where(lane == b * CAP + k, col, gate_rows)
    gs[...] = gate_rows[:, None, :]
    for b in range(2):
        for d, (lo, width) in enumerate(parts):
            ag[d][b, 0] = xs[b][:, lo:lo + width]

    def sem(phase, b, d, k):
        return sems[phase].at[0, b, d, k], sems[phase].at[1, b, d, k]

    def gather(b):
        out = []
        for i in range(1, side):
            for d, (f, s, t) in enumerate(order):
                lo, width = parts[d]
                dev = along(f, i)
                out.append(remote(vt[d].at[b, pl.ds(i * plane, plane)], vr[d].at[b, i], *sem(0, b, d, i), dev))
                out.append(remote(xs[b].at[:, pl.ds(lo, width)], ag[d].at[b, i], *sem(1, b, d, i), dev))
        return out

    def mid(d, b, j):
        f, s, t = order[d]
        return (b, slice(None), slice(None), slice(None), j) if f < s else (b, slice(None), slice(None), j)

    def second(b, steps):
        return [remote(p2s[d].at[b, j - 1], p2r[d].at[mid(d, b, j)], *sem(2, b, d, j), along(order[d][1], j))
                for j in steps for d in range(3)]

    def final(d, b, k, core):
        lo, width = parts[d]
        index = [slice(None)] * 3
        index[order[d][2]] = k
        return (b, *index, core, slice(None), pl.ds(lo, width))

    def third(b):
        return [remote(p2r[d].at[b, k, c], xr.at[final(d, b, k, c)], *sem(3, b, d, 2 * k + c), along(order[d][2], k, c))
                for k in range(side) for c in range(2) if k + c for d in range(3)]

    def back_third(b):
        return [remote(xr.at[final(d, b, k, c)], p2r[d].at[b, k, c], *sem(4, b, d, 2 * k + c),
                       along(order[d][2], -k, c))
                for k in range(side) for c in range(2) if k + c for d in range(3)]

    def back_second(b):
        return [remote(p2r[d].at[mid(d, b, j)], r2[d].at[b, j], *sem(5, b, d, j), along(order[d][1], -j))
                for j in range(1, side) for d in range(3)]

    def back_first(b, steps):
        return [remote(r2[d].at[b, :, :, :, i], zr[d].at[b, i], *sem(6, b, d, i), along(order[d][0], -i))
                for i in steps for d in range(3)]

    def start(copies):
        for copy in copies:
            copy.start()

    def arrived(copies):
        for copy in copies:
            copy.wait_recv()

    def left(copies):
        for copy in copies:
            copy.wait_send()

    def gate_copy(q):
        ox, oy, oz, oc = split(q)
        dev = at((ox, oy, oz), oc)
        return remote(gs.at[pl.ds(dev[0] * 2 + dev[1], 1)], gr.at[pl.ds(q, 1)], gsem.at[0], gsem.at[1], dev)

    def send_gate(q, carry):
        gate_copy(q).start()
        return carry

    gates_all = remote(gs.at[pl.ds(1, n - 1)], gr.at[pl.ds(1, n - 1)], gsem.at[0], gsem.at[1], (grp, ing))

    def expand():
        return (iota((rows, plane), 0) // CAP == iota((rows, plane), 1)).astype(f32).astype(bf16)

    def chosen(table):
        v = jnp.dot(expand(), table, preferred_element_type=f32)
        return jnp.where(v == (iota(v.shape, 0) % CAP + 1).astype(f32), 1.0, 0.0)

    def select(b):
        for d, (f, s, t) in enumerate(order):
            width = parts[d][1]

            def pick(i, carry, d=d, f=f, s=s, width=width):
                sel = chosen(vr[d][b, i]).astype(bf16)
                out = jnp.dot(sel, ag[d][b, i], preferred_element_type=f32)
                out = out.reshape(side, side, 2, CAP, width).astype(bf16)
                if f < s:
                    p2r[d][b, :, :, i, 0] = out[0]
                else:
                    p2r[d][b, :, :, 0, i] = out[0]
                for j in range(1, side):
                    p2s[d][b, j - 1, :, :, i] = out[j]
                return carry

            lax.fori_loop(0, side, pick, 0)

    def ffn(b, first, last):
        def chunk(ox, carry):
            rec = xr[b, ox].astype(f32).reshape(rows, hidden).astype(bf16)
            act_a = jnp.dot(rec, w1[...], preferred_element_type=f32)
            act_b = jnp.dot(rec, w3[...], preferred_element_type=f32)
            inner = (act_a * jax.nn.sigmoid(act_a) * act_b).astype(bf16)
            g = gr[pl.ds(ox * plane, plane)]
            g = jnp.broadcast_to(g, (plane, CAP, LANES)).reshape(rows, LANES)
            mine = iota(g.shape, 1) == b * CAP + iota(g.shape, 0) % CAP
            g = jnp.sum(jnp.where(mine, g, 0.0), axis=1, keepdims=True)
            out = jnp.dot(inner, w2[...], preferred_element_type=f32) * g
            xr[b, ox] = out.reshape(side, side, 2, CAP, hidden).astype(bf16)
            return carry

        lax.fori_loop(first, last, chunk, 0)

    def tables(b):
        for d in range(3):
            def one(i, carry, d=d):
                sel = chosen(vt[d][b, pl.ds(pl.multiple_of(i * plane, plane), plane), :])
                sel_t = sel.T.astype(bf16)
                same = jnp.dot(sel.astype(bf16), sel_t, preferred_element_type=f32)
                r, c = iota(same.shape, 0), iota(same.shape, 1)
                same = jnp.where(r // (2 * CAP) == c // (2 * CAP), same, 0.0)
                earlier = jnp.sum(jnp.where(c < r, same, 0.0), axis=1, keepdims=True)
                fold[d][i] = jnp.where(earlier > 0.0, 0.0, same).astype(bf16)
                selt[d][i] = sel_t
                return carry

            lax.fori_loop(0, side, one, 0)

    def combine(b):
        for d, (lo, width) in enumerate(parts):
            yacc[:, lo:lo + width] = jnp.zeros((tokens, width), f32)

            def one(i, carry, d=d, lo=lo, width=width):
                z = zr[d][b, i].astype(f32).reshape(rows, width).astype(bf16)
                part = jnp.dot(fold[d][i], z, preferred_element_type=f32).astype(bf16)
                yacc[:, lo:lo + width] += jnp.dot(selt[d][i], part, preferred_element_type=f32)
                return carry

            lax.fori_loop(0, side, one, 0)
        ys[b][...] = yacc[...].astype(bf16)

    def keep_third(b):
        for d in range(3):
            xr[final(d, b, 0, 0)] = p2r[d][b, 0, 0]

    def keep_back_third(b):
        for d in range(3):
            p2r[d][b, 0, 0] = xr[final(d, b, 0, 0)]

    def keep_back_second(b):
        for d in range(3):
            r2[d][b, 0] = p2r[d][mid(d, b, 0)]

    def keep_back_first(b):
        for d in range(3):
            zr[d][b, 0] = r2[d][b, :, :, :, 0]

    half = side // 2
    odd = [i for i in range(1, side) if i != half]

    pl.semaphore_wait(barrier, n - 1)
    start(gather(0))
    start(gather(1))
    lax.fori_loop(1, n, send_gate, 0)
    gr[0:1] = gs[pl.ds(grp * 2 + ing, 1)]

    arrived(gather(0))
    select(0)
    start(second(0, range(1, side)))
    arrived(gather(1))
    select(1)
    start(second(1, [half]))
    arrived(second(0, range(1, side)))
    start(third(0))
    start(second(1, odd))
    keep_third(0)
    for copy in weights:
        copy.wait()
    gates_all.wait_recv()
    arrived(third(0))
    ffn(0, 0, side - 1)
    arrived(second(1, range(1, side)))
    left(third(0))
    start(third(1))
    keep_third(1)
    ffn(0, side - 1, side)
    arrived(third(1))
    left(third(1))
    start(back_third(0))
    keep_back_third(0)
    ffn(1, 0, side - 1)
    arrived(back_third(0))
    start(back_second(0))
    keep_back_second(0)
    ffn(1, side - 1, side)
    start(back_third(1))
    keep_back_third(1)
    arrived(back_second(0))
    start(back_first(0, odd))
    keep_back_first(0)
    tables(0)
    arrived(back_third(1))
    start(back_second(1))
    keep_back_second(1)
    start(back_first(0, [half]))
    arrived(back_second(1))
    start(back_first(1, range(1, side)))
    keep_back_first(1)
    arrived(back_first(0, range(1, side)))
    combine(0)
    tables(1)
    arrived(back_first(1, range(1, side)))
    combine(1)

    gates_all.wait_send()
    for b in range(2):
        every = range(1, side)
        for copies in (gather(b), second(b, every), back_third(b), back_second(b), back_first(b, every)):
            left(copies)


def solution(mesh):
    n_grp = mesh.shape['grp']
    side = round(n_grp ** (1 / 3))
    n = side ** 3 * 2
    plane = n // side
    tok_spec = P(('dp', 'grp', 'ing'), None)
    w_spec = P(('grp', 'ing'), None, None)

    def body(x1, ids1, g1, x2, ids2, g2, w1, w3, w2):
        tokens, hidden = x1.shape
        ff = w1.shape[2]
        vmem = pl.BlockSpec(memory_space=pltpu.VMEM)
        hbm = pl.BlockSpec(memory_space=pl.ANY)
        out = jax.ShapeDtypeStruct((tokens, hidden), jnp.bfloat16)
        widths = [w for _, w in lane_parts(hidden)]

        def per_part(*shape):
            return [pltpu.VMEM((*shape, w), jnp.bfloat16) for w in widths]

        def per_dim(*shape):
            return [pltpu.VMEM(shape, jnp.bfloat16) for _ in widths]

        rows = plane * CAP
        gate = pltpu.VMEM((n, 1, LANES), jnp.float32)
        return pl.pallas_call(
            functools.partial(moe_kernel, side),
            out_shape=(out, out),
            in_specs=[vmem] * 6 + [hbm] * 3,
            out_specs=(vmem, vmem),
            scratch_shapes=[per_part(2, side, tokens),
                            per_part(2, side - 1, side, 2, side, CAP),
                            per_part(2, side, 2, side, side, CAP),
                            per_part(2, side, side, 2, side, CAP),
                            per_part(2, side, side, side, 2, CAP),
                            per_dim(2, n, tokens),
                            per_dim(2, side, plane, tokens),
                            per_dim(side, tokens, rows),
                            per_dim(side, rows, rows),
                            pltpu.VMEM((2, side, side, side, 2, CAP, hidden), jnp.bfloat16),
                            gate, gate,
                            pltpu.VMEM((hidden, ff), jnp.bfloat16),
                            pltpu.VMEM((hidden, ff), jnp.bfloat16),
                            pltpu.VMEM((ff, hidden), jnp.bfloat16),
                            pltpu.VMEM((tokens, hidden), jnp.float32),
                            pltpu.SemaphoreType.DMA((3,)), pltpu.SemaphoreType.DMA((2,)),
                            [pltpu.SemaphoreType.DMA((2, 2, 3, k * side)) for k in (1, 1, 1, 2, 2, 1, 1)]],
            compiler_params=pltpu.CompilerParams(collective_id=0, has_side_effects=True,
                                                 vmem_limit_bytes=67_000_000),
        )(x1, x2, ids1.T, ids2.T, g1.T, g2.T, w1, w3, w2)

    return jax.shard_map(body, mesh=mesh, in_specs=(tok_spec,) * 6 + (w_spec,) * 3,
                         out_specs=(tok_spec, tok_spec), check_vma=False)
```

```python
import functools

import jax
import jax.numpy as jnp
from jax import lax
from jax.experimental import pallas as pl
from jax.experimental.pallas import tpu as pltpu
from jax.sharding import PartitionSpec as P

MESH = pl.DeviceIdType.MESH
CAP = 8
LANES = 128


def lane_parts(hidden):
    tiles = hidden // LANES
    sizes = [(tiles // 3 + (1 if d < tiles % 3 else 0)) * LANES for d in range(3)]
    return [(sum(sizes[:d]), sizes[d]) for d in range(3)]


def moe_kernel(side, x1, x2, ids1, ids2, gt1, gt2, w1_hbm, w3_hbm, w2_hbm, y1, y2,
               ag, p2s, p2r, r2, zr, vt, vr, selt, fold, xr, gs, gr, w1, w3, w2,
               wsem, gsem, sems):
    xs, ys = (x1, x2), (y1, y2)
    tokens, hidden = x1.shape
    n = side ** 3 * 2
    plane = n // side
    rows = plane * CAP
    parts = lane_parts(hidden)
    grp = lax.axis_index('grp')
    ing = lax.axis_index('ing')
    me = (grp % side, (grp // side) % side, grp // (side * side))
    order = [(d, (d + 1) % 3, (d + 2) % 3) for d in range(3)]
    f32, bf16 = jnp.float32, jnp.bfloat16

    def at(off, core=0):
        x, y, z = ((m + o) % side for m, o in zip(me, off))
        return (z * side + y) * side + x, (ing + core) % 2

    def along(dim, step, core=0):
        off = [0, 0, 0]
        off[dim] = step % side
        return at(off, core)

    def remote(src, dst, send, recv, dev):
        return pltpu.make_async_remote_copy(src_ref=src, dst_ref=dst, send_sem=send, recv_sem=recv,
                                            device_id={'grp': dev[0], 'ing': dev[1]}, device_id_type=MESH)

    def iota(shape, dim):
        return lax.broadcasted_iota(jnp.int32, shape, dim)

    def split(q):
        return q // (side * side * 2), (q // (side * 2)) % side, (q // 2) % side, q % 2

    barrier = pltpu.get_barrier_semaphore()
    for c in range(2):
        def knock(q, carry, c=c):
            pl.semaphore_signal(barrier, inc=1, device_id_type=MESH,
                                device_id={'grp': lax.rem(grp + q, n // 2), 'ing': lax.rem(ing + c, 2)})
            return carry

        lax.fori_loop(1 - c, n // 2, knock, 0)
    weights = [pltpu.make_async_copy(src, dst, wsem.at[k])
               for k, (src, dst) in enumerate(((w1_hbm.at[0], w1), (w3_hbm.at[0], w3), (w2_hbm.at[0], w2)))]
    for copy in weights:
        copy.start()

    def expert_at(q, d):
        off = [None] * 3
        for dim, o in zip(order[d], split(q)):
            off[dim] = o
        to_grp, to_ing = at(off, q % 2)
        return to_grp * 2 + to_ing

    later = (iota((tokens, tokens), 0) < iota((tokens, tokens), 1)).astype(f32).astype(bf16)
    expert = expert_at(iota((n, 1), 0), 0)
    gate_rows = jnp.zeros((n, LANES), f32)
    lane = iota((n, LANES), 1)
    perms = [(expert_at(iota((n, 1), 0), d) == expert_at(iota((1, n), 1), 0)).astype(f32).astype(bf16) for d in (1, 2)]
    for b, (ids, gates) in enumerate(((ids1, gt1), (ids2, gt2))):
        member = jnp.zeros((n, tokens), f32)
        gate = jnp.zeros((n, tokens), f32)
        for j in range(ids.shape[0]):
            hit = ids[j:j + 1, :] == expert
            member = jnp.where(hit, 1.0, member)
            gate = jnp.where(hit, gates[j:j + 1, :], gate)
        before = jnp.dot(member.astype(bf16), later, preferred_element_type=f32)
        table = jnp.where(member > 0.0, before + 1.0, 0.0)
        short = table.astype(bf16)
        for d in range(3):
            vt[d][b] = jnp.dot(perms[d - 1], short, preferred_element_type=f32).astype(bf16) if d else short
            vr[d][b, 0] = vt[d][b, 0:plane, :]
        for k in range(CAP):
            col = jnp.sum(jnp.where(table == k + 1.0, gate, 0.0), axis=1, keepdims=True)
            gate_rows = jnp.where(lane == b * CAP + k, col, gate_rows)
    gs[...] = gate_rows[:, None, :]
    for b in range(2):
        for d, (lo, width) in enumerate(parts):
            ag[d][b, 0] = xs[b][:, lo:lo + width]

    up = [f < s for f, s, t in order]
    every = range(1, side)
    ends = [(k, c) for k in range(side) for c in range(2) if k + c]

    def sem(phase, b, d, k):
        return sems[phase].at[0, b, d, k], sems[phase].at[1, b, d, k]

    def gather(b, d):
        lo, width = parts[d]
        out = []
        for i in every:
            dev = along(order[d][0], i)
            out.append(remote(vt[d].at[b, pl.ds(i * plane, plane)], vr[d].at[b, i], *sem(0, b, d, i), dev))
            out.append(remote(xs[b].at[:, pl.ds(lo, width)], ag[d].at[b, i], *sem(1, b, d, i), dev))
        return out

    def mid(d, b, j):
        return (b, slice(None), slice(None), slice(None), j) if up[d] else (b, slice(None), slice(None), j)

    def second(b, d):
        return [remote(p2s[d].at[b, j], p2r[d].at[mid(d, b, j)], *sem(2, b, d, j), along(order[d][1], j)) for j in every]

    def final(d, b, k, core):
        lo, width = parts[d]
        index = [slice(None)] * 3
        index[order[d][2]] = k
        return (b, *index, core, slice(None), pl.ds(lo, width))

    def third(b, d):
        return [remote(p2r[d].at[b, k, c], xr.at[final(d, b, k, c)], *sem(3, b, d, 2 * k + c), along(order[d][2], k, c))
                for k, c in ends]

    def back_third(b, d):
        return [remote(xr.at[final(d, b, k, c)], p2s[d].at[b, :, k, c], *sem(4, b, d, 2 * k + c),
                       along(order[d][2], -k, c)) for k, c in ends]

    def back_mid(d, b, j):
        return (b, slice(None), slice(None), slice(None), j) if up[d] else (b, j)

    def back_second(b, d):
        return [remote(p2s[d].at[back_mid(d, b, j)], r2[d].at[b, j], *sem(5, b, d, j), along(order[d][1], -j))
                for j in every]

    def back_near(d, b, i):
        return (b, slice(None), i) if up[d] else (b, slice(None), slice(None), slice(None), i)

    def back_first(b, d):
        return [remote(r2[d].at[back_near(d, b, i)], zr[d].at[b, i], *sem(6, b, d, i), along(order[d][0], -i))
                for i in every]

    def gate_copy(q):
        ox, oy, oz, oc = split(q)
        return remote(gs.at[pl.ds(q, 1)], gr.at[pl.ds(q, 1)], gsem.at[0], gsem.at[1], at((ox, oy, oz), oc))

    def send_gate(q, carry):
        gate_copy(q).start()
        return carry

    gates_all = remote(gs.at[pl.ds(1, n - 1)], gr.at[pl.ds(1, n - 1)], gsem.at[0], gsem.at[1], (grp, ing))

    def start(copies):
        for copy in copies:
            copy.start()

    def arrived(copies):
        for copy in copies:
            copy.wait_recv()

    def left(copies):
        for copy in copies:
            copy.wait_send()

    def expand():
        return (iota((rows, plane), 0) // CAP == iota((rows, plane), 1)).astype(f32).astype(bf16)

    def chosen(table):
        v = jnp.dot(expand(), table, preferred_element_type=f32)
        return jnp.where(v == (iota(v.shape, 0) % CAP + 1).astype(f32), 1.0, 0.0)

    def select(b, d):
        width = parts[d][1]

        def pick(i, carry):
            sel = chosen(vr[d][b, i]).astype(bf16)
            out = jnp.dot(sel, ag[d][b, i], preferred_element_type=f32)
            out = out.reshape(side, side, 2, CAP, width).astype(bf16)
            if up[d]:
                p2r[d][b, :, :, i, 0] = out[0]
            else:
                p2r[d][b, :, :, 0, i] = out[0]
            for j in every:
                p2s[d][b, j, :, :, i] = out[j]
            return carry

        lax.fori_loop(0, side, pick, 0)

    def ffn(b):
        def chunk(ox, carry):
            rec = xr[b, ox].astype(f32).reshape(rows, hidden).astype(bf16)
            act_a = jnp.dot(rec, w1[...], preferred_element_type=f32)
            act_b = jnp.dot(rec, w3[...], preferred_element_type=f32)
            inner = (act_a * jax.nn.sigmoid(act_a) * act_b).astype(bf16)
            g = gr[pl.ds(ox * plane, plane)]
            g = jnp.broadcast_to(g, (plane, CAP, LANES)).reshape(rows, LANES)
            mine = iota(g.shape, 1) == b * CAP + iota(g.shape, 0) % CAP
            g = jnp.sum(jnp.where(mine, g, 0.0), axis=1, keepdims=True)
            out = jnp.dot(inner, w2[...], preferred_element_type=f32) * g
            xr[b, ox] = out.reshape(side, side, 2, CAP, hidden).astype(bf16)
            return carry

        lax.fori_loop(0, side, chunk, 0)

    def tables(b):
        for d in range(3):
            def one(i, carry, d=d):
                sel = chosen(vt[d][b, pl.ds(pl.multiple_of(i * plane, plane), plane), :])
                sel_t = sel.T.astype(bf16)
                same = jnp.dot(sel.astype(bf16), sel_t, preferred_element_type=f32)
                r, c = iota(same.shape, 0), iota(same.shape, 1)
                same = jnp.where(r // (2 * CAP) == c // (2 * CAP), same, 0.0)
                earlier = jnp.sum(jnp.where(c < r, same, 0.0), axis=1, keepdims=True)
                fold[d][i] = jnp.where(earlier > 0.0, 0.0, same).astype(bf16)
                selt[d][i] = sel_t
                return carry

            lax.fori_loop(0, side, one, 0)

    def combine(b, d):
        lo, width = parts[d]
        ys[b][:, lo:lo + width] = jnp.zeros((tokens, width), f32)

        def one(i, carry):
            z = zr[d][b, i].astype(f32).reshape(rows, width).astype(bf16)
            part = jnp.dot(fold[d][i], z, preferred_element_type=f32).astype(bf16)
            ys[b][:, lo:lo + width] += jnp.dot(selt[d][i], part, preferred_element_type=f32)
            return carry

        lax.fori_loop(0, side, one, 0)

    narrow_first = (1, 2, 0)
    pl.semaphore_wait(barrier, n - 1)
    for b in range(2):
        for d in narrow_first:
            start(gather(b, d))
    lax.fori_loop(1, n, send_gate, 0)
    gr[0:1] = gs[0:1]
    for b in range(2):
        for d in narrow_first:
            arrived(gather(b, d))
            select(b, d)
            start(second(b, d))
    for b in range(2):
        for d in narrow_first:
            arrived(second(b, d))
            left(second(b, d))
            start(third(b, d))
            xr[final(d, b, 0, 0)] = p2r[d][b, 0, 0]
    for copy in weights:
        copy.wait()
    for b in range(2):
        for d in narrow_first:
            arrived(third(b, d))
        if b == 0:
            gates_all.wait_recv()
        ffn(b)
        for d in narrow_first:
            start(back_third(b, d))
            p2s[d][b, :, 0, 0] = xr[final(d, b, 0, 0)]
    for b in range(2):
        for d in narrow_first:
            arrived(back_third(b, d))
            start(back_second(b, d))
            r2[d][b, 0] = p2s[d][back_mid(d, b, 0)]
    for b in range(2):
        for d in narrow_first:
            arrived(back_second(b, d))
            start(back_first(b, d))
            zr[d][b, 0] = r2[d][back_near(d, b, 0)]
        if b == 0:
            tables(0)
    for b in range(2):
        for d in narrow_first:
            arrived(back_first(b, d))
            combine(b, d)
        if b == 0:
            tables(1)

    gates_all.wait_send()
    for b in range(2):
        for d in range(3):
            left(gather(b, d) + third(b, d) + back_third(b, d) + back_second(b, d) + back_first(b, d))


def solution(mesh):
    n_grp = mesh.shape['grp']
    side = round(n_grp ** (1 / 3))
    n = side ** 3 * 2
    plane = n // side
    tok_spec = P(('dp', 'grp', 'ing'), None)
    w_spec = P(('grp', 'ing'), None, None)

    def body(x1, ids1, g1, x2, ids2, g2, w1, w3, w2):
        tokens, hidden = x1.shape
        ff = w1.shape[2]
        vmem = pl.BlockSpec(memory_space=pltpu.VMEM)
        hbm = pl.BlockSpec(memory_space=pl.ANY)
        out = jax.ShapeDtypeStruct((tokens, hidden), jnp.float32)
        widths = [w for _, w in lane_parts(hidden)]

        def per_part(*shape):
            return [pltpu.VMEM((*shape, w), jnp.bfloat16) for w in widths]

        def per_dim(*shape):
            return [pltpu.VMEM(shape, jnp.bfloat16) for _ in widths]

        rows = plane * CAP
        gate = pltpu.VMEM((n, 1, LANES), jnp.float32)
        y1, y2 = pl.pallas_call(
            functools.partial(moe_kernel, side),
            out_shape=(out, out),
            in_specs=[vmem] * 6 + [hbm] * 3,
            out_specs=(vmem, vmem),
            scratch_shapes=[per_part(2, side, tokens),
                            per_part(2, side, side, 2, side, CAP),
                            per_part(2, side, 2, side, side, CAP),
                            [pltpu.VMEM((2, side, *((side, side, 2) if d < 2 else (side, 2, side)), CAP, w), jnp.bfloat16)
                             for d, w in enumerate(widths)],
                            per_part(2, side, side, side, 2, CAP),
                            per_dim(2, n, tokens),
                            per_dim(2, side, plane, tokens),
                            per_dim(side, tokens, rows),
                            per_dim(side, rows, rows),
                            pltpu.VMEM((2, side, side, side, 2, CAP, hidden), jnp.bfloat16),
                            gate, gate,
                            pltpu.VMEM((hidden, ff), jnp.bfloat16),
                            pltpu.VMEM((hidden, ff), jnp.bfloat16),
                            pltpu.VMEM((ff, hidden), jnp.bfloat16),
                            pltpu.SemaphoreType.DMA((3,)), pltpu.SemaphoreType.DMA((2,)),
                            [pltpu.SemaphoreType.DMA((2, 2, 3, k * side)) for k in (1, 1, 1, 2, 2, 1, 1)]],
            compiler_params=pltpu.CompilerParams(collective_id=0, has_side_effects=True,
                                                 vmem_limit_bytes=67_000_000),
        )(x1, x2, ids1.T, ids2.T, g1.T, g2.T, w1, w3, w2)
        return y1.astype(jnp.bfloat16), y2.astype(jnp.bfloat16)

    return jax.shard_map(body, mesh=mesh, in_specs=(tok_spec,) * 6 + (w_spec,) * 3,
                         out_specs=(tok_spec, tok_spec), check_vma=False)
```

```python
import functools

import jax
import jax.numpy as jnp
from jax import lax
from jax.experimental import pallas as pl
from jax.experimental.pallas import tpu as pltpu
from jax.sharding import PartitionSpec as P

MESH = pl.DeviceIdType.MESH
CAP = 8
LANES = 128


def lane_parts(hidden):
    tiles = hidden // LANES
    sizes = [(tiles // 3 + (1 if d < tiles % 3 else 0)) * LANES for d in range(3)]
    return [(sum(sizes[:d]), sizes[d]) for d in range(3)]


def moe_kernel(side, x1, x2, ids1, ids2, gt1, gt2, w1_hbm, w3_hbm, w2_hbm, y,
               ag, p2s, p2r, r2, zr, vt, vr, selt, fold, xr, gs, ga, gb, gr, w1, w3, w2, yacc,
               wsem, gsem, sems):
    xs = (x1, x2)
    tokens, hidden = x1.shape
    n = side ** 3 * 2
    plane = n // side
    rows = plane * CAP
    parts = lane_parts(hidden)
    grp = lax.axis_index('grp')
    ing = lax.axis_index('ing')
    me = (grp % side, (grp // side) % side, grp // (side * side))
    order = [(d, (d + 1) % 3, (d + 2) % 3) for d in range(3)]
    f32, bf16 = jnp.float32, jnp.bfloat16

    def at(off, core=0):
        x, y, z = ((m + o) % side for m, o in zip(me, off))
        return (z * side + y) * side + x, (ing + core) % 2

    def along(dim, step, core=0):
        off = [0, 0, 0]
        off[dim] = step % side
        return at(off, core)

    def remote(src, dst, send, recv, dev):
        return pltpu.make_async_remote_copy(src_ref=src, dst_ref=dst, send_sem=send, recv_sem=recv,
                                            device_id={'grp': dev[0], 'ing': dev[1]}, device_id_type=MESH)

    def iota(shape, dim):
        return lax.broadcasted_iota(jnp.int32, shape, dim)

    def split(q):
        return q // (side * side * 2), (q // (side * 2)) % side, (q // 2) % side, q % 2

    barrier = pltpu.get_barrier_semaphore()
    for dim in range(3):
        def knock(q, carry, dim=dim):
            dev = along(dim, q // 2, q % 2)
            pl.semaphore_signal(barrier, inc=1, device_id={'grp': dev[0], 'ing': dev[1]}, device_id_type=MESH)
            return carry

        lax.fori_loop(2 if dim else 1, 2 * side, knock, 0)
    peers = 6 * side - 5
    weights = [pltpu.make_async_copy(src, dst, wsem.at[k])
               for k, (src, dst) in enumerate(((w1_hbm.at[0], w1), (w3_hbm.at[0], w3), (w2_hbm.at[0], w2)))]
    for copy in weights:
        copy.start()

    def expert_at(q, d):
        off = [None] * 3
        for dim, o in zip(order[d], split(q)):
            off[dim] = o
        to_grp, to_ing = at(off, q % 2)
        return to_grp * 2 + to_ing

    later = (iota((tokens, tokens), 0) < iota((tokens, tokens), 1)).astype(f32).astype(bf16)
    expert = expert_at(iota((n, 1), 0), 0)
    gate_rows = jnp.zeros((n, LANES), f32)
    lane = iota((n, LANES), 1)
    perms = [(expert_at(iota((n, 1), 0), d) == expert_at(iota((1, n), 1), 0)).astype(f32).astype(bf16) for d in (1, 2)]
    for b, (ids, gates) in enumerate(((ids1, gt1), (ids2, gt2))):
        member = jnp.zeros((n, tokens), f32)
        gate = jnp.zeros((n, tokens), f32)
        for j in range(ids.shape[0]):
            hit = ids[j:j + 1, :] == expert
            member = jnp.where(hit, 1.0, member)
            gate = jnp.where(hit, gates[j:j + 1, :], gate)
        before = jnp.dot(member.astype(bf16), later, preferred_element_type=f32)
        table = jnp.where(member > 0.0, before + 1.0, 0.0)
        short = table.astype(bf16)
        for d in range(3):
            vt[d][b] = jnp.dot(perms[d - 1], short, preferred_element_type=f32).astype(bf16) if d else short
            vr[d][b, 0] = vt[d][b, 0:plane, :]
        for k in range(CAP):
            col = jnp.sum(jnp.where(table == k + 1.0, gate, 0.0), axis=1, keepdims=True)
            gate_rows = jnp.where(lane == b * CAP + k, col, gate_rows)
    gs[...] = gate_rows[:, None, :]
    for b in range(2):
        for d, (lo, width) in enumerate(parts):
            ag[d][b, 0] = xs[b][:, lo:lo + width]

    up = [f < s for f, s, t in order]
    every = range(1, side)
    ends = [(k, c) for k in range(side) for c in range(2) if k + c]

    def sem(phase, b, d, k):
        return sems[phase].at[0, b, d, k], sems[phase].at[1, b, d, k]

    def gather(b, d):
        out = []
        for i in every:
            dev = along(order[d][0], i)
            out.append(remote(vt[d].at[b, pl.ds(i * plane, plane)], vr[d].at[b, i], *sem(0, b, d, i), dev))
            out.append(remote(ag[d].at[b, 0], ag[d].at[b, i], *sem(1, b, d, i), dev))
        return out

    def mid(d, b, j):
        return (b, slice(None), slice(None), slice(None), j) if up[d] else (b, slice(None), slice(None), j)

    def second(b, d):
        return [remote(p2s[d].at[b, j], p2r[d].at[mid(d, b, j)], *sem(2, b, d, j), along(order[d][1], j)) for j in every]

    def final(d, b, k, core):
        lo, width = parts[d]
        index = [slice(None)] * 3
        index[order[d][2]] = k
        return (b, *index, core, slice(None), pl.ds(lo, width))

    def third(b, d):
        return [remote(p2r[d].at[b, k, c], xr.at[final(d, b, k, c)], *sem(3, b, d, 2 * k + c), along(order[d][2], k, c))
                for k, c in ends]

    def back_third(b, d):
        return [remote(xr.at[final(d, b, k, c)], p2s[d].at[b, :, k, c], *sem(4, b, d, 2 * k + c),
                       along(order[d][2], -k, c)) for k, c in ends]

    def back_mid(d, b, j):
        return (b, slice(None), slice(None), slice(None), j) if up[d] else (b, j)

    def back_second(b, d):
        return [remote(p2s[d].at[back_mid(d, b, j)], r2[d].at[b, j], *sem(5, b, d, j), along(order[d][1], -j))
                for j in every]

    def back_near(d, b, i):
        return (b, slice(None), i) if up[d] else (b, slice(None), slice(None), slice(None), i)

    def back_first(b, d):
        return [remote(r2[d].at[back_near(d, b, i)], zr[d].at[b, i], *sem(6, b, d, i), along(order[d][0], -i))
                for i in every]

    far = 2 * side

    def gate_first():
        return [remote(gs.at[pl.ds(i * plane, plane)], ga.at[i], gsem.at[0, 0, i], gsem.at[1, 0, i], along(0, i))
                for i in every]

    def gate_second():
        return [remote(ga.at[:, pl.ds(j * far, far)], gb.at[:, j], gsem.at[0, 1, j], gsem.at[1, 1, j], along(1, j))
                for j in every]

    def gate_third():
        return [remote(gb.at[:, :, 2 * k + c], gr.at[:, :, 2 * k + c], gsem.at[0, 2, 2 * k + c],
                       gsem.at[1, 2, 2 * k + c], along(2, k, c)) for k, c in ends]

    def start(copies):
        for copy in copies:
            copy.start()

    def arrived(copies):
        for copy in copies:
            copy.wait_recv()

    def mixed(lists):
        return [copy for turn in zip(*lists) for copy in turn]

    def left(copies):
        for copy in copies:
            copy.wait_send()

    def expand():
        return (iota((rows, plane), 0) // CAP == iota((rows, plane), 1)).astype(f32).astype(bf16)

    def chosen(table):
        v = jnp.dot(expand(), table, preferred_element_type=f32)
        return jnp.where(v == (iota(v.shape, 0) % CAP + 1).astype(f32), 1.0, 0.0)

    def select(b, d):
        width = parts[d][1]

        def pick(i, carry):
            sel = chosen(vr[d][b, i]).astype(bf16)
            out = jnp.dot(sel, ag[d][b, i], preferred_element_type=f32)
            out = out.reshape(side, side, 2, CAP, width).astype(bf16)
            if up[d]:
                p2r[d][b, :, :, i, 0] = out[0]
            else:
                p2r[d][b, :, :, 0, i] = out[0]
            for j in every:
                p2s[d][b, j, :, :, i] = out[j]
            return carry

        lax.fori_loop(0, side, pick, 0)

    def ffn(b):
        def chunk(ox, carry):
            rec = xr[b, ox].astype(f32).reshape(rows, hidden).astype(bf16)
            act_a = jnp.dot(rec, w1[...], preferred_element_type=f32)
            act_b = jnp.dot(rec, w3[...], preferred_element_type=f32)
            inner = (act_a * jax.nn.sigmoid(act_a) * act_b).astype(bf16)
            g = gr[ox].reshape(plane, 1, LANES)
            g = jnp.broadcast_to(g, (plane, CAP, LANES)).reshape(rows, LANES)
            mine = iota(g.shape, 1) == b * CAP + iota(g.shape, 0) % CAP
            g = jnp.sum(jnp.where(mine, g, 0.0), axis=1, keepdims=True)
            out = jnp.dot(inner, w2[...], preferred_element_type=f32) * g
            xr[b, ox] = out.reshape(side, side, 2, CAP, hidden).astype(bf16)
            return carry

        lax.fori_loop(0, side, chunk, 0)

    def tables(b):
        for d in range(3):
            def one(i, carry, d=d):
                sel = chosen(vt[d][b, pl.ds(pl.multiple_of(i * plane, plane), plane), :])
                sel_t = sel.T.astype(bf16)
                same = jnp.dot(sel.astype(bf16), sel_t, preferred_element_type=f32)
                r, c = iota(same.shape, 0), iota(same.shape, 1)
                same = jnp.where(r // (2 * CAP) == c // (2 * CAP), same, 0.0)
                earlier = jnp.sum(jnp.where(c < r, same, 0.0), axis=1, keepdims=True)
                fold[d][i] = jnp.where(earlier > 0.0, 0.0, same).astype(bf16)
                selt[d][i] = sel_t
                return carry

            lax.fori_loop(0, side, one, 0)

    def combine(b, d):
        lo, width = parts[d]
        yacc[:, lo:lo + width] = jnp.zeros((tokens, width), f32)

        def one(i, carry):
            z = zr[d][b, i].astype(f32).reshape(rows, width).astype(bf16)
            part = jnp.dot(fold[d][i], z, preferred_element_type=f32).astype(bf16)
            yacc[:, lo:lo + width] += jnp.dot(selt[d][i], part, preferred_element_type=f32)
            return carry

        lax.fori_loop(0, side, one, 0)
        y[b, :, lo:lo + width] = yacc[:, lo:lo + width].astype(bf16)

    narrow_first = (1, 2, 0)

    def both(body):
        def step(b, carry):
            body(b)
            return carry

        lax.fori_loop(0, 2, step, 0)

    def gather_tokens(b):
        start(mixed([gather(b, d) for d in narrow_first]))
        pl.when(b == 0)(lambda: start(gate_first()))

    def pick_rows(b):
        for d in narrow_first:
            arrived(gather(b, d))
            select(b, d)
            start(second(b, d))

        @pl.when(b == 0)
        def _():
            arrived(gate_first())
            start(gate_second())
            gb[:, 0] = ga[:, 0:far]

    def last_hop(b):
        for d in narrow_first:
            arrived(second(b, d))
            left(second(b, d))
            start(third(b, d))
            xr[final(d, b, 0, 0)] = p2r[d][b, 0, 0]

        @pl.when(b == 0)
        def _():
            arrived(gate_second())
            start(gate_third())
            gr[:, :, 0] = gb[:, :, 0]

    def experts(b):
        for d in narrow_first:
            arrived(third(b, d))
        pl.when(b == 0)(lambda: arrived(gate_third()))
        ffn(b)
        start(mixed([back_third(b, d) for d in narrow_first]))
        for d in narrow_first:
            p2s[d][b, :, 0, 0] = xr[final(d, b, 0, 0)]

    def return_second(b):
        for d in narrow_first:
            arrived(back_third(b, d))
            start(back_second(b, d))
            r2[d][b, 0] = p2s[d][back_mid(d, b, 0)]

    def return_first(b):
        for d in narrow_first:
            arrived(back_second(b, d))
            start(back_first(b, d))
            zr[d][b, 0] = r2[d][back_near(d, b, 0)]

    def finish(b):
        for d in narrow_first:
            arrived(back_first(b, d))
            combine(b, d)
        pl.when(b == 0)(lambda: tables(1))

    def drain(b):
        for d in range(3):
            left(gather(b, d) + third(b, d) + back_third(b, d) + back_second(b, d) + back_first(b, d))

    pl.semaphore_wait(barrier, peers)
    ga[0] = gs[0:plane]
    both(gather_tokens)
    both(pick_rows)
    both(last_hop)
    for copy in weights:
        copy.wait()
    both(experts)
    both(return_second)
    both(return_first)
    tables(0)
    both(finish)
    left(gate_first() + gate_second() + gate_third())
    both(drain)


def copy_kernel(y, y1, y2, buf, sem):
    pieces = buf.shape[0] // 2
    size = buf.shape[1]
    moves = []
    for k in range(pieces):
        for b, dst in enumerate((y1, y2)):
            slot = 2 * k + b
            part = pl.ds(k * size, size)
            moves.append((pltpu.make_async_copy(y.at[b, part], buf.at[slot], sem.at[0, slot]),
                          pltpu.make_async_copy(buf.at[slot], dst.at[part], sem.at[1, slot])))
    for come, _ in moves:
        come.start()
    for come, go in moves:
        come.wait()
        go.start()
    for _, go in moves:
        go.wait()


def hand_on(y, pieces=4):
    hbm = pl.BlockSpec(memory_space=pl.ANY)
    _, tokens, hidden = y.shape
    shape = jax.ShapeDtypeStruct((tokens, hidden), y.dtype)
    if tokens // pieces % 16:
        pieces = 1
    return pl.pallas_call(
        copy_kernel, out_shape=(shape, shape), in_specs=[hbm], out_specs=(hbm, hbm),
        scratch_shapes=[pltpu.VMEM((2 * pieces, tokens // pieces, hidden), y.dtype),
                        pltpu.SemaphoreType.DMA((2, 2 * pieces))])(y)


def solution(mesh):
    n_grp = mesh.shape['grp']
    side = round(n_grp ** (1 / 3))
    n = side ** 3 * 2
    plane = n // side
    tok_spec = P(('dp', 'grp', 'ing'), None)
    w_spec = P(('grp', 'ing'), None, None)

    def body(x1, ids1, g1, x2, ids2, g2, w1, w3, w2):
        tokens, hidden = x1.shape
        ff = w1.shape[2]
        vmem = pl.BlockSpec(memory_space=pltpu.VMEM)
        hbm = pl.BlockSpec(memory_space=pl.ANY)
        out = jax.ShapeDtypeStruct((2, tokens, hidden), jnp.bfloat16)
        widths = [w for _, w in lane_parts(hidden)]

        def per_part(*shape):
            return [pltpu.VMEM((*shape, w), jnp.bfloat16) for w in widths]

        def per_dim(*shape):
            return [pltpu.VMEM(shape, jnp.bfloat16) for _ in widths]

        rows = plane * CAP

        def gate(*shape):
            return pltpu.VMEM((*shape, 1, LANES), jnp.float32)

        y = pl.pallas_call(
            functools.partial(moe_kernel, side),
            out_shape=out,
            in_specs=[vmem] * 6 + [hbm] * 3,
            out_specs=vmem,
            scratch_shapes=[per_part(2, side, tokens),
                            per_part(2, side, side, 2, side, CAP),
                            per_part(2, side, 2, side, side, CAP),
                            [pltpu.VMEM((2, side, *((side, side, 2) if d < 2 else (side, 2, side)), CAP, w), jnp.bfloat16)
                             for d, w in enumerate(widths)],
                            per_part(2, side, side, side, 2, CAP),
                            per_dim(2, n, tokens),
                            per_dim(2, side, plane, tokens),
                            per_dim(side, tokens, rows),
                            per_dim(side, rows, rows),
                            pltpu.VMEM((2, side, side, side, 2, CAP, hidden), jnp.bfloat16),
                            gate(n), gate(side, plane), gate(side, side, 2 * side), gate(side, side, 2 * side),
                            pltpu.VMEM((hidden, ff), jnp.bfloat16),
                            pltpu.VMEM((hidden, ff), jnp.bfloat16),
                            pltpu.VMEM((ff, hidden), jnp.bfloat16),
                            pltpu.VMEM((tokens, hidden), jnp.float32),
                            pltpu.SemaphoreType.DMA((3,)), pltpu.SemaphoreType.DMA((2, 3, 2 * side)),
                            [pltpu.SemaphoreType.DMA((2, 2, 3, k * side)) for k in (1, 1, 1, 2, 2, 1, 1)]],
            compiler_params=pltpu.CompilerParams(collective_id=0, has_side_effects=True,
                                                 vmem_limit_bytes=67_000_000),
        )(x1, x2, ids1.T, ids2.T, g1.T, g2.T, w1, w3, w2)
        return hand_on(y)

    return jax.shard_map(body, mesh=mesh, in_specs=(tok_spec,) * 6 + (w_spec,) * 3,
                         out_specs=(tok_spec, tok_spec), check_vma=False)
```

```python
import functools

import jax
import jax.numpy as jnp
from jax import lax
from jax.experimental import pallas as pl
from jax.experimental.pallas import tpu as pltpu
from jax.sharding import PartitionSpec as P

MESH = pl.DeviceIdType.MESH
CAP = 8
LANES = 128


def lane_parts(hidden):
    tiles = hidden // LANES
    sizes = [(tiles // 3 + (1 if d < tiles % 3 else 0)) * LANES for d in range(3)]
    return [(sum(sizes[:d]), sizes[d]) for d in range(3)]


def moe_kernel(side, x1, x2, ids1, ids2, gt1, gt2, w1_hbm, w3_hbm, w2_hbm, y,
               ag, p2s, p2r, r2, ps, pr, rel, vt, vr, xr, gs, ga, gb, gr, w1, w3, w2,
               wsem, gsem, sems):
    xs = (x1, x2)
    tokens, hidden = x1.shape
    n = side ** 3 * 2
    plane = n // side
    rows = plane * CAP
    parts = lane_parts(hidden)
    grp = lax.axis_index('grp')
    ing = lax.axis_index('ing')
    me = (grp % side, (grp // side) % side, grp // (side * side))
    order = [(d, (d + 1) % 3, (d + 2) % 3) for d in range(3)]
    f32, bf16 = jnp.float32, jnp.bfloat16

    def at(off, core=0):
        x, y, z = ((m + o) % side for m, o in zip(me, off))
        return (z * side + y) * side + x, (ing + core) % 2

    def along(dim, step, core=0):
        off = [0, 0, 0]
        off[dim] = step % side
        return at(off, core)

    def remote(src, dst, send, recv, dev):
        return pltpu.make_async_remote_copy(src_ref=src, dst_ref=dst, send_sem=send, recv_sem=recv,
                                            device_id={'grp': dev[0], 'ing': dev[1]}, device_id_type=MESH)

    def iota(shape, dim):
        return lax.broadcasted_iota(jnp.int32, shape, dim)

    def split(q):
        return q // (side * side * 2), (q // (side * 2)) % side, (q // 2) % side, q % 2

    barrier = pltpu.get_barrier_semaphore()
    for dim in range(3):
        def knock(q, carry, dim=dim):
            dev = along(dim, q // 2, q % 2)
            pl.semaphore_signal(barrier, inc=1, device_id={'grp': dev[0], 'ing': dev[1]}, device_id_type=MESH)
            return carry

        lax.fori_loop(2 if dim else 1, 2 * side, knock, 0)
    peers = 6 * side - 5
    weights = [pltpu.make_async_copy(src, dst, wsem.at[k])
               for k, (src, dst) in enumerate(((w1_hbm.at[0], w1), (w3_hbm.at[0], w3), (w2_hbm.at[0], w2)))]
    for copy in weights:
        copy.start()

    def expert_at(q, d):
        off = [None] * 3
        for dim, o in zip(order[d], split(q)):
            off[dim] = o
        to_grp, to_ing = at(off, q % 2)
        return to_grp * 2 + to_ing

    later = (iota((tokens, tokens), 0) < iota((tokens, tokens), 1)).astype(f32).astype(bf16)
    expert = expert_at(iota((n, 1), 0), 0)
    gate_rows = jnp.zeros((n, LANES), f32)
    lane = iota((n, LANES), 1)
    perms = [(expert_at(iota((n, 1), 0), d) == expert_at(iota((1, n), 1), 0)).astype(f32).astype(bf16) for d in (1, 2)]
    for b, (ids, gates) in enumerate(((ids1, gt1), (ids2, gt2))):
        member = jnp.zeros((n, tokens), f32)
        gate = jnp.zeros((n, tokens), f32)
        for j in range(ids.shape[0]):
            hit = ids[j:j + 1, :] == expert
            member = jnp.where(hit, 1.0, member)
            gate = jnp.where(hit, gates[j:j + 1, :], gate)
        before = jnp.dot(member.astype(bf16), later, preferred_element_type=f32)
        table = jnp.where(member > 0.0, before + 1.0, 0.0)
        short = table.astype(bf16)
        for d in range(3):
            vt[d][b] = jnp.dot(perms[d - 1], short, preferred_element_type=f32).astype(bf16) if d else short
            vr[d][b, 0] = vt[d][b, 0:plane, :]
        for k in range(CAP):
            col = jnp.sum(jnp.where(table == k + 1.0, gate, 0.0), axis=1, keepdims=True)
            gate_rows = jnp.where(lane == b * CAP + k, col, gate_rows)
    gs[...] = gate_rows[:, None, :]
    for b in range(2):
        for d, (lo, width) in enumerate(parts):
            ag[d][b, 0] = xs[b][:, lo:lo + width]

    up = [f < s for f, s, t in order]
    every = range(1, side)
    ends = [(k, c) for k in range(side) for c in range(2) if k + c]

    def sem(phase, b, d, k):
        return sems[phase].at[0, b, d, k], sems[phase].at[1, b, d, k]

    def gather(b, d):
        out = []
        for i in every:
            dev = along(order[d][0], i)
            out.append(remote(vt[d].at[b, pl.ds(i * plane, plane)], vr[d].at[b, i], *sem(0, b, d, i), dev))
            out.append(remote(ag[d].at[b, 0], ag[d].at[b, i], *sem(1, b, d, i), dev))
        return out

    def mid(d, b, j):
        return (b, slice(None), slice(None), slice(None), j) if up[d] else (b, slice(None), slice(None), j)

    def second(b, d):
        return [remote(p2s[d].at[b, j], p2r[d].at[mid(d, b, j)], *sem(2, b, d, j), along(order[d][1], j)) for j in every]

    def final(d, b, k, core):
        lo, width = parts[d]
        index = [slice(None)] * 3
        index[order[d][2]] = k
        return (b, *index, core, slice(None), pl.ds(lo, width))

    def third(b, d):
        return [remote(p2r[d].at[b, k, c], xr.at[final(d, b, k, c)], *sem(3, b, d, 2 * k + c), along(order[d][2], k, c))
                for k, c in ends]

    def back_third(b, d):
        return [remote(xr.at[final(d, b, k, c)], p2s[d].at[b, :, k, c], *sem(4, b, d, 2 * k + c),
                       along(order[d][2], -k, c)) for k, c in ends]

    def back_mid(d, b, j):
        return (b, slice(None), slice(None), slice(None), j) if up[d] else (b, j)

    def back_second(b, d):
        return [remote(p2s[d].at[back_mid(d, b, j)], r2[d].at[b, j], *sem(5, b, d, j), along(order[d][1], -j))
                for j in every]

    def back_near(d, b, i):
        return (b, slice(None), i) if up[d] else (b, slice(None), slice(None), slice(None), i)

    low, high = pl.ds(0, tokens // 2), pl.ds(tokens // 2, tokens // 2)
    ring = side > 2

    def back_relay(b, d):
        f = order[d][0]
        return [remote(ps[d].at[b, 1, low], rel[d].at[b, 0], *sem(6, b, d, 0), along(f, -1)),
                remote(ps[d].at[b, 1, high], rel[d].at[b, 1], *sem(6, b, d, 1), along(f, 1))] if ring else []

    def back_first(b, d):
        f = order[d][0]
        out = [remote(ps[d].at[b, 0, high], pr[d].at[b, 0, high], *sem(6, b, d, 2), along(f, -1))]
        if ring:
            out.append(remote(ps[d].at[b, 2, low], pr[d].at[b, 1, low], *sem(6, b, d, 3), along(f, 1)))
        return out

    def back_last(b, d):
        f = order[d][0]
        out = [remote(ps[d].at[b, 0, low], pr[d].at[b, 0, low], *sem(6, b, d, 4), along(f, -1))]
        if ring:
            out.append(remote(ps[d].at[b, 2, high], pr[d].at[b, 1, high], *sem(6, b, d, 5), along(f, 1)))
        return out

    far = 2 * side

    def gate_first():
        return [remote(gs.at[pl.ds(i * plane, plane)], ga.at[i], gsem.at[0, 0, i], gsem.at[1, 0, i], along(0, i))
                for i in every]

    def gate_second():
        return [remote(ga.at[:, pl.ds(j * far, far)], gb.at[:, j], gsem.at[0, 1, j], gsem.at[1, 1, j], along(1, j))
                for j in every]

    def gate_third():
        return [remote(gb.at[:, :, 2 * k + c], gr.at[:, :, 2 * k + c], gsem.at[0, 2, 2 * k + c],
                       gsem.at[1, 2, 2 * k + c], along(2, k, c)) for k, c in ends]

    def start(copies):
        for copy in copies:
            copy.start()

    def arrived(copies):
        for copy in copies:
            copy.wait_recv()

    def mixed(lists):
        return [copy for turn in zip(*lists) for copy in turn]

    def left(copies):
        for copy in copies:
            copy.wait_send()

    def expand():
        return (iota((rows, plane), 0) // CAP == iota((rows, plane), 1)).astype(f32).astype(bf16)

    def chosen(table):
        v = jnp.dot(expand(), table, preferred_element_type=f32)
        return jnp.where(v == (iota(v.shape, 0) % CAP + 1).astype(f32), 1.0, 0.0)

    def select(b, d):
        width = parts[d][1]

        def pick(i, carry):
            sel = chosen(vr[d][b, i]).astype(bf16)
            out = jnp.dot(sel, ag[d][b, i], preferred_element_type=f32)
            out = out.reshape(side, side, 2, CAP, width).astype(bf16)
            if up[d]:
                p2r[d][b, :, :, i, 0] = out[0]
            else:
                p2r[d][b, :, :, 0, i] = out[0]
            for j in every:
                p2s[d][b, j, :, :, i] = out[j]
            return carry

        lax.fori_loop(0, side, pick, 0)

    def ffn(b):
        def chunk(ox, carry):
            rec = xr[b, ox].astype(f32).reshape(rows, hidden).astype(bf16)
            act_a = jnp.dot(rec, w1[...], preferred_element_type=f32)
            act_b = jnp.dot(rec, w3[...], preferred_element_type=f32)
            inner = (act_a * jax.nn.sigmoid(act_a) * act_b).astype(bf16)
            g = gr[ox].reshape(plane, 1, LANES)
            g = jnp.broadcast_to(g, (plane, CAP, LANES)).reshape(rows, LANES)
            mine = iota(g.shape, 1) == b * CAP + iota(g.shape, 0) % CAP
            g = jnp.sum(jnp.where(mine, g, 0.0), axis=1, keepdims=True)
            out = jnp.dot(inner, w2[...], preferred_element_type=f32) * g
            xr[b, ox] = out.reshape(side, side, 2, CAP, hidden).astype(bf16)
            return carry

        lax.fori_loop(0, side, chunk, 0)

    def tables(b):
        for d in range(3):
            def one(i, carry, d=d):
                sel = chosen(vr[d][b, i])
                sel_t = sel.T.astype(bf16)
                same = jnp.dot(sel.astype(bf16), sel_t, preferred_element_type=f32)
                r, c = iota(same.shape, 0), iota(same.shape, 1)
                same = jnp.where(r // (2 * CAP) == c // (2 * CAP), same, 0.0)
                earlier = jnp.sum(jnp.where(c < r, same, 0.0), axis=1, keepdims=True)
                fold = jnp.where(earlier > 0.0, 0.0, same).astype(bf16)
                for k in range(rows // tokens):
                    ag[d][0, i, :, k * rows:(k + 1) * rows] = fold[k * tokens:(k + 1) * tokens]
                ag[d][1, i, :, 0:rows] = sel_t
                return carry

            lax.fori_loop(0, side, one, 0)

    def partial(b, d, i):
        width = parts[d][1]
        z = r2[d][back_near(d, b, i)].astype(f32).reshape(rows, width).astype(bf16)
        fold = jnp.concatenate([ag[d][0, i, :, k * rows:(k + 1) * rows] for k in range(rows // tokens)], axis=0)
        part = jnp.dot(fold, z, preferred_element_type=f32).astype(bf16)
        return jnp.dot(ag[d][1, i, :, 0:rows], part, preferred_element_type=f32)

    narrow_first = (1, 2, 0)

    def both(body):
        def step(b, carry):
            body(b)
            return carry

        lax.fori_loop(0, 2, step, 0)

    def gather_tokens(b):
        start(mixed([gather(b, d) for d in narrow_first]))
        pl.when(b == 0)(lambda: start(gate_first()))

    def pick_rows(b):
        for d in narrow_first:
            arrived(gather(b, d))
            select(b, d)
            start(second(b, d))

        @pl.when(b == 0)
        def _():
            arrived(gate_first())
            start(gate_second())
            gb[:, 0] = ga[:, 0:far]

    def last_hop(b):
        for d in narrow_first:
            arrived(second(b, d))
            left(second(b, d))
            start(third(b, d))
            xr[final(d, b, 0, 0)] = p2r[d][b, 0, 0]

        @pl.when(b == 0)
        def _():
            arrived(gate_second())
            start(gate_third())
            gr[:, :, 0] = gb[:, :, 0]

    def experts(b):
        for d in narrow_first:
            arrived(third(b, d))
        pl.when(b == 0)(lambda: arrived(gate_third()))
        ffn(b)
        start(mixed([back_third(b, d) for d in narrow_first]))
        for d in narrow_first:
            p2s[d][b, :, 0, 0] = xr[final(d, b, 0, 0)]

    def return_second(b):
        for d in narrow_first:
            arrived(back_third(b, d))
            start(back_second(b, d))
            r2[d][b, 0] = p2s[d][back_mid(d, b, 0)]

    def return_first(b):
        for d, (lo, width) in [(d, parts[d]) for d in narrow_first]:
            arrived(back_second(b, d))

            def one(i, carry, d=d):
                ps[d][b, i - 1] = partial(b, d, i)
                return carry

            lax.fori_loop(1, side, one, 0)
            start(back_relay(b, d) + back_first(b, d))
            y[b, :, lo:lo + width] = partial(b, d, 0)
        pl.when(b == 0)(lambda: tables(1))

    def pass_on(b):
        half = tokens // 2
        for d in narrow_first:
            arrived(back_relay(b, d))
            if ring:
                ps[d][b, 0, 0:half] += rel[d][b, 0]
                ps[d][b, 2, half:tokens] += rel[d][b, 1]
            start(back_last(b, d))

    def finish(b):
        for d, (lo, width) in [(d, parts[d]) for d in narrow_first]:
            arrived(back_first(b, d) + back_last(b, d))
            total = y[b, :, lo:lo + width] + pr[d][b, 0]
            y[b, :, lo:lo + width] = total + pr[d][b, 1] if ring else total

    def drain(b):
        for d in range(3):
            left(third(b, d) + back_third(b, d) + back_second(b, d))
            left(back_relay(b, d) + back_first(b, d) + back_last(b, d))

    pl.semaphore_wait(barrier, peers)
    ga[0] = gs[0:plane]
    both(gather_tokens)
    both(pick_rows)
    both(last_hop)
    for copy in weights:
        copy.wait()
    both(experts)
    both(lambda b: [left(gather(b, d)) for d in range(3)])
    tables(0)
    both(return_second)
    both(return_first)
    both(pass_on)
    both(finish)
    left(gate_first() + gate_second() + gate_third())
    both(drain)


def copy_kernel(y, y1, y2, buf, narrow, sem):
    pieces = buf.shape[0] // 2
    size = buf.shape[1]
    moves = []
    for k in range(pieces):
        for b, dst in enumerate((y1, y2)):
            slot = 2 * k + b
            part = pl.ds(k * size, size)
            moves.append((pltpu.make_async_copy(y.at[b, part], buf.at[slot], sem.at[0, slot]),
                          pltpu.make_async_copy(narrow.at[slot], dst.at[part], sem.at[1, slot])))
    for come, _ in moves:
        come.start()
    for slot, (come, go) in enumerate(moves):
        come.wait()
        narrow[slot] = buf[slot].astype(narrow.dtype)
        go.start()
    for _, go in moves:
        go.wait()


def hand_on(y, pieces=4):
    hbm = pl.BlockSpec(memory_space=pl.ANY)
    _, tokens, hidden = y.shape
    shape = jax.ShapeDtypeStruct((tokens, hidden), jnp.bfloat16)
    if tokens // pieces % 16:
        pieces = 1
    return pl.pallas_call(
        copy_kernel, out_shape=(shape, shape), in_specs=[hbm], out_specs=(hbm, hbm),
        scratch_shapes=[pltpu.VMEM((2 * pieces, tokens // pieces, hidden), y.dtype),
                        pltpu.VMEM((2 * pieces, tokens // pieces, hidden), jnp.bfloat16),
                        pltpu.SemaphoreType.DMA((2, 2 * pieces))])(y)


def solution(mesh):
    n_grp = mesh.shape['grp']
    side = round(n_grp ** (1 / 3))
    n = side ** 3 * 2
    plane = n // side
    tok_spec = P(('dp', 'grp', 'ing'), None)
    w_spec = P(('grp', 'ing'), None, None)

    def body(x1, ids1, g1, x2, ids2, g2, w1, w3, w2):
        tokens, hidden = x1.shape
        ff = w1.shape[2]
        vmem = pl.BlockSpec(memory_space=pltpu.VMEM)
        hbm = pl.BlockSpec(memory_space=pl.ANY)
        out = jax.ShapeDtypeStruct((2, tokens, hidden), jnp.float32)
        widths = [w for _, w in lane_parts(hidden)]

        def per_part(*shape):
            return [pltpu.VMEM((*shape, w), jnp.bfloat16) for w in widths]

        def wide(*shape):
            return [pltpu.VMEM((*shape, w), jnp.float32) for w in widths]

        def per_dim(*shape):
            return [pltpu.VMEM(shape, jnp.bfloat16) for _ in widths]

        rows = plane * CAP

        def gate(*shape):
            return pltpu.VMEM((*shape, 1, LANES), jnp.float32)

        y = pl.pallas_call(
            functools.partial(moe_kernel, side),
            out_shape=out,
            in_specs=[vmem] * 6 + [hbm] * 3,
            out_specs=vmem,
            scratch_shapes=[per_part(2, side, tokens),
                            per_part(2, side, side, 2, side, CAP),
                            per_part(2, side, 2, side, side, CAP),
                            [pltpu.VMEM((2, side, *((side, side, 2) if d < 2 else (side, 2, side)), CAP, w), jnp.bfloat16)
                             for d, w in enumerate(widths)],
                            wide(2, side - 1, tokens), wide(2, 2, tokens), wide(2, 2, tokens // 2),
                            per_dim(2, n, tokens),
                            per_dim(2, side, plane, tokens),
                            pltpu.VMEM((2, side, side, side, 2, CAP, hidden), jnp.bfloat16),
                            gate(n), gate(side, plane), gate(side, side, 2 * side), gate(side, side, 2 * side),
                            pltpu.VMEM((hidden, ff), jnp.bfloat16),
                            pltpu.VMEM((hidden, ff), jnp.bfloat16),
                            pltpu.VMEM((ff, hidden), jnp.bfloat16),
                            pltpu.SemaphoreType.DMA((3,)), pltpu.SemaphoreType.DMA((2, 3, 2 * side)),
                            [pltpu.SemaphoreType.DMA((2, 2, 3, k * side)) for k in (1, 1, 1, 2, 2, 1, 3)]],
            compiler_params=pltpu.CompilerParams(collective_id=0, has_side_effects=True,
                                                 vmem_limit_bytes=67_000_000),
        )(x1, x2, ids1.T, ids2.T, g1.T, g2.T, w1, w3, w2)
        return hand_on(y)

    return jax.shard_map(body, mesh=mesh, in_specs=(tok_spec,) * 6 + (w_spec,) * 3,
                         out_specs=(tok_spec, tok_spec), check_vma=False)
```

```python
import functools

import jax
import jax.numpy as jnp
from jax import lax
from jax.experimental import pallas as pl
from jax.experimental.pallas import tpu as pltpu
from jax.sharding import PartitionSpec as P

MESH = pl.DeviceIdType.MESH
CAP = 8
LANES = 128


def lane_parts(hidden):
    tiles = hidden // LANES
    sizes = [(tiles // 3 + (1 if d < tiles % 3 else 0)) * LANES for d in range(3)]
    return [(sum(sizes[:d]), sizes[d]) for d in range(3)]


def moe_kernel(side, x1, x2, ids1, ids2, gt1, gt2, w1_hbm, w3_hbm, w2_hbm, y,
               ag, p2s, p2r, r2, ps, pr, rel, vt, vr, xr, gs, ga, gb, gr, w1, w3, w2, total, rounded,
               xsem, ysem, wsem, gsem, sems):
    xs = (x1, x2)
    tokens, hidden = x1.shape
    n = side ** 3 * 2
    plane = n // side
    rows = plane * CAP
    parts = lane_parts(hidden)
    grp = lax.axis_index('grp')
    ing = lax.axis_index('ing')
    me = (grp % side, (grp // side) % side, grp // (side * side))
    order = [(d, (d + 1) % 3, (d + 2) % 3) for d in range(3)]
    f32, bf16 = jnp.float32, jnp.bfloat16

    def at(off, core=0):
        x, y, z = ((m + o) % side for m, o in zip(me, off))
        return (z * side + y) * side + x, (ing + core) % 2

    def along(dim, step, core=0):
        off = [0, 0, 0]
        off[dim] = step % side
        return at(off, core)

    def remote(src, dst, send, recv, dev):
        return pltpu.make_async_remote_copy(src_ref=src, dst_ref=dst, send_sem=send, recv_sem=recv,
                                            device_id={'grp': dev[0], 'ing': dev[1]}, device_id_type=MESH)

    def iota(shape, dim):
        return lax.broadcasted_iota(jnp.int32, shape, dim)

    def split(q):
        return q // (side * side * 2), (q // (side * 2)) % side, (q // 2) % side, q % 2

    barrier = pltpu.get_barrier_semaphore()
    for dim in range(3):
        def knock(q, carry, dim=dim):
            dev = along(dim, q // 2, q % 2)
            pl.semaphore_signal(barrier, inc=1, device_id={'grp': dev[0], 'ing': dev[1]}, device_id_type=MESH)
            return carry

        lax.fori_loop(2 if dim else 1, 2 * side, knock, 0)
    peers = 6 * side - 5
    own = [[pltpu.make_async_copy(xs[b].at[:, pl.ds(lo, width)], ag[d].at[b, 0], xsem.at[b, d])
            for d, (lo, width) in enumerate(parts)] for b in range(2)]
    for copy in own[0] + own[1]:
        copy.start()
    def expert_at(q, d):
        off = [None] * 3
        for dim, o in zip(order[d], split(q)):
            off[dim] = o
        to_grp, to_ing = at(off, q % 2)
        return to_grp * 2 + to_ing

    up = [f < s for f, s, t in order]
    every = range(1, side)
    ends = [(k, c) for k in range(side) for c in range(2) if k + c]

    def sem(phase, b, d, k):
        return sems[phase].at[0, b, d, k], sems[phase].at[1, b, d, k]

    low, high = pl.ds(0, tokens // 2), pl.ds(tokens // 2, tokens // 2)
    ring = side > 2

    def gather_tables(b, d):
        return [remote(vt[d].at[b, pl.ds(i * plane, plane)], vr[d].at[b, i], *sem(0, b, d, i), along(order[d][0], i))
                for i in every]

    def gather_near(b, d):
        f = order[d][0]
        return [remote(ag[d].at[b, 0], ag[d].at[b, i], *sem(1, b, d, i), along(f, i)) for i in ((1, side - 1) if ring else (1,))]

    def gather_relay(b, d):
        f = order[d][0]
        return [remote(ag[d].at[b, 1, low], ag[d].at[b, 2, low], *sem(1, b, d, 2), along(f, 1)),
                remote(ag[d].at[b, side - 1, high], ag[d].at[b, 2, high], *sem(1, b, d, 0), along(f, -1))] if ring else []

    def mid(d, b, j):
        return (b, slice(None), slice(None), slice(None), j) if up[d] else (b, slice(None), slice(None), j)

    def second(b, d):
        return [remote(p2s[d].at[b, j], p2r[d].at[mid(d, b, j)], *sem(2, b, d, j), along(order[d][1], j)) for j in every]

    def final(d, b, k, core):
        lo, width = parts[d]
        index = [slice(None)] * 3
        index[order[d][2]] = k
        return (b, *index, core, slice(None), pl.ds(lo, width))

    def third(b, d):
        return [remote(p2r[d].at[b, k, c], xr.at[final(d, b, k, c)], *sem(3, b, d, 2 * k + c), along(order[d][2], k, c))
                for k, c in ends]

    def back_third(b, d):
        return [remote(xr.at[final(d, b, k, c)], p2s[d].at[b, :, k, c], *sem(4, b, d, 2 * k + c),
                       along(order[d][2], -k, c)) for k, c in ends]

    def back_mid(d, b, j):
        return (b, slice(None), slice(None), slice(None), j) if up[d] else (b, j)

    def back_second(b, d):
        return [remote(p2s[d].at[back_mid(d, b, j)], r2[d].at[b, j], *sem(5, b, d, j), along(order[d][1], -j))
                for j in every]

    def back_near(d, b, i):
        return (b, slice(None), i) if up[d] else (b, slice(None), slice(None), slice(None), i)

    def back_relay(b, d):
        f = order[d][0]
        return [remote(ps[d].at[b, 1, low], rel[d].at[b, 0], *sem(6, b, d, 0), along(f, -1)),
                remote(ps[d].at[b, 1, high], rel[d].at[b, 1], *sem(6, b, d, 1), along(f, 1))] if ring else []

    def back_first(b, d):
        f = order[d][0]
        out = [remote(ps[d].at[b, 0, high], pr[d].at[b, 0, high], *sem(6, b, d, 2), along(f, -1))]
        if ring:
            out.append(remote(ps[d].at[b, 2, low], pr[d].at[b, 1, low], *sem(6, b, d, 3), along(f, 1)))
        return out

    def back_last(b, d):
        f = order[d][0]
        out = [remote(ps[d].at[b, 0, low], pr[d].at[b, 0, low], *sem(6, b, d, 4), along(f, -1))]
        if ring:
            out.append(remote(ps[d].at[b, 2, high], pr[d].at[b, 1, high], *sem(6, b, d, 5), along(f, 1)))
        return out

    far = 2 * side

    def gate_first():
        return [remote(gs.at[pl.ds(i * plane, plane)], ga.at[i], gsem.at[0, 0, i], gsem.at[1, 0, i], along(0, i))
                for i in every]

    def gate_second():
        return [remote(ga.at[:, pl.ds(j * far, far)], gb.at[:, j], gsem.at[0, 1, j], gsem.at[1, 1, j], along(1, j))
                for j in every]

    def gate_third():
        return [remote(gb.at[:, :, 2 * k + c], gr.at[:, :, 2 * k + c], gsem.at[0, 2, 2 * k + c],
                       gsem.at[1, 2, 2 * k + c], along(2, k, c)) for k, c in ends]

    def start(copies):
        for copy in copies:
            copy.start()

    def arrived(copies):
        for copy in copies:
            copy.wait_recv()

    def mixed(lists):
        return [copy for turn in zip(*lists) for copy in turn]

    def left(copies):
        for copy in copies:
            copy.wait_send()

    def expand():
        return (iota((rows, plane), 0) // CAP == iota((rows, plane), 1)).astype(f32).astype(bf16)

    def chosen(table):
        v = jnp.dot(expand(), table, preferred_element_type=f32)
        return jnp.where(v == (iota(v.shape, 0) % CAP + 1).astype(f32), 1.0, 0.0)

    def select(b, d):
        width = parts[d][1]

        def pick(i, carry):
            sel = chosen(vr[d][b, i]).astype(bf16)
            out = jnp.dot(sel, ag[d][b, i], preferred_element_type=f32)
            out = out.reshape(side, side, 2, CAP, width).astype(bf16)
            if up[d]:
                p2r[d][b, :, :, i, 0] = out[0]
            else:
                p2r[d][b, :, :, 0, i] = out[0]
            for j in every:
                p2s[d][b, j, :, :, i] = out[j]
            return carry

        lax.fori_loop(0, side, pick, 0)

    def ffn(b):
        def chunk(ox, carry):
            rec = xr[b, ox].astype(f32).reshape(rows, hidden).astype(bf16)
            act_a = jnp.dot(rec, w1[...], preferred_element_type=f32)
            act_b = jnp.dot(rec, w3[...], preferred_element_type=f32)
            inner = (act_a * jax.nn.sigmoid(act_a) * act_b).astype(bf16)
            g = gr[ox].reshape(plane, 1, LANES)
            g = jnp.broadcast_to(g, (plane, CAP, LANES)).reshape(rows, LANES)
            mine = iota(g.shape, 1) == b * CAP + iota(g.shape, 0) % CAP
            g = jnp.sum(jnp.where(mine, g, 0.0), axis=1, keepdims=True)
            out = jnp.dot(inner, w2[...], preferred_element_type=f32) * g
            xr[b, ox] = out.reshape(side, side, 2, CAP, hidden).astype(bf16)
            return carry

        lax.fori_loop(0, side, chunk, 0)

    def tables(b):
        for d in range(3):
            def one(i, carry, d=d):
                sel = chosen(vr[d][b, i])
                sel_t = sel.T.astype(bf16)
                same = jnp.dot(sel.astype(bf16), sel_t, preferred_element_type=f32)
                r, c = iota(same.shape, 0), iota(same.shape, 1)
                same = jnp.where(r // (2 * CAP) == c // (2 * CAP), same, 0.0)
                earlier = jnp.sum(jnp.where(c < r, same, 0.0), axis=1, keepdims=True)
                fold = jnp.where(earlier > 0.0, 0.0, same).astype(bf16)
                for k in range(rows // tokens):
                    ag[d][0, i, :, k * rows:(k + 1) * rows] = fold[k * tokens:(k + 1) * tokens]
                ag[d][1, i, :, 0:rows] = sel_t
                return carry

            lax.fori_loop(0, side, one, 0)

    def partial(b, d, i):
        width = parts[d][1]
        z = r2[d][back_near(d, b, i)].astype(f32).reshape(rows, width).astype(bf16)
        fold = jnp.concatenate([ag[d][0, i, :, k * rows:(k + 1) * rows] for k in range(rows // tokens)], axis=0)
        part = jnp.dot(fold, z, preferred_element_type=f32).astype(bf16)
        return jnp.dot(ag[d][1, i, :, 0:rows], part, preferred_element_type=f32)

    narrow_first = (1, 2, 0)

    def both(body):
        def step(b, carry):
            body(b)
            return carry

        lax.fori_loop(0, 2, step, 0)

    def gather_rest(b):
        for d in narrow_first:
            arrived(gather_near(b, d))
            start(gather_relay(b, d))

    def pick_rows(b):
        for d in narrow_first:
            arrived(gather_tables(b, d) + gather_relay(b, d))
            select(b, d)
            start(second(b, d))

        @pl.when(b == 0)
        def _():
            arrived(gate_first())
            start(gate_second())
            gb[:, 0] = ga[:, 0:far]

    def last_hop(b):
        for d in narrow_first:
            arrived(second(b, d))
            left(second(b, d))
            start(third(b, d))
            xr[final(d, b, 0, 0)] = p2r[d][b, 0, 0]

        @pl.when(b == 0)
        def _():
            arrived(gate_second())
            start(gate_third())
            gr[:, :, 0] = gb[:, :, 0]

    def experts(b):
        for d in narrow_first:
            arrived(third(b, d))
        pl.when(b == 0)(lambda: arrived(gate_third()))
        ffn(b)
        start(mixed([back_third(b, d) for d in narrow_first]))
        for d in narrow_first:
            p2s[d][b, :, 0, 0] = xr[final(d, b, 0, 0)]

    def return_second(b):
        for d in narrow_first:
            arrived(back_third(b, d))
            start(back_second(b, d))
            r2[d][b, 0] = p2s[d][back_mid(d, b, 0)]

    def return_first(b):
        for d, (lo, width) in [(d, parts[d]) for d in narrow_first]:
            arrived(back_second(b, d))

            def one(i, carry, d=d):
                ps[d][b, i - 1] = partial(b, d, i)
                return carry

            lax.fori_loop(1, side, one, 0)
            start(back_relay(b, d) + back_first(b, d))
            total[b, :, lo:lo + width] = partial(b, d, 0)
        pl.when(b == 0)(lambda: tables(1))

    def pass_on(b):
        half = tokens // 2
        for d in narrow_first:
            arrived(back_relay(b, d))
            if ring:
                ps[d][b, 0, 0:half] += rel[d][b, 0]
                ps[d][b, 2, half:tokens] += rel[d][b, 1]
            start(back_last(b, d))

    def result(b):
        return pltpu.make_async_copy(rounded.at[b], y.at[b], ysem.at[b])

    def finish(b):
        for d, (lo, width) in [(d, parts[d]) for d in narrow_first]:
            arrived(back_first(b, d) + back_last(b, d))
            out = total[b, :, lo:lo + width] + pr[d][b, 0]
            out = out + pr[d][b, 1] if ring else out
            rounded[b, :, lo:lo + width] = out.astype(bf16)
        result(b).start()

    def drain(b):
        for d in range(3):
            left(gather_tables(b, d) + third(b, d) + back_third(b, d) + back_second(b, d))
            left(back_relay(b, d) + back_first(b, d) + back_last(b, d))

    pl.semaphore_wait(barrier, peers)
    for copy in own[0]:
        copy.wait()
    start(mixed([gather_near(0, d) for d in narrow_first]))
    weights = [pltpu.make_async_copy(src, dst, wsem.at[k])
               for k, (src, dst) in enumerate(((w1_hbm.at[0], w1), (w3_hbm.at[0], w3), (w2_hbm.at[0], w2)))]
    for copy in weights:
        copy.start()


    later = (iota((tokens, tokens), 0) < iota((tokens, tokens), 1)).astype(f32).astype(bf16)
    expert = expert_at(iota((n, 1), 0), 0)
    gate_rows = jnp.zeros((n, LANES), f32)
    lane = iota((n, LANES), 1)
    perms = [(expert_at(iota((n, 1), 0), d) == expert_at(iota((1, n), 1), 0)).astype(f32).astype(bf16) for d in (1, 2)]
    for b, (ids, gates) in enumerate(((ids1, gt1), (ids2, gt2))):
        member = jnp.zeros((n, tokens), f32)
        gate = jnp.zeros((n, tokens), f32)
        for j in range(ids.shape[0]):
            hit = ids[j:j + 1, :] == expert
            member = jnp.where(hit, 1.0, member)
            gate = jnp.where(hit, gates[j:j + 1, :], gate)
        before = jnp.dot(member.astype(bf16), later, preferred_element_type=f32)
        table = jnp.where(member > 0.0, before + 1.0, 0.0)
        short = table.astype(bf16)
        for d in range(3):
            vt[d][b] = jnp.dot(perms[d - 1], short, preferred_element_type=f32).astype(bf16) if d else short
            vr[d][b, 0] = vt[d][b, 0:plane, :]
        for k in range(CAP):
            col = jnp.sum(jnp.where(table == k + 1.0, gate, 0.0), axis=1, keepdims=True)
            gate_rows = jnp.where(lane == b * CAP + k, col, gate_rows)
    gs[...] = gate_rows[:, None, :]
    start(mixed([gather_tables(0, d) for d in narrow_first]))
    start(gate_first())
    ga[0] = gs[0:plane]
    for copy in own[1]:
        copy.wait()
    start(mixed([gather_near(1, d) + gather_tables(1, d) for d in narrow_first]))
    both(gather_rest)
    both(pick_rows)
    both(last_hop)
    for copy in weights:
        copy.wait()
    both(experts)
    both(lambda b: [left(gather_near(b, d) + gather_relay(b, d)) for d in range(3)])
    tables(0)
    both(return_second)
    both(return_first)
    both(pass_on)
    both(finish)
    left(gate_first() + gate_second() + gate_third())
    both(drain)
    for b in range(2):
        result(b).wait()


def copy_kernel(y, y1, y2, buf, sem):
    pieces = buf.shape[0] // 2
    size = buf.shape[1]
    moves = []
    for k in range(pieces):
        for b, dst in enumerate((y1, y2)):
            slot = 2 * k + b
            part = pl.ds(k * size, size)
            moves.append((pltpu.make_async_copy(y.at[b, part], buf.at[slot], sem.at[0, slot]),
                          pltpu.make_async_copy(buf.at[slot], dst.at[part], sem.at[1, slot])))
    for come, _ in moves:
        come.start()
    for come, go in moves:
        come.wait()
        go.start()
    for _, go in moves:
        go.wait()


def hand_on(y, pieces=4):
    hbm = pl.BlockSpec(memory_space=pl.ANY)
    _, tokens, hidden = y.shape
    shape = jax.ShapeDtypeStruct((tokens, hidden), jnp.bfloat16)
    if tokens // pieces % 16:
        pieces = 1
    return pl.pallas_call(
        copy_kernel, out_shape=(shape, shape), in_specs=[hbm], out_specs=(hbm, hbm),
        scratch_shapes=[pltpu.VMEM((2 * pieces, tokens // pieces, hidden), y.dtype),
                        pltpu.SemaphoreType.DMA((2, 2 * pieces))])(y)


def solution(mesh):
    n_grp = mesh.shape['grp']
    side = round(n_grp ** (1 / 3))
    n = side ** 3 * 2
    plane = n // side
    tok_spec = P(('dp', 'grp', 'ing'), None)
    w_spec = P(('grp', 'ing'), None, None)

    def body(x1, ids1, g1, x2, ids2, g2, w1, w3, w2):
        tokens, hidden = x1.shape
        ff = w1.shape[2]
        vmem = pl.BlockSpec(memory_space=pltpu.VMEM)
        hbm = pl.BlockSpec(memory_space=pl.ANY)
        out = jax.ShapeDtypeStruct((2, tokens, hidden), jnp.bfloat16)
        widths = [w for _, w in lane_parts(hidden)]

        def per_part(*shape):
            return [pltpu.VMEM((*shape, w), jnp.bfloat16) for w in widths]

        def wide(*shape):
            return [pltpu.VMEM((*shape, w), jnp.float32) for w in widths]

        def per_dim(*shape):
            return [pltpu.VMEM(shape, jnp.bfloat16) for _ in widths]

        rows = plane * CAP

        def gate(*shape):
            return pltpu.VMEM((*shape, 1, LANES), jnp.float32)

        y = pl.pallas_call(
            functools.partial(moe_kernel, side),
            out_shape=out,
            in_specs=[hbm] * 2 + [vmem] * 4 + [hbm] * 3,
            out_specs=hbm,
            scratch_shapes=[per_part(2, side, tokens),
                            per_part(2, side, side, 2, side, CAP),
                            per_part(2, side, 2, side, side, CAP),
                            [pltpu.VMEM((2, side, *((side, side, 2) if d < 2 else (side, 2, side)), CAP, w), jnp.bfloat16)
                             for d, w in enumerate(widths)],
                            wide(2, side - 1, tokens), wide(2, 2, tokens), wide(2, 2, tokens // 2),
                            per_dim(2, n, tokens),
                            per_dim(2, side, plane, tokens),
                            pltpu.VMEM((2, side, side, side, 2, CAP, hidden), jnp.bfloat16),
                            gate(n), gate(side, plane), gate(side, side, 2 * side), gate(side, side, 2 * side),
                            pltpu.VMEM((hidden, ff), jnp.bfloat16),
                            pltpu.VMEM((hidden, ff), jnp.bfloat16),
                            pltpu.VMEM((ff, hidden), jnp.bfloat16),
                            pltpu.VMEM((2, tokens, hidden), jnp.float32),
                            pltpu.VMEM((2, tokens, hidden), jnp.bfloat16),
                            pltpu.SemaphoreType.DMA((2, 3)), pltpu.SemaphoreType.DMA((2,)),
                            pltpu.SemaphoreType.DMA((3,)), pltpu.SemaphoreType.DMA((2, 3, 2 * side)),
                            [pltpu.SemaphoreType.DMA((2, 2, 3, k * side)) for k in (1, 1, 1, 2, 2, 1, 3)]],
            compiler_params=pltpu.CompilerParams(collective_id=0, has_side_effects=True,
                                                 vmem_limit_bytes=67_000_000),
        )(x1, x2, ids1.T, ids2.T, g1.T, g2.T, w1, w3, w2)
        return hand_on(y)

    return jax.shard_map(body, mesh=mesh, in_specs=(tok_spec,) * 6 + (w_spec,) * 3,
                         out_specs=(tok_spec, tok_spec), check_vma=False)
```

```python
import functools

import jax
import jax.numpy as jnp
from jax import lax
from jax.experimental import pallas as pl
from jax.experimental.pallas import tpu as pltpu
from jax.sharding import PartitionSpec as P

MESH = pl.DeviceIdType.MESH
CAP = 8
LANES = 128


def lane_parts(hidden):
    tiles = hidden // LANES
    sizes = [(tiles // 3 + (1 if d < tiles % 3 else 0)) * LANES for d in range(3)]
    return [(sum(sizes[:d]), sizes[d]) for d in range(3)]


def moe_kernel(side, x1, x2, ids1, ids2, gt1, gt2, w1_hbm, w3_hbm, w2_hbm, y,
               ag, p2s, p2r, r2, ps, pr, rel, vt, vr, xr, gs, ga, gb, gr, w1, w3, w2, total, rounded,
               xsem, ysem, wsem, gsem, sems):
    xs = (x1, x2)
    tokens, hidden = x1.shape
    n = side ** 3 * 2
    plane = n // side
    rows = plane * CAP
    parts = lane_parts(hidden)
    grp = lax.axis_index('grp')
    ing = lax.axis_index('ing')
    me = (grp % side, (grp // side) % side, grp // (side * side))
    order = [(d, (d + 1) % 3, (d + 2) % 3) for d in range(3)]
    f32, bf16 = jnp.float32, jnp.bfloat16

    def at(off, core=0):
        x, y, z = ((m + o) % side for m, o in zip(me, off))
        return (z * side + y) * side + x, (ing + core) % 2

    def along(dim, step, core=0):
        off = [0, 0, 0]
        off[dim] = step % side
        return at(off, core)

    def remote(src, dst, send, recv, dev):
        return pltpu.make_async_remote_copy(src_ref=src, dst_ref=dst, send_sem=send, recv_sem=recv,
                                            device_id={'grp': dev[0], 'ing': dev[1]}, device_id_type=MESH)

    def iota(shape, dim):
        return lax.broadcasted_iota(jnp.int32, shape, dim)

    def split(q):
        return q // (side * side * 2), (q // (side * 2)) % side, (q // 2) % side, q % 2

    barrier = pltpu.get_barrier_semaphore()
    for dim in range(3):
        def knock(q, carry, dim=dim):
            dev = along(dim, q // 2, q % 2)
            pl.semaphore_signal(barrier, inc=1, device_id={'grp': dev[0], 'ing': dev[1]}, device_id_type=MESH)
            return carry

        lax.fori_loop(2 if dim else 1, 2 * side, knock, 0)
    peers = 6 * side - 5
    own = [[pltpu.make_async_copy(xs[b].at[:, pl.ds(lo, width)], ag[d].at[b, 0], xsem.at[b, d])
            for d, (lo, width) in enumerate(parts)] for b in range(2)]
    for copy in own[0] + own[1]:
        copy.start()
    def expert_at(q, d):
        off = [None] * 3
        for dim, o in zip(order[d], split(q)):
            off[dim] = o
        to_grp, to_ing = at(off, q % 2)
        return to_grp * 2 + to_ing

    up = [f < s for f, s, t in order]
    every = sorted(range(1, side), key=lambda k: k == side // 2 and side > 2)
    ends = [(0, 1)] + [(k, c) for k in every for c in range(2)]

    def sem(phase, b, d, k):
        return sems[phase].at[0, b, d, k], sems[phase].at[1, b, d, k]

    low, high = pl.ds(0, tokens // 2), pl.ds(tokens // 2, tokens // 2)
    ring = side > 2

    def gather_tables(b, d):
        return [remote(vt[d].at[b, pl.ds(i * plane, plane)], vr[d].at[b, i], *sem(0, b, d, i), along(order[d][0], i))
                for i in every]

    def gather_near(b, d):
        f = order[d][0]
        return [remote(ag[d].at[b, 0], ag[d].at[b, i], *sem(1, b, d, i), along(f, i)) for i in ((1, side - 1) if ring else (1,))]

    def gather_relay(b, d):
        f = order[d][0]
        return [remote(ag[d].at[b, 1, low], ag[d].at[b, 2, low], *sem(1, b, d, 2), along(f, 1)),
                remote(ag[d].at[b, side - 1, high], ag[d].at[b, 2, high], *sem(1, b, d, 0), along(f, -1))] if ring else []

    def mid(d, b, j):
        return (b, slice(None), slice(None), slice(None), j) if up[d] else (b, slice(None), slice(None), j)

    def second(b, d):
        return [remote(p2s[d].at[b, j], p2r[d].at[mid(d, b, j)], *sem(2, b, d, j), along(order[d][1], j)) for j in every]

    def final(d, b, k, core):
        lo, width = parts[d]
        index = [slice(None)] * 3
        index[order[d][2]] = k
        return (b, *index, core, slice(None), pl.ds(lo, width))

    def third(b, d):
        return [remote(p2r[d].at[b, k, c], xr.at[final(d, b, k, c)], *sem(3, b, d, 2 * k + c), along(order[d][2], k, c))
                for k, c in ends]

    def back_one(b, d, k, c):
        return remote(xr.at[final(d, b, k, c)], p2s[d].at[b, :, k, c], *sem(4, b, d, 2 * k + c),
                      along(order[d][2], -k, c))

    def back_third(b, d):
        return [back_one(b, d, k, c) for k, c in ends]

    def back_mid(d, b, j):
        return (b, slice(None), slice(None), slice(None), j) if up[d] else (b, j)

    def back_second(b, d):
        return [remote(p2s[d].at[back_mid(d, b, j)], r2[d].at[b, j], *sem(5, b, d, j), along(order[d][1], -j))
                for j in every]

    def back_near(d, b, i):
        return (b, slice(None), i) if up[d] else (b, slice(None), slice(None), slice(None), i)

    def back_relay(b, d):
        f = order[d][0]
        return [remote(ps[d].at[b, 1, low], rel[d].at[b, 0], *sem(6, b, d, 0), along(f, -1)),
                remote(ps[d].at[b, 1, high], rel[d].at[b, 1], *sem(6, b, d, 1), along(f, 1))] if ring else []

    def back_first(b, d):
        f = order[d][0]
        out = [remote(ps[d].at[b, 0, high], pr[d].at[b, 0, high], *sem(6, b, d, 2), along(f, -1))]
        if ring:
            out.append(remote(ps[d].at[b, 2, low], pr[d].at[b, 1, low], *sem(6, b, d, 3), along(f, 1)))
        return out

    def back_last(b, d):
        f = order[d][0]
        out = [remote(ps[d].at[b, 0, low], pr[d].at[b, 0, low], *sem(6, b, d, 4), along(f, -1))]
        if ring:
            out.append(remote(ps[d].at[b, 2, high], pr[d].at[b, 1, high], *sem(6, b, d, 5), along(f, 1)))
        return out

    far = 2 * side

    def gate_first():
        return [remote(gs.at[pl.ds(i * plane, plane)], ga.at[i], gsem.at[0, 0, i], gsem.at[1, 0, i], along(0, i))
                for i in every]

    def gate_second():
        return [remote(ga.at[:, pl.ds(j * far, far)], gb.at[:, j], gsem.at[0, 1, j], gsem.at[1, 1, j], along(1, j))
                for j in every]

    def gate_third():
        return [remote(gb.at[:, :, 2 * k + c], gr.at[:, :, 2 * k + c], gsem.at[0, 2, 2 * k + c],
                       gsem.at[1, 2, 2 * k + c], along(2, k, c)) for k, c in ends]

    def start(copies):
        for copy in copies:
            copy.start()

    def arrived(copies):
        for copy in copies:
            copy.wait_recv()

    def mixed(lists):
        return [copy for turn in zip(*lists) for copy in turn]

    def left(copies):
        for copy in copies:
            copy.wait_send()

    def expand():
        return (iota((rows, plane), 0) // CAP == iota((rows, plane), 1)).astype(f32).astype(bf16)

    def chosen(table):
        v = jnp.dot(expand(), table, preferred_element_type=f32)
        return jnp.where(v == (iota(v.shape, 0) % CAP + 1).astype(f32), 1.0, 0.0)

    def select(b, d):
        width = parts[d][1]

        def pick(i, carry):
            sel = chosen(vr[d][b, i]).astype(bf16)
            out = jnp.dot(sel, ag[d][b, i], preferred_element_type=f32)
            out = out.reshape(side, side, 2, CAP, width).astype(bf16)
            if up[d]:
                p2r[d][b, :, :, i, 0] = out[0]
            else:
                p2r[d][b, :, :, 0, i] = out[0]
            for j in every:
                p2s[d][b, j, :, :, i] = out[j]
            return carry

        lax.fori_loop(0, side, pick, 0)

    def ffn(b):
        def chunk(ox, carry):
            rec = xr[b, ox].astype(f32).reshape(rows, hidden).astype(bf16)
            act_a = jnp.dot(rec, w1[...], preferred_element_type=f32)
            act_b = jnp.dot(rec, w3[...], preferred_element_type=f32)
            inner = (act_a * jax.nn.sigmoid(act_a) * act_b).astype(bf16)
            g = gr[ox].reshape(plane, 1, LANES)
            g = jnp.broadcast_to(g, (plane, CAP, LANES)).reshape(rows, LANES)
            mine = iota(g.shape, 1) == b * CAP + iota(g.shape, 0) % CAP
            g = jnp.sum(jnp.where(mine, g, 0.0), axis=1, keepdims=True)
            out = jnp.dot(inner, w2[...], preferred_element_type=f32) * g
            xr[b, ox] = out.reshape(side, side, 2, CAP, hidden).astype(bf16)
            for c in range(2):
                pl.when(ox + c > 0)(back_one(b, 1, ox, c).start)
            return carry

        lax.fori_loop(0, side, chunk, 0)

    def tables(b):
        for d in range(3):
            def one(i, carry, d=d):
                sel = chosen(vr[d][b, i])
                sel_t = sel.T.astype(bf16)
                same = jnp.dot(sel.astype(bf16), sel_t, preferred_element_type=f32)
                r, c = iota(same.shape, 0), iota(same.shape, 1)
                same = jnp.where(r // (2 * CAP) == c // (2 * CAP), same, 0.0)
                earlier = jnp.sum(jnp.where(c < r, same, 0.0), axis=1, keepdims=True)
                fold = jnp.where(earlier > 0.0, 0.0, same).astype(bf16)
                for k in range(rows // tokens):
                    ag[d][0, i, :, k * rows:(k + 1) * rows] = fold[k * tokens:(k + 1) * tokens]
                ag[d][1, i, :, 0:rows] = sel_t
                return carry

            lax.fori_loop(0, side, one, 0)

    def partial(b, d, i):
        width = parts[d][1]
        z = r2[d][back_near(d, b, i)].astype(f32).reshape(rows, width).astype(bf16)
        fold = jnp.concatenate([ag[d][0, i, :, k * rows:(k + 1) * rows] for k in range(rows // tokens)], axis=0)
        part = jnp.dot(fold, z, preferred_element_type=f32).astype(bf16)
        return jnp.dot(ag[d][1, i, :, 0:rows], part, preferred_element_type=f32)

    narrow_first = (1, 2, 0)

    def both(body):
        def step(b, carry):
            body(b)
            return carry

        lax.fori_loop(0, 2, step, 0)

    def gather_rest(b):
        for d in narrow_first:
            arrived(gather_near(b, d))
            start(gather_relay(b, d))

    def pick_rows(b):
        for d in narrow_first:
            arrived(gather_tables(b, d) + gather_relay(b, d))
            select(b, d)
            start(second(b, d))

        @pl.when(b == 0)
        def _():
            arrived(gate_first())
            start(gate_second())
            gb[:, 0] = ga[:, 0:far]

    def last_hop(b):
        for d in narrow_first:
            arrived(second(b, d))
            left(second(b, d))
        start(mixed([third(b, d) for d in narrow_first]))
        for d in narrow_first:
            xr[final(d, b, 0, 0)] = p2r[d][b, 0, 0]

        @pl.when(b == 0)
        def _():
            arrived(gate_second())
            start(gate_third())
            gr[:, :, 0] = gb[:, :, 0]

    def experts(b):
        for d in narrow_first:
            arrived(third(b, d))
        pl.when(b == 0)(lambda: arrived(gate_third()))
        ffn(b)
        start(mixed([back_third(b, d) for d in (2, 0)]))
        for d in narrow_first:
            p2s[d][b, :, 0, 0] = xr[final(d, b, 0, 0)]

    def return_second(b):
        for d in narrow_first:
            arrived(back_third(b, d))
        start(mixed([back_second(b, d) for d in narrow_first]))
        for d in narrow_first:
            r2[d][b, 0] = p2s[d][back_mid(d, b, 0)]

    def return_first(b):
        for d, (lo, width) in [(d, parts[d]) for d in narrow_first]:
            arrived(back_second(b, d))

            def one(i, carry, d=d):
                ps[d][b, i - 1] = partial(b, d, i)
                return carry

            lax.fori_loop(1, side, one, 0)
            start(back_relay(b, d) + back_first(b, d))
            total[b, :, lo:lo + width] = partial(b, d, 0)
        pl.when(b == 0)(lambda: tables(1))

    def pass_on(b):
        half = tokens // 2
        for d in narrow_first:
            arrived(back_relay(b, d))
            if ring:
                ps[d][b, 0, 0:half] += rel[d][b, 0]
                ps[d][b, 2, half:tokens] += rel[d][b, 1]
            start(back_last(b, d))

    def result(b):
        return pltpu.make_async_copy(rounded.at[b], y.at[b], ysem.at[b])

    def finish(b):
        for d, (lo, width) in [(d, parts[d]) for d in narrow_first]:
            arrived(back_first(b, d) + back_last(b, d))
            out = total[b, :, lo:lo + width] + pr[d][b, 0]
            out = out + pr[d][b, 1] if ring else out
            rounded[b, :, lo:lo + width] = out.astype(bf16)
        result(b).start()

    def drain(b):
        for d in range(3):
            left(gather_tables(b, d) + third(b, d) + back_third(b, d) + back_second(b, d))
            left(back_relay(b, d) + back_first(b, d) + back_last(b, d))

    pl.semaphore_wait(barrier, peers)
    for copy in own[0]:
        copy.wait()
    start(mixed([gather_near(0, d) for d in narrow_first]))
    weights = [pltpu.make_async_copy(src, dst, wsem.at[k])
               for k, (src, dst) in enumerate(((w1_hbm.at[0], w1), (w3_hbm.at[0], w3), (w2_hbm.at[0], w2)))]
    for copy in weights:
        copy.start()


    later = (iota((tokens, tokens), 0) < iota((tokens, tokens), 1)).astype(f32).astype(bf16)
    expert = expert_at(iota((n, 1), 0), 0)
    gate_rows = jnp.zeros((n, LANES), f32)
    lane = iota((n, LANES), 1)
    perms = [(expert_at(iota((n, 1), 0), d) == expert_at(iota((1, n), 1), 0)).astype(f32).astype(bf16) for d in (1, 2)]
    for b, (ids, gates) in enumerate(((ids1, gt1), (ids2, gt2))):
        member = jnp.zeros((n, tokens), f32)
        gate = jnp.zeros((n, tokens), f32)
        for j in range(ids.shape[0]):
            hit = ids[j:j + 1, :] == expert
            member = jnp.where(hit, 1.0, member)
            gate = jnp.where(hit, gates[j:j + 1, :], gate)
        before = jnp.dot(member.astype(bf16), later, preferred_element_type=f32)
        table = jnp.where(member > 0.0, before + 1.0, 0.0)
        short = table.astype(bf16)
        for d in range(3):
            vt[d][b] = jnp.dot(perms[d - 1], short, preferred_element_type=f32).astype(bf16) if d else short
            vr[d][b, 0] = vt[d][b, 0:plane, :]
        for k in range(CAP):
            col = jnp.sum(jnp.where(table == k + 1.0, gate, 0.0), axis=1, keepdims=True)
            gate_rows = jnp.where(lane == b * CAP + k, col, gate_rows)
    gs[...] = gate_rows[:, None, :]
    start(mixed([gather_tables(0, d) for d in narrow_first]))
    start(gate_first())
    ga[0] = gs[0:plane]
    for copy in own[1]:
        copy.wait()
    start(mixed([gather_near(1, d) + gather_tables(1, d) for d in narrow_first]))
    both(gather_rest)
    both(pick_rows)
    both(last_hop)
    for copy in weights:
        copy.wait()
    both(experts)
    both(lambda b: [left(gather_near(b, d) + gather_relay(b, d)) for d in range(3)])
    tables(0)
    both(return_second)
    both(return_first)
    both(pass_on)
    both(finish)
    left(gate_first() + gate_second() + gate_third())
    both(drain)
    for b in range(2):
        result(b).wait()


def copy_kernel(y, y1, y2, buf, sem):
    pieces = buf.shape[0] // 2
    size = buf.shape[1]
    moves = []
    for k in range(pieces):
        for b, dst in enumerate((y1, y2)):
            slot = 2 * k + b
            part = pl.ds(k * size, size)
            moves.append((pltpu.make_async_copy(y.at[b, part], buf.at[slot], sem.at[0, slot]),
                          pltpu.make_async_copy(buf.at[slot], dst.at[part], sem.at[1, slot])))
    for come, _ in moves:
        come.start()
    for come, go in moves:
        come.wait()
        go.start()
    for _, go in moves:
        go.wait()


def hand_on(y, pieces=4):
    hbm = pl.BlockSpec(memory_space=pl.ANY)
    _, tokens, hidden = y.shape
    shape = jax.ShapeDtypeStruct((tokens, hidden), jnp.bfloat16)
    if tokens // pieces % 16:
        pieces = 1
    return pl.pallas_call(
        copy_kernel, out_shape=(shape, shape), in_specs=[hbm], out_specs=(hbm, hbm),
        scratch_shapes=[pltpu.VMEM((2 * pieces, tokens // pieces, hidden), y.dtype),
                        pltpu.SemaphoreType.DMA((2, 2 * pieces))])(y)


def solution(mesh):
    n_grp = mesh.shape['grp']
    side = round(n_grp ** (1 / 3))
    n = side ** 3 * 2
    plane = n // side
    tok_spec = P(('dp', 'grp', 'ing'), None)
    w_spec = P(('grp', 'ing'), None, None)

    def body(x1, ids1, g1, x2, ids2, g2, w1, w3, w2):
        tokens, hidden = x1.shape
        ff = w1.shape[2]
        vmem = pl.BlockSpec(memory_space=pltpu.VMEM)
        hbm = pl.BlockSpec(memory_space=pl.ANY)
        out = jax.ShapeDtypeStruct((2, tokens, hidden), jnp.bfloat16)
        widths = [w for _, w in lane_parts(hidden)]

        def per_part(*shape):
            return [pltpu.VMEM((*shape, w), jnp.bfloat16) for w in widths]

        def wide(*shape):
            return [pltpu.VMEM((*shape, w), jnp.float32) for w in widths]

        def per_dim(*shape):
            return [pltpu.VMEM(shape, jnp.bfloat16) for _ in widths]

        rows = plane * CAP

        def gate(*shape):
            return pltpu.VMEM((*shape, 1, LANES), jnp.float32)

        y = pl.pallas_call(
            functools.partial(moe_kernel, side),
            out_shape=out,
            in_specs=[hbm] * 2 + [vmem] * 4 + [hbm] * 3,
            out_specs=hbm,
            scratch_shapes=[per_part(2, side, tokens),
                            per_part(2, side, side, 2, side, CAP),
                            per_part(2, side, 2, side, side, CAP),
                            [pltpu.VMEM((2, side, *((side, side, 2) if d < 2 else (side, 2, side)), CAP, w), jnp.bfloat16)
                             for d, w in enumerate(widths)],
                            wide(2, side - 1, tokens), wide(2, 2, tokens), wide(2, 2, tokens // 2),
                            per_dim(2, n, tokens),
                            per_dim(2, side, plane, tokens),
                            pltpu.VMEM((2, side, side, side, 2, CAP, hidden), jnp.bfloat16),
                            gate(n), gate(side, plane), gate(side, side, 2 * side), gate(side, side, 2 * side),
                            pltpu.VMEM((hidden, ff), jnp.bfloat16),
                            pltpu.VMEM((hidden, ff), jnp.bfloat16),
                            pltpu.VMEM((ff, hidden), jnp.bfloat16),
                            pltpu.VMEM((2, tokens, hidden), jnp.float32),
                            pltpu.VMEM((2, tokens, hidden), jnp.bfloat16),
                            pltpu.SemaphoreType.DMA((2, 3)), pltpu.SemaphoreType.DMA((2,)),
                            pltpu.SemaphoreType.DMA((3,)), pltpu.SemaphoreType.DMA((2, 3, 2 * side)),
                            [pltpu.SemaphoreType.DMA((2, 2, 3, k * side)) for k in (1, 1, 1, 2, 2, 1, 3)]],
            compiler_params=pltpu.CompilerParams(collective_id=0, has_side_effects=True,
                                                 vmem_limit_bytes=67_000_000),
        )(x1, x2, ids1.T, ids2.T, g1.T, g2.T, w1, w3, w2)
        return hand_on(y)

    return jax.shard_map(body, mesh=mesh, in_specs=(tok_spec,) * 6 + (w_spec,) * 3,
                         out_specs=(tok_spec, tok_spec), check_vma=False)
```

```python
import functools

import jax
import jax.numpy as jnp
from jax import lax
from jax.experimental import pallas as pl
from jax.experimental.pallas import tpu as pltpu
from jax.sharding import PartitionSpec as P

MESH = pl.DeviceIdType.MESH
CAP = 8
LANES = 128


def lane_parts(hidden):
    tiles = hidden // LANES
    sizes = [(tiles // 3 + (1 if d < tiles % 3 else 0)) * LANES for d in range(3)]
    return [(sum(sizes[:d]), sizes[d]) for d in range(3)]


def moe_kernel(side, x1, x2, ids1_hbm, ids2_hbm, gt1_hbm, gt2_hbm, w1_hbm, w3_hbm, w2_hbm, y,
               ag, p2s, p2r, r2, ps, pr, rel, vt, vr, xr, gs, ga, gb, gr, w1, w3, w2, total, rounded, ids1, ids2, gt1, gt2,
               rsem, xsem, ysem, wsem, gsem, sems):
    xs = (x1, x2)
    tokens, hidden = x1.shape
    n = side ** 3 * 2
    plane = n // side
    rows = plane * CAP
    parts = lane_parts(hidden)
    grp = lax.axis_index('grp')
    ing = lax.axis_index('ing')
    me = (grp % side, (grp // side) % side, grp // (side * side))
    order = [(d, (d + 1) % 3, (d + 2) % 3) for d in range(3)]
    f32, bf16 = jnp.float32, jnp.bfloat16

    def at(off, core=0):
        x, y, z = ((m + o) % side for m, o in zip(me, off))
        return (z * side + y) * side + x, (ing + core) % 2

    def along(dim, step, core=0):
        off = [0, 0, 0]
        off[dim] = step % side
        return at(off, core)

    def remote(src, dst, send, recv, dev):
        return pltpu.make_async_remote_copy(src_ref=src, dst_ref=dst, send_sem=send, recv_sem=recv,
                                            device_id={'grp': dev[0], 'ing': dev[1]}, device_id_type=MESH)

    def iota(shape, dim):
        return lax.broadcasted_iota(jnp.int32, shape, dim)

    def split(q):
        return q // (side * side * 2), (q // (side * 2)) % side, (q // 2) % side, q % 2

    barrier = pltpu.get_barrier_semaphore()
    for dim in range(3):
        def knock(q, carry, dim=dim):
            dev = along(dim, q // 2, q % 2)
            pl.semaphore_signal(barrier, inc=1, device_id={'grp': dev[0], 'ing': dev[1]}, device_id_type=MESH)
            return carry

        lax.fori_loop(2 if dim else 1, 2 * side, knock, 0)
    peers = 6 * side - 5
    routes = [pltpu.make_async_copy(src, dst, rsem.at[k]) for k, (src, dst) in enumerate(
        ((ids1_hbm, ids1), (ids2_hbm, ids2), (gt1_hbm, gt1), (gt2_hbm, gt2)))]
    own = [[pltpu.make_async_copy(xs[b].at[:, pl.ds(lo, width)], ag[d].at[b, 0], xsem.at[b, d])
            for d, (lo, width) in enumerate(parts)] for b in range(2)]
    for copy in own[0] + routes + own[1]:
        copy.start()
    def expert_at(q, d):
        off = [None] * 3
        for dim, o in zip(order[d], split(q)):
            off[dim] = o
        to_grp, to_ing = at(off, q % 2)
        return to_grp * 2 + to_ing

    up = [f < s for f, s, t in order]
    every = sorted(range(1, side), key=lambda k: k == side // 2 and side > 2)
    ends = [(0, 1)] + [(k, c) for k in every for c in range(2)]

    def sem(phase, b, d, k):
        return sems[phase].at[0, b, d, k], sems[phase].at[1, b, d, k]

    low, high = pl.ds(0, tokens // 2), pl.ds(tokens // 2, tokens // 2)
    ring = side > 2

    def gather_tables(b, d):
        return [remote(vt[d].at[b, pl.ds(i * plane, plane)], vr[d].at[b, i], *sem(0, b, d, i), along(order[d][0], i))
                for i in every]

    def gather_near(b, d):
        f = order[d][0]
        return [remote(ag[d].at[b, 0], ag[d].at[b, i], *sem(1, b, d, i), along(f, i)) for i in ((1, side - 1) if ring else (1,))]

    def gather_relay(b, d):
        f = order[d][0]
        return [remote(ag[d].at[b, 1, low], ag[d].at[b, 2, low], *sem(1, b, d, 2), along(f, 1)),
                remote(ag[d].at[b, side - 1, high], ag[d].at[b, 2, high], *sem(1, b, d, 0), along(f, -1))] if ring else []

    def mid(d, b, j):
        return (b, slice(None), slice(None), slice(None), j) if up[d] else (b, slice(None), slice(None), j)

    def second(b, d):
        return [remote(p2s[d].at[b, j], p2r[d].at[mid(d, b, j)], *sem(2, b, d, j), along(order[d][1], j)) for j in every]

    def final(d, b, k, core):
        lo, width = parts[d]
        index = [slice(None)] * 3
        index[order[d][2]] = k
        return (b, *index, core, slice(None), pl.ds(lo, width))

    def third(b, d):
        return [remote(p2r[d].at[b, k, c], xr.at[final(d, b, k, c)], *sem(3, b, d, 2 * k + c), along(order[d][2], k, c))
                for k, c in ends]

    def back_one(b, d, k, c):
        return remote(xr.at[final(d, b, k, c)], p2s[d].at[b, :, k, c], *sem(4, b, d, 2 * k + c),
                      along(order[d][2], -k, c))

    def back_third(b, d):
        return [back_one(b, d, k, c) for k, c in ends]

    def back_mid(d, b, j):
        return (b, slice(None), slice(None), slice(None), j) if up[d] else (b, j)

    def back_second(b, d):
        return [remote(p2s[d].at[back_mid(d, b, j)], r2[d].at[b, j], *sem(5, b, d, j), along(order[d][1], -j))
                for j in every]

    def back_near(d, b, i):
        return (b, slice(None), i) if up[d] else (b, slice(None), slice(None), slice(None), i)

    def back_relay(b, d):
        f = order[d][0]
        return [remote(ps[d].at[b, 1, low], rel[d].at[b, 0], *sem(6, b, d, 0), along(f, -1)),
                remote(ps[d].at[b, 1, high], rel[d].at[b, 1], *sem(6, b, d, 1), along(f, 1))] if ring else []

    def back_first(b, d):
        f = order[d][0]
        out = [remote(ps[d].at[b, 0, high], pr[d].at[b, 0, high], *sem(6, b, d, 2), along(f, -1))]
        if ring:
            out.append(remote(ps[d].at[b, 2, low], pr[d].at[b, 1, low], *sem(6, b, d, 3), along(f, 1)))
        return out

    def back_last(b, d):
        f = order[d][0]
        out = [remote(ps[d].at[b, 0, low], pr[d].at[b, 0, low], *sem(6, b, d, 4), along(f, -1))]
        if ring:
            out.append(remote(ps[d].at[b, 2, high], pr[d].at[b, 1, high], *sem(6, b, d, 5), along(f, 1)))
        return out

    far = 2 * side

    def gate_first():
        return [remote(gs.at[pl.ds(i * plane, plane)], ga.at[i], gsem.at[0, 0, i], gsem.at[1, 0, i], along(0, i))
                for i in every]

    def gate_second():
        return [remote(ga.at[:, pl.ds(j * far, far)], gb.at[:, j], gsem.at[0, 1, j], gsem.at[1, 1, j], along(1, j))
                for j in every]

    def gate_third():
        return [remote(gb.at[:, :, 2 * k + c], gr.at[:, :, 2 * k + c], gsem.at[0, 2, 2 * k + c],
                       gsem.at[1, 2, 2 * k + c], along(2, k, c)) for k, c in ends]

    def start(copies):
        for copy in copies:
            copy.start()

    def arrived(copies):
        for copy in copies:
            copy.wait_recv()

    def mixed(lists):
        return [copy for turn in zip(*lists) for copy in turn]

    def left(copies):
        for copy in copies:
            copy.wait_send()

    def expand():
        return (iota((rows, plane), 0) // CAP == iota((rows, plane), 1)).astype(f32).astype(bf16)

    def chosen(table):
        v = jnp.dot(expand(), table, preferred_element_type=f32)
        return jnp.where(v == (iota(v.shape, 0) % CAP + 1).astype(f32), 1.0, 0.0)

    def select(b, d, first, last):
        width = parts[d][1]

        def pick(m, carry):
            i = (m + side - 1) % side
            sel = chosen(vr[d][b, i]).astype(bf16)
            out = jnp.dot(sel, ag[d][b, i], preferred_element_type=f32)
            out = out.reshape(side, side, 2, CAP, width).astype(bf16)
            if up[d]:
                p2r[d][b, :, :, i, 0] = out[0]
            else:
                p2r[d][b, :, :, 0, i] = out[0]
            for j in every:
                p2s[d][b, j, :, :, i] = out[j]
            return carry

        lax.fori_loop(first, last, pick, 0)

    def ffn(b):
        def chunk(ox, carry):
            rec = xr[b, ox].astype(f32).reshape(rows, hidden).astype(bf16)
            act_a = jnp.dot(rec, w1[...], preferred_element_type=f32)
            act_b = jnp.dot(rec, w3[...], preferred_element_type=f32)
            inner = (act_a * jax.nn.sigmoid(act_a) * act_b).astype(bf16)
            g = gr[ox].reshape(plane, 1, LANES)
            g = jnp.broadcast_to(g, (plane, CAP, LANES)).reshape(rows, LANES)
            mine = iota(g.shape, 1) == b * CAP + iota(g.shape, 0) % CAP
            g = jnp.sum(jnp.where(mine, g, 0.0), axis=1, keepdims=True)
            out = jnp.dot(inner, w2[...], preferred_element_type=f32) * g
            xr[b, ox] = out.reshape(side, side, 2, CAP, hidden).astype(bf16)
            for c in range(2):
                pl.when(ox + c > 0)(back_one(b, 1, ox, c).start)
            return carry

        lax.fori_loop(0, side, chunk, 0)

    def tables(b):
        for d in range(3):
            def one(i, carry, d=d):
                sel = chosen(vr[d][b, i])
                sel_t = sel.T.astype(bf16)
                same = jnp.dot(sel.astype(bf16), sel_t, preferred_element_type=f32)
                r, c = iota(same.shape, 0), iota(same.shape, 1)
                same = jnp.where(r // (2 * CAP) == c // (2 * CAP), same, 0.0)
                earlier = jnp.sum(jnp.where(c < r, same, 0.0), axis=1, keepdims=True)
                fold = jnp.where(earlier > 0.0, 0.0, same).astype(bf16)
                for k in range(rows // tokens):
                    ag[d][0, i, :, k * rows:(k + 1) * rows] = fold[k * tokens:(k + 1) * tokens]
                ag[d][1, i, :, 0:rows] = sel_t
                return carry

            lax.fori_loop(0, side, one, 0)

    def partial(b, d, i):
        width = parts[d][1]
        z = r2[d][back_near(d, b, i)].astype(f32).reshape(rows, width).astype(bf16)
        fold = jnp.concatenate([ag[d][0, i, :, k * rows:(k + 1) * rows] for k in range(rows // tokens)], axis=0)
        part = jnp.dot(fold, z, preferred_element_type=f32).astype(bf16)
        return jnp.dot(ag[d][1, i, :, 0:rows], part, preferred_element_type=f32)

    narrow_first = (1, 2, 0)

    def both(body):
        def step(b, carry):
            body(b)
            return carry

        lax.fori_loop(0, 2, step, 0)

    def gather_rest(b):
        for d in narrow_first:
            arrived(gather_near(b, d))
            start(gather_relay(b, d))
        for d in narrow_first:
            arrived(gather_tables(b, d))
            select(b, d, 0, side - 1)

    def pick_rows(b):
        for d in narrow_first:
            arrived(gather_relay(b, d))
            select(b, d, side - 1, side)
            start(second(b, d))

        @pl.when(b == 0)
        def _():
            arrived(gate_first())
            start(gate_second())
            gb[:, 0] = ga[:, 0:far]

    def last_hop(b):
        for d in narrow_first:
            arrived(second(b, d))
            left(second(b, d))
        start(mixed([third(b, d) for d in narrow_first]))
        for d in narrow_first:
            xr[final(d, b, 0, 0)] = p2r[d][b, 0, 0]

        @pl.when(b == 0)
        def _():
            arrived(gate_second())
            start(gate_third())
            gr[:, :, 0] = gb[:, :, 0]

    def experts(b):
        for d in narrow_first:
            arrived(third(b, d))
        pl.when(b == 0)(lambda: arrived(gate_third()))
        ffn(b)
        start(mixed([back_third(b, d) for d in (2, 0)]))
        for d in narrow_first:
            p2s[d][b, :, 0, 0] = xr[final(d, b, 0, 0)]

    def return_second(b):
        for d in narrow_first:
            arrived(back_third(b, d))
        start(mixed([back_second(b, d) for d in narrow_first]))
        for d in narrow_first:
            r2[d][b, 0] = p2s[d][back_mid(d, b, 0)]

    def return_first(b):
        for d, (lo, width) in [(d, parts[d]) for d in narrow_first]:
            arrived(back_second(b, d))

            def one(i, carry, d=d):
                ps[d][b, i - 1] = partial(b, d, i)
                return carry

            lax.fori_loop(1, side, one, 0)
            start(back_relay(b, d) + back_first(b, d))
            total[b, :, lo:lo + width] = partial(b, d, 0)
        pl.when(b == 0)(lambda: tables(1))

    def pass_on(b):
        half = tokens // 2
        for d in narrow_first:
            arrived(back_relay(b, d))
            if ring:
                ps[d][b, 0, 0:half] += rel[d][b, 0]
                ps[d][b, 2, half:tokens] += rel[d][b, 1]
            start(back_last(b, d))

    def result(b):
        return pltpu.make_async_copy(rounded.at[b], y.at[b], ysem.at[b])

    def finish(b):
        for d, (lo, width) in [(d, parts[d]) for d in narrow_first]:
            arrived(back_first(b, d) + back_last(b, d))
            out = total[b, :, lo:lo + width] + pr[d][b, 0]
            out = out + pr[d][b, 1] if ring else out
            rounded[b, :, lo:lo + width] = out.astype(bf16)
        result(b).start()

    def drain(b):
        for d in range(3):
            left(gather_tables(b, d) + third(b, d) + back_third(b, d) + back_second(b, d))
            left(back_relay(b, d) + back_first(b, d) + back_last(b, d))

    pl.semaphore_wait(barrier, peers)
    for copy in own[0]:
        copy.wait()
    start(mixed([gather_near(0, d) for d in narrow_first]))
    weights = [pltpu.make_async_copy(src, dst, wsem.at[k])
               for k, (src, dst) in enumerate(((w1_hbm.at[0], w1), (w3_hbm.at[0], w3), (w2_hbm.at[0], w2)))]
    for copy in weights:
        copy.start()


    for copy in routes:
        copy.wait()

    later = (iota((tokens, tokens), 0) < iota((tokens, tokens), 1)).astype(f32).astype(bf16)
    expert = expert_at(iota((n, 1), 0), 0)
    gate_rows = jnp.zeros((n, LANES), f32)
    lane = iota((n, LANES), 1)
    perms = [(expert_at(iota((n, 1), 0), d) == expert_at(iota((1, n), 1), 0)).astype(f32).astype(bf16) for d in (1, 2)]
    for b, (ids, gates) in enumerate(((ids1, gt1), (ids2, gt2))):
        member = jnp.zeros((n, tokens), f32)
        gate = jnp.zeros((n, tokens), f32)
        for j in range(ids.shape[0]):
            hit = ids[j:j + 1, :] == expert
            member = jnp.where(hit, 1.0, member)
            gate = jnp.where(hit, gates[j:j + 1, :], gate)
        before = jnp.dot(member.astype(bf16), later, preferred_element_type=f32)
        table = jnp.where(member > 0.0, before + 1.0, 0.0)
        short = table.astype(bf16)
        for d in range(3):
            vt[d][b] = jnp.dot(perms[d - 1], short, preferred_element_type=f32).astype(bf16) if d else short
            vr[d][b, 0] = vt[d][b, 0:plane, :]
        for k in range(CAP):
            col = jnp.sum(jnp.where(table == k + 1.0, gate, 0.0), axis=1, keepdims=True)
            gate_rows = jnp.where(lane == b * CAP + k, col, gate_rows)
    gs[...] = gate_rows[:, None, :]
    start(mixed([gather_tables(0, d) for d in narrow_first]))
    start(gate_first())
    ga[0] = gs[0:plane]
    for copy in own[1]:
        copy.wait()
    start(mixed([gather_near(1, d) + gather_tables(1, d) for d in narrow_first]))
    both(gather_rest)
    both(pick_rows)
    both(last_hop)
    for copy in weights:
        copy.wait()
    both(experts)
    both(lambda b: [left(gather_near(b, d) + gather_relay(b, d)) for d in range(3)])
    tables(0)
    both(return_second)
    both(return_first)
    both(pass_on)
    both(finish)
    left(gate_first() + gate_second() + gate_third())
    both(drain)
    for b in range(2):
        result(b).wait()


def copy_kernel(y, y1, y2, buf, sem):
    pieces = buf.shape[0] // 2
    size = buf.shape[1]
    moves = []
    for k in range(pieces):
        for b, dst in enumerate((y1, y2)):
            slot = 2 * k + b
            part = pl.ds(k * size, size)
            moves.append((pltpu.make_async_copy(y.at[b, part], buf.at[slot], sem.at[0, slot]),
                          pltpu.make_async_copy(buf.at[slot], dst.at[part], sem.at[1, slot])))
    for come, _ in moves:
        come.start()
    for come, go in moves:
        come.wait()
        go.start()
    for _, go in moves:
        go.wait()


def hand_on(y, pieces=2):
    hbm = pl.BlockSpec(memory_space=pl.ANY)
    _, tokens, hidden = y.shape
    shape = jax.ShapeDtypeStruct((tokens, hidden), jnp.bfloat16)
    if tokens // pieces % 16:
        pieces = 1
    return pl.pallas_call(
        copy_kernel, out_shape=(shape, shape), in_specs=[hbm], out_specs=(hbm, hbm),
        scratch_shapes=[pltpu.VMEM((2 * pieces, tokens // pieces, hidden), y.dtype),
                        pltpu.SemaphoreType.DMA((2, 2 * pieces))])(y)


def solution(mesh):
    n_grp = mesh.shape['grp']
    side = round(n_grp ** (1 / 3))
    n = side ** 3 * 2
    plane = n // side
    tok_spec = P(('dp', 'grp', 'ing'), None)
    w_spec = P(('grp', 'ing'), None, None)

    def body(x1, ids1, g1, x2, ids2, g2, w1, w3, w2):
        tokens, hidden = x1.shape
        ff = w1.shape[2]
        top_k = ids1.shape[1]
        hbm = pl.BlockSpec(memory_space=pl.ANY)
        out = jax.ShapeDtypeStruct((2, tokens, hidden), jnp.bfloat16)
        widths = [w for _, w in lane_parts(hidden)]

        def per_part(*shape):
            return [pltpu.VMEM((*shape, w), jnp.bfloat16) for w in widths]

        def wide(*shape):
            return [pltpu.VMEM((*shape, w), jnp.float32) for w in widths]

        def per_dim(*shape):
            return [pltpu.VMEM(shape, jnp.bfloat16) for _ in widths]

        rows = plane * CAP

        def gate(*shape):
            return pltpu.VMEM((*shape, 1, LANES), jnp.float32)

        y = pl.pallas_call(
            functools.partial(moe_kernel, side),
            out_shape=out,
            in_specs=[hbm] * 9,
            out_specs=hbm,
            scratch_shapes=[per_part(2, side, tokens),
                            per_part(2, side, side, 2, side, CAP),
                            per_part(2, side, 2, side, side, CAP),
                            [pltpu.VMEM((2, side, *((side, side, 2) if d < 2 else (side, 2, side)), CAP, w), jnp.bfloat16)
                             for d, w in enumerate(widths)],
                            wide(2, side - 1, tokens), wide(2, 2, tokens), wide(2, 2, tokens // 2),
                            per_dim(2, n, tokens),
                            per_dim(2, side, plane, tokens),
                            pltpu.VMEM((2, side, side, side, 2, CAP, hidden), jnp.bfloat16),
                            gate(n), gate(side, plane), gate(side, side, 2 * side), gate(side, side, 2 * side),
                            pltpu.VMEM((hidden, ff), jnp.bfloat16),
                            pltpu.VMEM((hidden, ff), jnp.bfloat16),
                            pltpu.VMEM((ff, hidden), jnp.bfloat16),
                            pltpu.VMEM((2, tokens, hidden), jnp.float32),
                            pltpu.VMEM((2, tokens, hidden), jnp.bfloat16),
                            *[pltpu.VMEM((top_k, tokens), t) for t in (ids1.dtype, ids2.dtype, g1.dtype, g2.dtype)],
                            pltpu.SemaphoreType.DMA((4,)), pltpu.SemaphoreType.DMA((2, 3)), pltpu.SemaphoreType.DMA((2,)),
                            pltpu.SemaphoreType.DMA((3,)), pltpu.SemaphoreType.DMA((2, 3, 2 * side)),
                            [pltpu.SemaphoreType.DMA((2, 2, 3, k * side)) for k in (1, 1, 1, 2, 2, 1, 3)]],
            compiler_params=pltpu.CompilerParams(collective_id=0, has_side_effects=True,
                                                 vmem_limit_bytes=67_000_000),
        )(x1, x2, ids1.T, ids2.T, g1.T, g2.T, w1, w3, w2)
        return hand_on(y)

    return jax.shard_map(body, mesh=mesh, in_specs=(tok_spec,) * 6 + (w_spec,) * 3,
                         out_specs=(tok_spec, tok_spec), check_vma=False)
```

```python
import functools

import jax
import jax.numpy as jnp
from jax import lax
from jax.experimental import pallas as pl
from jax.experimental.pallas import tpu as pltpu
from jax.sharding import PartitionSpec as P

MESH = pl.DeviceIdType.MESH
CAP = 8
LANES = 128


def lane_parts(hidden):
    tiles = hidden // LANES
    sizes = [(tiles // 3 + (1 if d < tiles % 3 else 0)) * LANES for d in range(3)]
    return [(sum(sizes[:d]), sizes[d]) for d in range(3)]


def moe_kernel(side, x1, x2, ids1_hbm, ids2_hbm, gt1_hbm, gt2_hbm, w1_hbm, w3_hbm, w2_hbm, y,
               ag, p2s, p2r, r2, ps, pr, rel, vt, vr, xr, gs, ga, gb, gr, w1, w3, w2, total, rounded, ids1, ids2, gt1, gt2,
               rsem, xsem, ysem, wsem, gsem, sems):
    xs = (x1, x2)
    tokens, hidden = x1.shape
    n = side ** 3 * 2
    plane = n // side
    rows = plane * CAP
    parts = lane_parts(hidden)
    grp = lax.axis_index('grp')
    ing = lax.axis_index('ing')
    me = (grp % side, (grp // side) % side, grp // (side * side))
    order = [(d, (d + 1) % 3, (d + 2) % 3) for d in range(3)]
    f32, bf16 = jnp.float32, jnp.bfloat16

    def at(off, core=0):
        x, y, z = ((m + o) % side for m, o in zip(me, off))
        return (z * side + y) * side + x, (ing + core) % 2

    def along(dim, step, core=0):
        off = [0, 0, 0]
        off[dim] = step % side
        return at(off, core)

    def remote(src, dst, send, recv, dev):
        return pltpu.make_async_remote_copy(src_ref=src, dst_ref=dst, send_sem=send, recv_sem=recv,
                                            device_id={'grp': dev[0], 'ing': dev[1]}, device_id_type=MESH)

    def iota(shape, dim):
        return lax.broadcasted_iota(jnp.int32, shape, dim)

    def split(q):
        return q // (side * side * 2), (q // (side * 2)) % side, (q // 2) % side, q % 2

    barrier = pltpu.get_barrier_semaphore()
    for dim in range(3):
        def knock(q, carry, dim=dim):
            dev = along(dim, q // 2, q % 2)
            pl.semaphore_signal(barrier, inc=1, device_id={'grp': dev[0], 'ing': dev[1]}, device_id_type=MESH)
            return carry

        lax.fori_loop(2 if dim else 1, 2 * side, knock, 0)
    peers = 6 * side - 5
    routes = [pltpu.make_async_copy(src, dst, rsem.at[k]) for k, (src, dst) in enumerate(
        ((ids1_hbm, ids1), (ids2_hbm, ids2), (gt1_hbm, gt1), (gt2_hbm, gt2)))]
    own = [[pltpu.make_async_copy(xs[b].at[:, pl.ds(lo, width)], ag[d].at[b, 0], xsem.at[b, d])
            for d, (lo, width) in enumerate(parts)] for b in range(2)]
    for copy in own[0] + routes + own[1]:
        copy.start()
    def expert_at(q, d):
        off = [None] * 3
        for dim, o in zip(order[d], split(q)):
            off[dim] = o
        to_grp, to_ing = at(off, q % 2)
        return to_grp * 2 + to_ing

    up = [f < s for f, s, t in order]
    every = sorted(range(1, side), key=lambda k: k == side // 2 and side > 2)
    ends = [(0, 1)] + [(k, c) for k in every for c in range(2)]

    def sem(phase, b, d, k):
        return sems[phase].at[0, b, d, k], sems[phase].at[1, b, d, k]

    low, high = pl.ds(0, tokens // 2), pl.ds(tokens // 2, tokens // 2)
    ring = side > 2

    def gather_tables(b, d):
        return [remote(vt[d].at[b, pl.ds(i * plane, plane)], vr[d].at[b, i], *sem(0, b, d, i), along(order[d][0], i))
                for i in every]

    def gather_near(b, d):
        f = order[d][0]
        return [remote(ag[d].at[b, 0], ag[d].at[b, i], *sem(1, b, d, i), along(f, i)) for i in ((1, side - 1) if ring else (1,))]

    def gather_relay(b, d):
        f = order[d][0]
        return [remote(ag[d].at[b, 1, low], ag[d].at[b, 2, low], *sem(1, b, d, 2), along(f, 1)),
                remote(ag[d].at[b, side - 1, high], ag[d].at[b, 2, high], *sem(1, b, d, 0), along(f, -1))] if ring else []

    def mid(d, b, j):
        return (b, slice(None), slice(None), slice(None), j) if up[d] else (b, slice(None), slice(None), j)

    def second(b, d):
        return [remote(p2s[d].at[b, j], p2r[d].at[mid(d, b, j)], *sem(2, b, d, j), along(order[d][1], j)) for j in every]

    def final(d, b, k, core):
        lo, width = parts[d]
        index = [slice(None)] * 3
        index[order[d][2]] = k
        return (b, *index, core, slice(None), pl.ds(lo, width))

    def third(b, d):
        return [remote(p2r[d].at[b, k, c], xr.at[final(d, b, k, c)], *sem(3, b, d, 2 * k + c), along(order[d][2], k, c))
                for k, c in ends]

    piece = side // 2

    def back_one(b, d, k, c, h):
        if d == 1:
            src, dst = final(d, b, k, c), (b, slice(None), k, c)
        else:
            part = pl.ds(h * piece, piece)
            src = list(final(d, b, k, c))
            src[1] = part
            src, dst = tuple(src), (b, part, k, c)
        return remote(xr.at[src], p2s[d].at[dst], *sem(4, b, d, (2 * k + c) * 2 + h), along(order[d][2], -k, c))

    def back_third(b, d):
        return [back_one(b, d, k, c, h) for h in range(1 if d == 1 else 2) for k, c in ends]

    def back_mid(d, b, j):
        return (b, slice(None), slice(None), slice(None), j) if up[d] else (b, j)

    def back_second(b, d):
        return [remote(p2s[d].at[back_mid(d, b, j)], r2[d].at[b, j], *sem(5, b, d, j), along(order[d][1], -j))
                for j in every]

    def back_near(d, b, i):
        return (b, slice(None), i) if up[d] else (b, slice(None), slice(None), slice(None), i)

    def back_relay(b, d):
        f = order[d][0]
        return [remote(ps[d].at[b, 1, low], rel[d].at[b, 0], *sem(6, b, d, 0), along(f, -1)),
                remote(ps[d].at[b, 1, high], rel[d].at[b, 1], *sem(6, b, d, 1), along(f, 1))] if ring else []

    def back_first(b, d):
        f = order[d][0]
        out = [remote(ps[d].at[b, 0, high], pr[d].at[b, 0, high], *sem(6, b, d, 2), along(f, -1))]
        if ring:
            out.append(remote(ps[d].at[b, 2, low], pr[d].at[b, 1, low], *sem(6, b, d, 3), along(f, 1)))
        return out

    def back_last(b, d):
        f = order[d][0]
        out = [remote(ps[d].at[b, 0, low], pr[d].at[b, 0, low], *sem(6, b, d, 4), along(f, -1))]
        if ring:
            out.append(remote(ps[d].at[b, 2, high], pr[d].at[b, 1, high], *sem(6, b, d, 5), along(f, 1)))
        return out

    far = 2 * side

    def gate_first():
        return [remote(gs.at[pl.ds(i * plane, plane)], ga.at[i], gsem.at[0, 0, i], gsem.at[1, 0, i], along(0, i))
                for i in every]

    def gate_second():
        return [remote(ga.at[:, pl.ds(j * far, far)], gb.at[:, j], gsem.at[0, 1, j], gsem.at[1, 1, j], along(1, j))
                for j in every]

    def gate_third():
        return [remote(gb.at[:, :, 2 * k + c], gr.at[:, :, 2 * k + c], gsem.at[0, 2, 2 * k + c],
                       gsem.at[1, 2, 2 * k + c], along(2, k, c)) for k, c in ends]

    def start(copies):
        for copy in copies:
            copy.start()

    def arrived(copies):
        for copy in copies:
            copy.wait_recv()

    def mixed(lists):
        return [copy for turn in zip(*lists) for copy in turn]

    def left(copies):
        for copy in copies:
            copy.wait_send()

    def expand():
        return (iota((rows, plane), 0) // CAP == iota((rows, plane), 1)).astype(f32).astype(bf16)

    def chosen(table):
        v = jnp.dot(expand(), table, preferred_element_type=f32)
        return jnp.where(v == (iota(v.shape, 0) % CAP + 1).astype(f32), 1.0, 0.0)

    def select(b, d, first, last):
        width = parts[d][1]

        def pick(m, carry):
            i = (m + side - 1) % side
            sel = chosen(vr[d][b, i]).astype(bf16)
            out = jnp.dot(sel, ag[d][b, i], preferred_element_type=f32)
            out = out.reshape(side, side, 2, CAP, width).astype(bf16)
            if up[d]:
                p2r[d][b, :, :, i, 0] = out[0]
            else:
                p2r[d][b, :, :, 0, i] = out[0]
            for j in every:
                p2s[d][b, j, :, :, i] = out[j]
            return carry

        lax.fori_loop(first, last, pick, 0)

    def ffn(b):
        def chunk(ox, carry):
            rec = xr[b, ox].astype(f32).reshape(rows, hidden).astype(bf16)
            act_a = jnp.dot(rec, w1[...], preferred_element_type=f32)
            act_b = jnp.dot(rec, w3[...], preferred_element_type=f32)
            inner = (act_a * jax.nn.sigmoid(act_a) * act_b).astype(bf16)
            g = gr[ox].reshape(plane, 1, LANES)
            g = jnp.broadcast_to(g, (plane, CAP, LANES)).reshape(rows, LANES)
            mine = iota(g.shape, 1) == b * CAP + iota(g.shape, 0) % CAP
            g = jnp.sum(jnp.where(mine, g, 0.0), axis=1, keepdims=True)
            out = jnp.dot(inner, w2[...], preferred_element_type=f32) * g
            xr[b, ox] = out.reshape(side, side, 2, CAP, hidden).astype(bf16)
            for c in range(2):
                pl.when(ox + c > 0)(back_one(b, 1, ox, c, 0).start)

            @pl.when(ox % piece == piece - 1)
            def _():
                start(mixed([[back_one(b, d, k, c, ox // piece) for k, c in ends] for d in (2, 0)]))

            return carry

        lax.fori_loop(0, side, chunk, 0)

    def tables(b):
        for d in range(3):
            def one(i, carry, d=d):
                sel = chosen(vr[d][b, i])
                sel_t = sel.T.astype(bf16)
                same = jnp.dot(sel.astype(bf16), sel_t, preferred_element_type=f32)
                r, c = iota(same.shape, 0), iota(same.shape, 1)
                same = jnp.where(r // (2 * CAP) == c // (2 * CAP), same, 0.0)
                earlier = jnp.sum(jnp.where(c < r, same, 0.0), axis=1, keepdims=True)
                fold = jnp.where(earlier > 0.0, 0.0, same).astype(bf16)
                for k in range(rows // tokens):
                    ag[d][0, i, :, k * rows:(k + 1) * rows] = fold[k * tokens:(k + 1) * tokens]
                ag[d][1, i, :, 0:rows] = sel_t
                return carry

            lax.fori_loop(0, side, one, 0)

    def partial(b, d, i):
        width = parts[d][1]
        z = r2[d][back_near(d, b, i)].astype(f32).reshape(rows, width).astype(bf16)
        fold = jnp.concatenate([ag[d][0, i, :, k * rows:(k + 1) * rows] for k in range(rows // tokens)], axis=0)
        part = jnp.dot(fold, z, preferred_element_type=f32).astype(bf16)
        return jnp.dot(ag[d][1, i, :, 0:rows], part, preferred_element_type=f32)

    narrow_first = (1, 2, 0)

    def both(body):
        def step(b, carry):
            body(b)
            return carry

        lax.fori_loop(0, 2, step, 0)

    def gather_rest(b):
        for d in narrow_first:
            arrived(gather_near(b, d))
            start(gather_relay(b, d))
        for d in narrow_first:
            arrived(gather_tables(b, d))
            select(b, d, 0, side - 1)

    def pick_rows(b):
        for d in narrow_first:
            arrived(gather_relay(b, d))
            select(b, d, side - 1, side)
            start(second(b, d))

        @pl.when(b == 0)
        def _():
            arrived(gate_first())
            start(gate_second())
            gb[:, 0] = ga[:, 0:far]

    def last_hop(b):
        for d in narrow_first:
            arrived(second(b, d))
            left(second(b, d))
        start(mixed([third(b, d) for d in narrow_first]))
        for d in narrow_first:
            xr[final(d, b, 0, 0)] = p2r[d][b, 0, 0]

        @pl.when(b == 0)
        def _():
            arrived(gate_second())
            start(gate_third())
            gr[:, :, 0] = gb[:, :, 0]

    def experts(b):
        for d in narrow_first:
            arrived(third(b, d))
        pl.when(b == 0)(lambda: arrived(gate_third()))
        ffn(b)
        for d in narrow_first:
            p2s[d][b, :, 0, 0] = xr[final(d, b, 0, 0)]

    def return_second(b):
        for d in narrow_first:
            arrived(back_third(b, d))
        start(mixed([back_second(b, d) for d in narrow_first]))
        for d in narrow_first:
            r2[d][b, 0] = p2s[d][back_mid(d, b, 0)]

    def return_first(b):
        for d, (lo, width) in [(d, parts[d]) for d in narrow_first]:
            arrived(back_second(b, d))

            def one(i, carry, d=d):
                ps[d][b, i - 1] = partial(b, d, i)
                return carry

            lax.fori_loop(1, side, one, 0)
            start(back_relay(b, d) + back_first(b, d))
            total[b, :, lo:lo + width] = partial(b, d, 0)
        pl.when(b == 0)(lambda: tables(1))

    def pass_on(b):
        half = tokens // 2
        for d in narrow_first:
            arrived(back_relay(b, d))
            if ring:
                ps[d][b, 0, 0:half] += rel[d][b, 0]
                ps[d][b, 2, half:tokens] += rel[d][b, 1]
            start(back_last(b, d))

    def result(b):
        return pltpu.make_async_copy(rounded.at[b], y.at[b], ysem.at[b])

    def finish(b):
        for d, (lo, width) in [(d, parts[d]) for d in narrow_first]:
            arrived(back_first(b, d) + back_last(b, d))
            out = total[b, :, lo:lo + width] + pr[d][b, 0]
            out = out + pr[d][b, 1] if ring else out
            rounded[b, :, lo:lo + width] = out.astype(bf16)
        result(b).start()

    def drain(b):
        for d in range(3):
            left(gather_tables(b, d) + third(b, d) + back_third(b, d) + back_second(b, d))
            left(back_relay(b, d) + back_first(b, d) + back_last(b, d))

    pl.semaphore_wait(barrier, peers)
    for copy in own[0]:
        copy.wait()
    start(mixed([gather_near(0, d) for d in narrow_first]))
    weights = [pltpu.make_async_copy(src, dst, wsem.at[k])
               for k, (src, dst) in enumerate(((w1_hbm.at[0], w1), (w3_hbm.at[0], w3), (w2_hbm.at[0], w2)))]
    for copy in weights:
        copy.start()


    for copy in routes:
        copy.wait()

    later = (iota((tokens, tokens), 0) < iota((tokens, tokens), 1)).astype(f32).astype(bf16)
    expert = expert_at(iota((n, 1), 0), 0)
    gate_rows = jnp.zeros((n, LANES), f32)
    lane = iota((n, LANES), 1)
    perms = [(expert_at(iota((n, 1), 0), d) == expert_at(iota((1, n), 1), 0)).astype(f32).astype(bf16) for d in (1, 2)]
    for b, (ids, gates) in enumerate(((ids1, gt1), (ids2, gt2))):
        member = jnp.zeros((n, tokens), f32)
        gate = jnp.zeros((n, tokens), f32)
        for j in range(ids.shape[0]):
            hit = ids[j:j + 1, :] == expert
            member = jnp.where(hit, 1.0, member)
            gate = jnp.where(hit, gates[j:j + 1, :], gate)
        before = jnp.dot(member.astype(bf16), later, preferred_element_type=f32)
        table = jnp.where(member > 0.0, before + 1.0, 0.0)
        short = table.astype(bf16)
        for d in range(3):
            vt[d][b] = jnp.dot(perms[d - 1], short, preferred_element_type=f32).astype(bf16) if d else short
            vr[d][b, 0] = vt[d][b, 0:plane, :]
        for k in range(CAP):
            col = jnp.sum(jnp.where(table == k + 1.0, gate, 0.0), axis=1, keepdims=True)
            gate_rows = jnp.where(lane == b * CAP + k, col, gate_rows)
    gs[...] = gate_rows[:, None, :]
    start(mixed([gather_tables(0, d) for d in narrow_first]))
    start(gate_first())
    ga[0] = gs[0:plane]
    for copy in own[1]:
        copy.wait()
    start(mixed([gather_near(1, d) + gather_tables(1, d) for d in narrow_first]))
    both(gather_rest)
    both(pick_rows)
    both(last_hop)
    for copy in weights:
        copy.wait()
    both(experts)
    both(lambda b: [left(gather_near(b, d) + gather_relay(b, d)) for d in range(3)])
    tables(0)
    both(return_second)
    both(return_first)
    both(pass_on)
    both(finish)
    left(gate_first() + gate_second() + gate_third())
    both(drain)
    for b in range(2):
        result(b).wait()


def copy_kernel(y, y1, y2, buf, sem):
    pieces = buf.shape[0] // 2
    size = buf.shape[1]
    moves = []
    for k in range(pieces):
        for b, dst in enumerate((y1, y2)):
            slot = 2 * k + b
            part = pl.ds(k * size, size)
            moves.append((pltpu.make_async_copy(y.at[b, part], buf.at[slot], sem.at[0, slot]),
                          pltpu.make_async_copy(buf.at[slot], dst.at[part], sem.at[1, slot])))
    for come, _ in moves:
        come.start()
    for come, go in moves:
        come.wait()
        go.start()
    for _, go in moves:
        go.wait()


def hand_on(y, pieces=2):
    hbm = pl.BlockSpec(memory_space=pl.ANY)
    _, tokens, hidden = y.shape
    shape = jax.ShapeDtypeStruct((tokens, hidden), jnp.bfloat16)
    if tokens // pieces % 16:
        pieces = 1
    return pl.pallas_call(
        copy_kernel, out_shape=(shape, shape), in_specs=[hbm], out_specs=(hbm, hbm),
        scratch_shapes=[pltpu.VMEM((2 * pieces, tokens // pieces, hidden), y.dtype),
                        pltpu.SemaphoreType.DMA((2, 2 * pieces))])(y)


def solution(mesh):
    n_grp = mesh.shape['grp']
    side = round(n_grp ** (1 / 3))
    n = side ** 3 * 2
    plane = n // side
    tok_spec = P(('dp', 'grp', 'ing'), None)
    w_spec = P(('grp', 'ing'), None, None)

    def body(x1, ids1, g1, x2, ids2, g2, w1, w3, w2):
        tokens, hidden = x1.shape
        ff = w1.shape[2]
        top_k = ids1.shape[1]
        hbm = pl.BlockSpec(memory_space=pl.ANY)
        out = jax.ShapeDtypeStruct((2, tokens, hidden), jnp.bfloat16)
        widths = [w for _, w in lane_parts(hidden)]

        def per_part(*shape):
            return [pltpu.VMEM((*shape, w), jnp.bfloat16) for w in widths]

        def wide(*shape):
            return [pltpu.VMEM((*shape, w), jnp.float32) for w in widths]

        def per_dim(*shape):
            return [pltpu.VMEM(shape, jnp.bfloat16) for _ in widths]

        rows = plane * CAP

        def gate(*shape):
            return pltpu.VMEM((*shape, 1, LANES), jnp.float32)

        y = pl.pallas_call(
            functools.partial(moe_kernel, side),
            out_shape=out,
            in_specs=[hbm] * 9,
            out_specs=hbm,
            scratch_shapes=[per_part(2, side, tokens),
                            per_part(2, side, side, 2, side, CAP),
                            per_part(2, side, 2, side, side, CAP),
                            [pltpu.VMEM((2, side, *((side, side, 2) if d < 2 else (side, 2, side)), CAP, w), jnp.bfloat16)
                             for d, w in enumerate(widths)],
                            wide(2, side - 1, tokens), wide(2, 2, tokens), wide(2, 2, tokens // 2),
                            per_dim(2, n, tokens),
                            per_dim(2, side, plane, tokens),
                            pltpu.VMEM((2, side, side, side, 2, CAP, hidden), jnp.bfloat16),
                            gate(n), gate(side, plane), gate(side, side, 2 * side), gate(side, side, 2 * side),
                            pltpu.VMEM((hidden, ff), jnp.bfloat16),
                            pltpu.VMEM((hidden, ff), jnp.bfloat16),
                            pltpu.VMEM((ff, hidden), jnp.bfloat16),
                            pltpu.VMEM((2, tokens, hidden), jnp.float32),
                            pltpu.VMEM((2, tokens, hidden), jnp.bfloat16),
                            *[pltpu.VMEM((top_k, tokens), t) for t in (ids1.dtype, ids2.dtype, g1.dtype, g2.dtype)],
                            pltpu.SemaphoreType.DMA((4,)), pltpu.SemaphoreType.DMA((2, 3)), pltpu.SemaphoreType.DMA((2,)),
                            pltpu.SemaphoreType.DMA((3,)), pltpu.SemaphoreType.DMA((2, 3, 2 * side)),
                            [pltpu.SemaphoreType.DMA((2, 2, 3, k * side)) for k in (1, 1, 1, 2, 4, 1, 3)]],
            compiler_params=pltpu.CompilerParams(collective_id=0, has_side_effects=True,
                                                 vmem_limit_bytes=67_000_000),
        )(x1, x2, ids1.T, ids2.T, g1.T, g2.T, w1, w3, w2)
        return hand_on(y)

    return jax.shard_map(body, mesh=mesh, in_specs=(tok_spec,) * 6 + (w_spec,) * 3,
                         out_specs=(tok_spec, tok_spec), check_vma=False)
```

```python
import functools

import jax
import jax.numpy as jnp
from jax import lax
from jax.experimental import pallas as pl
from jax.experimental.pallas import tpu as pltpu
from jax.sharding import PartitionSpec as P

MESH = pl.DeviceIdType.MESH
CAP = 8
LANES = 128


def lane_parts(hidden):
    tiles = hidden // LANES
    sizes = [(tiles // 3 + (1 if d < tiles % 3 else 0)) * LANES for d in range(3)]
    return [(sum(sizes[:d]), sizes[d]) for d in range(3)]


def moe_kernel(side, x1, x2, ids1_hbm, ids2_hbm, gt1_hbm, gt2_hbm, w1_hbm, w3_hbm, w2_hbm, y,
               ag, p2s, p2r, r2, ps, pr, rel, vt, vr, xr, gs, ga, gb, gr, w1, w3, w2, total, rounded, ids1, ids2, gt1, gt2,
               rsem, xsem, ysem, wsem, gsem, sems):
    xs = (x1, x2)
    tokens, hidden = x1.shape
    n = side ** 3 * 2
    plane = n // side
    rows = plane * CAP
    parts = lane_parts(hidden)
    grp = lax.axis_index('grp')
    ing = lax.axis_index('ing')
    me = (grp % side, (grp // side) % side, grp // (side * side))
    order = [(d, (d + 1) % 3, (d + 2) % 3) for d in range(3)]
    f32, bf16 = jnp.float32, jnp.bfloat16

    def at(off, core=0):
        x, y, z = ((m + o) % side for m, o in zip(me, off))
        return (z * side + y) * side + x, (ing + core) % 2

    def along(dim, step, core=0):
        off = [0, 0, 0]
        off[dim] = step % side
        return at(off, core)

    def remote(src, dst, send, recv, dev):
        return pltpu.make_async_remote_copy(src_ref=src, dst_ref=dst, send_sem=send, recv_sem=recv,
                                            device_id={'grp': dev[0], 'ing': dev[1]}, device_id_type=MESH)

    def iota(shape, dim):
        return lax.broadcasted_iota(jnp.int32, shape, dim)

    def split(q):
        return q // (side * side * 2), (q // (side * 2)) % side, (q // 2) % side, q % 2

    barrier = pltpu.get_barrier_semaphore()
    for dim in range(3):
        def knock(q, carry, dim=dim):
            dev = along(dim, q // 2, q % 2)
            pl.semaphore_signal(barrier, inc=1, device_id={'grp': dev[0], 'ing': dev[1]}, device_id_type=MESH)
            return carry

        lax.fori_loop(2 if dim else 1, 2 * side, knock, 0)
    peers = 6 * side - 5
    routes = [pltpu.make_async_copy(src, dst, rsem.at[k]) for k, (src, dst) in enumerate(
        ((ids1_hbm, ids1), (ids2_hbm, ids2), (gt1_hbm, gt1), (gt2_hbm, gt2)))]
    own = [[pltpu.make_async_copy(xs[b].at[:, pl.ds(lo, width)], ag[d].at[b, 0], xsem.at[b, d])
            for d, (lo, width) in enumerate(parts)] for b in range(2)]
    for copy in own[0] + routes + own[1]:
        copy.start()
    def expert_at(q, d):
        off = [None] * 3
        for dim, o in zip(order[d], split(q)):
            off[dim] = o
        to_grp, to_ing = at(off, q % 2)
        return to_grp * 2 + to_ing

    up = [f < s for f, s, t in order]
    every = sorted(range(1, side), key=lambda k: k == side // 2 and side > 2)
    ends = [(0, 1)] + [(k, c) for k in every for c in range(2)]

    def sem(phase, b, d, k):
        return sems[phase].at[0, b, d, k], sems[phase].at[1, b, d, k]

    low, high = pl.ds(0, tokens // 2), pl.ds(tokens // 2, tokens // 2)
    ring = side > 2

    def gather_tables(b, d):
        return [remote(vt[d].at[b, pl.ds(i * plane, plane)], vr[d].at[b, i], *sem(0, b, d, i), along(order[d][0], i))
                for i in every]

    def gather_near(b, d):
        f = order[d][0]
        return [remote(ag[d].at[b, 0], ag[d].at[b, i], *sem(1, b, d, i), along(f, i)) for i in ((1, side - 1) if ring else (1,))]

    def gather_relay(b, d):
        f = order[d][0]
        return [remote(ag[d].at[b, 1, low], ag[d].at[b, 2, low], *sem(1, b, d, 2), along(f, 1)),
                remote(ag[d].at[b, side - 1, high], ag[d].at[b, 2, high], *sem(1, b, d, 0), along(f, -1))] if ring else []

    def mid(d, b, j):
        return (b, slice(None), slice(None), slice(None), j) if up[d] else (b, slice(None), slice(None), j)

    def second(b, d):
        return [remote(p2s[d].at[b, j], p2r[d].at[mid(d, b, j)], *sem(2, b, d, j), along(order[d][1], j)) for j in every]

    def final(d, b, k, core):
        lo, width = parts[d]
        index = [slice(None)] * 3
        index[order[d][2]] = k
        return (b, *index, core, slice(None), pl.ds(lo, width))

    def third(b, d):
        return [remote(p2r[d].at[b, k, c], xr.at[final(d, b, k, c)], *sem(3, b, d, 2 * k + c), along(order[d][2], k, c))
                for k, c in ends]

    def back_one(b, d, k, c):
        return remote(xr.at[final(d, b, k, c)], p2s[d].at[b, :, k, c], *sem(4, b, d, 2 * k + c),
                      along(order[d][2], -k, c))

    def back_third(b, d):
        return [back_one(b, d, k, c) for k, c in ends]

    def back_mid(d, b, j):
        return (b, slice(None), slice(None), slice(None), j) if up[d] else (b, j)

    def back_second(b, d):
        return [remote(p2s[d].at[back_mid(d, b, j)], r2[d].at[b, j], *sem(5, b, d, j), along(order[d][1], -j))
                for j in every]

    def back_near(d, b, i):
        return (b, slice(None), i) if up[d] else (b, slice(None), slice(None), slice(None), i)

    def back_relay(b, d):
        f = order[d][0]
        return [remote(ps[d].at[b, 1, low], rel[d].at[b, 0], *sem(6, b, d, 0), along(f, -1)),
                remote(ps[d].at[b, 1, high], rel[d].at[b, 1], *sem(6, b, d, 1), along(f, 1))] if ring else []

    def back_first(b, d):
        f = order[d][0]
        out = [remote(ps[d].at[b, 0, high], pr[d].at[b, 0, high], *sem(6, b, d, 2), along(f, -1))]
        if ring:
            out.append(remote(ps[d].at[b, 2, low], pr[d].at[b, 1, low], *sem(6, b, d, 3), along(f, 1)))
        return out

    def back_last(b, d):
        f = order[d][0]
        out = [remote(ps[d].at[b, 0, low], pr[d].at[b, 0, low], *sem(6, b, d, 4), along(f, -1))]
        if ring:
            out.append(remote(ps[d].at[b, 2, high], pr[d].at[b, 1, high], *sem(6, b, d, 5), along(f, 1)))
        return out

    far = 2 * side

    def gate_first():
        return [remote(gs.at[pl.ds(i * plane, plane)], ga.at[i], gsem.at[0, 0, i], gsem.at[1, 0, i], along(0, i))
                for i in every]

    def gate_second():
        return [remote(ga.at[:, pl.ds(j * far, far)], gb.at[:, j], gsem.at[0, 1, j], gsem.at[1, 1, j], along(1, j))
                for j in every]

    def gate_third():
        return [remote(gb.at[:, :, 2 * k + c], gr.at[:, :, 2 * k + c], gsem.at[0, 2, 2 * k + c],
                       gsem.at[1, 2, 2 * k + c], along(2, k, c)) for k, c in ends]

    def start(copies):
        for copy in copies:
            copy.start()

    def arrived(copies):
        for copy in copies:
            copy.wait_recv()

    def mixed(lists):
        return [copy for turn in zip(*lists) for copy in turn]

    def left(copies):
        for copy in copies:
            copy.wait_send()

    def expand():
        return (iota((rows, plane), 0) // CAP == iota((rows, plane), 1)).astype(f32).astype(bf16)

    def chosen(table):
        v = jnp.dot(expand(), table, preferred_element_type=f32)
        return jnp.where(v == (iota(v.shape, 0) % CAP + 1).astype(f32), 1.0, 0.0)

    def select(b, d, first, last):
        width = parts[d][1]

        def pick(m, carry):
            i = (m + side - 1) % side
            sel = chosen(vr[d][b, i]).astype(bf16)
            out = jnp.dot(sel, ag[d][b, i], preferred_element_type=f32)
            out = out.reshape(side, side, 2, CAP, width).astype(bf16)
            if up[d]:
                p2r[d][b, :, :, i, 0] = out[0]
            else:
                p2r[d][b, :, :, 0, i] = out[0]
            for j in every:
                p2s[d][b, j, :, :, i] = out[j]
            return carry

        lax.fori_loop(first, last, pick, 0)

    def ffn(b):
        def chunk(ox, carry):
            rec = xr[b, ox].astype(f32).reshape(rows, hidden).astype(bf16)
            act_a = jnp.dot(rec, w1[...], preferred_element_type=f32)
            act_b = jnp.dot(rec, w3[...], preferred_element_type=f32)
            inner = (act_a * jax.nn.sigmoid(act_a) * act_b).astype(bf16)
            g = gr[ox].reshape(plane, 1, LANES)
            g = jnp.broadcast_to(g, (plane, CAP, LANES)).reshape(rows, LANES)
            mine = iota(g.shape, 1) == b * CAP + iota(g.shape, 0) % CAP
            g = jnp.sum(jnp.where(mine, g, 0.0), axis=1, keepdims=True)
            out = jnp.dot(inner, w2[...], preferred_element_type=f32) * g
            xr[b, ox] = out.reshape(side, side, 2, CAP, hidden).astype(bf16)
            for c in range(2):
                pl.when(ox + c > 0)(back_one(b, 1, ox, c).start)
            return carry

        lax.fori_loop(0, side, chunk, 0)

    def tables(b):
        for d in range(3):
            def one(i, carry, d=d):
                sel = chosen(vr[d][b, i])
                sel_t = sel.T.astype(bf16)
                same = jnp.dot(sel.astype(bf16), sel_t, preferred_element_type=f32)
                r, c = iota(same.shape, 0), iota(same.shape, 1)
                same = jnp.where(r // (2 * CAP) == c // (2 * CAP), same, 0.0)
                earlier = jnp.sum(jnp.where(c < r, same, 0.0), axis=1, keepdims=True)
                fold = jnp.where(earlier > 0.0, 0.0, same).astype(bf16)
                for k in range(rows // tokens):
                    ag[d][0, i, :, k * rows:(k + 1) * rows] = fold[k * tokens:(k + 1) * tokens]
                ag[d][1, i, :, 0:rows] = sel_t
                return carry

            lax.fori_loop(0, side, one, 0)

    def partial(b, d, i):
        width = parts[d][1]
        z = r2[d][back_near(d, b, i)].astype(f32).reshape(rows, width).astype(bf16)
        fold = jnp.concatenate([ag[d][0, i, :, k * rows:(k + 1) * rows] for k in range(rows // tokens)], axis=0)
        part = jnp.dot(fold, z, preferred_element_type=f32).astype(bf16)
        return jnp.dot(ag[d][1, i, :, 0:rows], part, preferred_element_type=f32)

    narrow_first, wide_first = (1, 2, 0), (0, 1, 2)

    def both(body):
        def step(b, carry):
            body(b)
            return carry

        lax.fori_loop(0, 2, step, 0)

    def gather_rest(b):
        for d in narrow_first:
            arrived(gather_near(b, d))
            start(gather_relay(b, d))
        for d in narrow_first:
            arrived(gather_tables(b, d))
            select(b, d, 0, side - 1)

    def pick_rows(b):
        for d in narrow_first:
            arrived(gather_relay(b, d))
            select(b, d, side - 1, side)
            start(second(b, d))

        @pl.when(b == 0)
        def _():
            arrived(gate_first())
            start(gate_second())
            gb[:, 0] = ga[:, 0:far]

    def last_hop(b):
        for d in narrow_first:
            arrived(second(b, d))
            left(second(b, d))
        start(mixed([third(b, d) for d in narrow_first]))
        for d in narrow_first:
            xr[final(d, b, 0, 0)] = p2r[d][b, 0, 0]

        @pl.when(b == 0)
        def _():
            arrived(gate_second())
            start(gate_third())
            gr[:, :, 0] = gb[:, :, 0]

    def experts(b):
        for d in narrow_first:
            arrived(third(b, d))
        pl.when(b == 0)(lambda: arrived(gate_third()))
        ffn(b)
        start(mixed([back_third(b, d) for d in (2, 0)]))
        for d in narrow_first:
            p2s[d][b, :, 0, 0] = xr[final(d, b, 0, 0)]

    def return_second(b):
        for d in narrow_first:
            arrived(back_third(b, d))
        start(mixed([back_second(b, d) for d in narrow_first]))
        for d in narrow_first:
            r2[d][b, 0] = p2s[d][back_mid(d, b, 0)]

    def return_first(b):
        for d, (lo, width) in [(d, parts[d]) for d in wide_first]:
            arrived(back_second(b, d))

            def one(i, carry, d=d):
                ps[d][b, i - 1] = partial(b, d, i)
                return carry

            lax.fori_loop(1, side, one, 0)
            start(back_relay(b, d) + back_first(b, d))
            total[b, :, lo:lo + width] = partial(b, d, 0)
        pl.when(b == 0)(lambda: tables(1))

    def pass_on(b):
        half = tokens // 2
        for d in wide_first:
            arrived(back_relay(b, d))
            if ring:
                ps[d][b, 0, 0:half] += rel[d][b, 0]
                ps[d][b, 2, half:tokens] += rel[d][b, 1]
            start(back_last(b, d))

    def result(b):
        return pltpu.make_async_copy(rounded.at[b], y.at[b], ysem.at[b])

    def finish(b):
        for d, (lo, width) in [(d, parts[d]) for d in wide_first]:
            arrived(back_first(b, d) + back_last(b, d))
            out = total[b, :, lo:lo + width] + pr[d][b, 0]
            out = out + pr[d][b, 1] if ring else out
            rounded[b, :, lo:lo + width] = out.astype(bf16)
        result(b).start()

    def drain(b):
        for d in range(3):
            left(gather_tables(b, d) + third(b, d) + back_third(b, d) + back_second(b, d))
            left(back_relay(b, d) + back_first(b, d) + back_last(b, d))

    pl.semaphore_wait(barrier, peers)
    for copy in own[0]:
        copy.wait()
    start(mixed([gather_near(0, d) for d in narrow_first]))
    weights = [pltpu.make_async_copy(src, dst, wsem.at[k])
               for k, (src, dst) in enumerate(((w1_hbm.at[0], w1), (w3_hbm.at[0], w3), (w2_hbm.at[0], w2)))]
    for copy in weights:
        copy.start()


    for copy in routes:
        copy.wait()

    later = (iota((tokens, tokens), 0) < iota((tokens, tokens), 1)).astype(f32).astype(bf16)
    expert = expert_at(iota((n, 1), 0), 0)
    gate_rows = jnp.zeros((n, LANES), f32)
    lane = iota((n, LANES), 1)
    perms = [(expert_at(iota((n, 1), 0), d) == expert_at(iota((1, n), 1), 0)).astype(f32).astype(bf16) for d in (1, 2)]
    for b, (ids, gates) in enumerate(((ids1, gt1), (ids2, gt2))):
        member = jnp.zeros((n, tokens), f32)
        gate = jnp.zeros((n, tokens), f32)
        for j in range(ids.shape[0]):
            hit = ids[j:j + 1, :] == expert
            member = jnp.where(hit, 1.0, member)
            gate = jnp.where(hit, gates[j:j + 1, :], gate)
        before = jnp.dot(member.astype(bf16), later, preferred_element_type=f32)
        table = jnp.where(member > 0.0, before + 1.0, 0.0)
        short = table.astype(bf16)
        for d in range(3):
            vt[d][b] = jnp.dot(perms[d - 1], short, preferred_element_type=f32).astype(bf16) if d else short
            vr[d][b, 0] = vt[d][b, 0:plane, :]
        for k in range(CAP):
            col = jnp.sum(jnp.where(table == k + 1.0, gate, 0.0), axis=1, keepdims=True)
            gate_rows = jnp.where(lane == b * CAP + k, col, gate_rows)
    gs[...] = gate_rows[:, None, :]
    start(mixed([gather_tables(0, d) for d in narrow_first]))
    start(gate_first())
    ga[0] = gs[0:plane]
    for copy in own[1]:
        copy.wait()
    start(mixed([gather_near(1, d) + gather_tables(1, d) for d in narrow_first]))
    both(gather_rest)
    both(pick_rows)
    both(last_hop)
    for copy in weights:
        copy.wait()
    both(experts)
    both(lambda b: [left(gather_near(b, d) + gather_relay(b, d)) for d in range(3)])
    tables(0)
    both(return_second)
    both(return_first)
    both(pass_on)
    both(finish)
    left(gate_first() + gate_second() + gate_third())
    both(drain)
    for b in range(2):
        result(b).wait()


def copy_kernel(y, y1, y2, buf, sem):
    pieces = buf.shape[0] // 2
    size = buf.shape[1]
    moves = []
    for k in range(pieces):
        for b, dst in enumerate((y1, y2)):
            slot = 2 * k + b
            part = pl.ds(k * size, size)
            moves.append((pltpu.make_async_copy(y.at[b, part], buf.at[slot], sem.at[0, slot]),
                          pltpu.make_async_copy(buf.at[slot], dst.at[part], sem.at[1, slot])))
    for come, _ in moves:
        come.start()
    for come, go in moves:
        come.wait()
        go.start()
    for _, go in moves:
        go.wait()


def hand_on(y, pieces=2):
    hbm = pl.BlockSpec(memory_space=pl.ANY)
    _, tokens, hidden = y.shape
    shape = jax.ShapeDtypeStruct((tokens, hidden), jnp.bfloat16)
    if tokens // pieces % 16:
        pieces = 1
    return pl.pallas_call(
        copy_kernel, out_shape=(shape, shape), in_specs=[hbm], out_specs=(hbm, hbm),
        scratch_shapes=[pltpu.VMEM((2 * pieces, tokens // pieces, hidden), y.dtype),
                        pltpu.SemaphoreType.DMA((2, 2 * pieces))])(y)


def solution(mesh):
    n_grp = mesh.shape['grp']
    side = round(n_grp ** (1 / 3))
    n = side ** 3 * 2
    plane = n // side
    tok_spec = P(('dp', 'grp', 'ing'), None)
    w_spec = P(('grp', 'ing'), None, None)

    def body(x1, ids1, g1, x2, ids2, g2, w1, w3, w2):
        tokens, hidden = x1.shape
        ff = w1.shape[2]
        top_k = ids1.shape[1]
        hbm = pl.BlockSpec(memory_space=pl.ANY)
        out = jax.ShapeDtypeStruct((2, tokens, hidden), jnp.bfloat16)
        widths = [w for _, w in lane_parts(hidden)]

        def per_part(*shape):
            return [pltpu.VMEM((*shape, w), jnp.bfloat16) for w in widths]

        def wide(*shape):
            return [pltpu.VMEM((*shape, w), jnp.float32) for w in widths]

        def per_dim(*shape):
            return [pltpu.VMEM(shape, jnp.bfloat16) for _ in widths]

        rows = plane * CAP

        def gate(*shape):
            return pltpu.VMEM((*shape, 1, LANES), jnp.float32)

        y = pl.pallas_call(
            functools.partial(moe_kernel, side),
            out_shape=out,
            in_specs=[hbm] * 9,
            out_specs=hbm,
            scratch_shapes=[per_part(2, side, tokens),
                            per_part(2, side, side, 2, side, CAP),
                            per_part(2, side, 2, side, side, CAP),
                            [pltpu.VMEM((2, side, *((side, side, 2) if d < 2 else (side, 2, side)), CAP, w), jnp.bfloat16)
                             for d, w in enumerate(widths)],
                            wide(2, side - 1, tokens), wide(2, 2, tokens), wide(2, 2, tokens // 2),
                            per_dim(2, n, tokens),
                            per_dim(2, side, plane, tokens),
                            pltpu.VMEM((2, side, side, side, 2, CAP, hidden), jnp.bfloat16),
                            gate(n), gate(side, plane), gate(side, side, 2 * side), gate(side, side, 2 * side),
                            pltpu.VMEM((hidden, ff), jnp.bfloat16),
                            pltpu.VMEM((hidden, ff), jnp.bfloat16),
                            pltpu.VMEM((ff, hidden), jnp.bfloat16),
                            pltpu.VMEM((2, tokens, hidden), jnp.float32),
                            pltpu.VMEM((2, tokens, hidden), jnp.bfloat16),
                            *[pltpu.VMEM((top_k, tokens), t) for t in (ids1.dtype, ids2.dtype, g1.dtype, g2.dtype)],
                            pltpu.SemaphoreType.DMA((4,)), pltpu.SemaphoreType.DMA((2, 3)), pltpu.SemaphoreType.DMA((2,)),
                            pltpu.SemaphoreType.DMA((3,)), pltpu.SemaphoreType.DMA((2, 3, 2 * side)),
                            [pltpu.SemaphoreType.DMA((2, 2, 3, k * side)) for k in (1, 1, 1, 2, 2, 1, 3)]],
            compiler_params=pltpu.CompilerParams(collective_id=0, has_side_effects=True,
                                                 vmem_limit_bytes=67_000_000),
        )(x1, x2, ids1.T, ids2.T, g1.T, g2.T, w1, w3, w2)
        return hand_on(y)

    return jax.shard_map(body, mesh=mesh, in_specs=(tok_spec,) * 6 + (w_spec,) * 3,
                         out_specs=(tok_spec, tok_spec), check_vma=False)
```

```python
import functools

import jax
import jax.numpy as jnp
from jax import lax
from jax.experimental import pallas as pl
from jax.experimental.pallas import tpu as pltpu
from jax.sharding import PartitionSpec as P

MESH = pl.DeviceIdType.MESH
CAP = 8
LANES = 128


def lane_parts(hidden):
    tiles = hidden // LANES
    sizes = [(tiles // 3 + (1 if d < tiles % 3 else 0)) * LANES for d in range(3)]
    return [(sum(sizes[:d]), sizes[d]) for d in range(3)]


def moe_kernel(side, x1, x2, ids1_hbm, ids2_hbm, gt1_hbm, gt2_hbm, w1_hbm, w3_hbm, w2_hbm, y,
               ag, p2s, p2r, r2, ps, pr, rel, vt, vr, xr, gs, ga, gb, gr, w1, w3, w2, total, rounded, ids1, ids2, gt1, gt2,
               rsem, xsem, ysem, wsem, gsem, sems):
    xs = (x1, x2)
    tokens, hidden = x1.shape
    n = side ** 3 * 2
    plane = n // side
    rows = plane * CAP
    parts = lane_parts(hidden)
    grp = lax.axis_index('grp')
    ing = lax.axis_index('ing')
    me = (grp % side, (grp // side) % side, grp // (side * side))
    order = [(d, (d + 1) % 3, (d + 2) % 3) for d in range(3)]
    f32, bf16 = jnp.float32, jnp.bfloat16

    def at(off, core=0):
        x, y, z = ((m + o) % side for m, o in zip(me, off))
        return (z * side + y) * side + x, (ing + core) % 2

    def along(dim, step, core=0):
        off = [0, 0, 0]
        off[dim] = step % side
        return at(off, core)

    def remote(src, dst, send, recv, dev):
        return pltpu.make_async_remote_copy(src_ref=src, dst_ref=dst, send_sem=send, recv_sem=recv,
                                            device_id={'grp': dev[0], 'ing': dev[1]}, device_id_type=MESH)

    def iota(shape, dim):
        return lax.broadcasted_iota(jnp.int32, shape, dim)

    def split(q):
        return q // (side * side * 2), (q // (side * 2)) % side, (q // 2) % side, q % 2

    barrier = pltpu.get_barrier_semaphore()
    for dim in range(3):
        def knock(q, carry, dim=dim):
            dev = along(dim, q // 2, q % 2)
            pl.semaphore_signal(barrier, inc=1, device_id={'grp': dev[0], 'ing': dev[1]}, device_id_type=MESH)
            return carry

        lax.fori_loop(2 if dim else 1, 2 * side, knock, 0)
    peers = 6 * side - 5
    routes = [pltpu.make_async_copy(src, dst, rsem.at[k]) for k, (src, dst) in enumerate(
        ((ids1_hbm, ids1), (ids2_hbm, ids2), (gt1_hbm, gt1), (gt2_hbm, gt2)))]
    own = [[pltpu.make_async_copy(xs[b].at[:, pl.ds(lo, width)], ag[d].at[b, 0], xsem.at[b, d])
            for d, (lo, width) in enumerate(parts)] for b in range(2)]
    for copy in own[0] + routes + own[1]:
        copy.start()
    def expert_at(q, d):
        off = [None] * 3
        for dim, o in zip(order[d], split(q)):
            off[dim] = o
        to_grp, to_ing = at(off, q % 2)
        return to_grp * 2 + to_ing

    up = [f < s for f, s, t in order]
    every = sorted(range(1, side), key=lambda k: k == side // 2 and side > 2)
    ends = [(0, 1)] + [(k, c) for k in every for c in range(2)]

    def sem(phase, b, d, k):
        return sems[phase].at[0, b, d, k], sems[phase].at[1, b, d, k]

    low, high = pl.ds(0, tokens // 2), pl.ds(tokens // 2, tokens // 2)
    ring = side > 2

    def gather_tables(b, d):
        return [remote(vt[d].at[b, pl.ds(i * plane, plane)], vr[d].at[b, i], *sem(0, b, d, i), along(order[d][0], i))
                for i in every]

    def gather_near(b, d):
        f = order[d][0]
        return [remote(ag[d].at[b, 0], ag[d].at[b, i], *sem(1, b, d, i), along(f, i)) for i in ((1, side - 1) if ring else (1,))]

    def gather_relay(b, d):
        f = order[d][0]
        return [remote(ag[d].at[b, 1, low], ag[d].at[b, 2, low], *sem(1, b, d, 2), along(f, 1)),
                remote(ag[d].at[b, side - 1, high], ag[d].at[b, 2, high], *sem(1, b, d, 0), along(f, -1))] if ring else []

    def mid(d, b, j):
        return (b, slice(None), slice(None), slice(None), j) if up[d] else (b, slice(None), slice(None), j)

    def second(b, d):
        return [remote(p2s[d].at[b, j], p2r[d].at[mid(d, b, j)], *sem(2, b, d, j), along(order[d][1], j)) for j in every]

    def final(d, b, k, core):
        lo, width = parts[d]
        index = [slice(None)] * 3
        index[order[d][2]] = k
        return (b, *index, core, slice(None), pl.ds(lo, width))

    def third(b, d):
        return [remote(p2r[d].at[b, k, c], xr.at[final(d, b, k, c)], *sem(3, b, d, 2 * k + c), along(order[d][2], k, c))
                for k, c in ends]

    def back_one(b, d, k, c):
        return remote(xr.at[final(d, b, k, c)], p2s[d].at[b, :, k, c], *sem(4, b, d, 2 * k + c),
                      along(order[d][2], -k, c))

    def back_third(b, d):
        return [back_one(b, d, k, c) for k, c in ends]

    def back_mid(d, b, j):
        return (b, slice(None), slice(None), slice(None), j) if up[d] else (b, j)

    def back_second(b, d):
        return [remote(p2s[d].at[back_mid(d, b, j)], r2[d].at[b, j], *sem(5, b, d, j), along(order[d][1], -j))
                for j in every]

    def back_near(d, b, i):
        return (b, slice(None), i) if up[d] else (b, slice(None), slice(None), slice(None), i)

    def back_relay(b, d):
        f = order[d][0]
        return [remote(ps[d].at[b, 1, low], rel[d].at[b, 0], *sem(6, b, d, 0), along(f, -1)),
                remote(ps[d].at[b, 1, high], rel[d].at[b, 1], *sem(6, b, d, 1), along(f, 1))] if ring else []

    def back_first(b, d):
        f = order[d][0]
        out = [remote(ps[d].at[b, 0, high], pr[d].at[b, 0, high], *sem(6, b, d, 2), along(f, -1))]
        if ring:
            out.append(remote(ps[d].at[b, 2, low], pr[d].at[b, 1, low], *sem(6, b, d, 3), along(f, 1)))
        return out

    def back_last(b, d):
        f = order[d][0]
        out = [remote(ps[d].at[b, 0, low], pr[d].at[b, 0, low], *sem(6, b, d, 4), along(f, -1))]
        if ring:
            out.append(remote(ps[d].at[b, 2, high], pr[d].at[b, 1, high], *sem(6, b, d, 5), along(f, 1)))
        return out

    far = 2 * side

    def gate_first():
        return [remote(gs.at[pl.ds(i * plane, plane)], ga.at[i], gsem.at[0, 0, i], gsem.at[1, 0, i], along(0, i))
                for i in every]

    def gate_second():
        return [remote(ga.at[:, pl.ds(j * far, far)], gb.at[:, j], gsem.at[0, 1, j], gsem.at[1, 1, j], along(1, j))
                for j in every]

    def gate_third():
        return [remote(gb.at[:, :, 2 * k + c], gr.at[:, :, 2 * k + c], gsem.at[0, 2, 2 * k + c],
                       gsem.at[1, 2, 2 * k + c], along(2, k, c)) for k, c in ends]

    def start(copies):
        for copy in copies:
            copy.start()

    def arrived(copies):
        for copy in copies:
            copy.wait_recv()

    def mixed(lists):
        return [copy for turn in zip(*lists) for copy in turn]

    def left(copies):
        for copy in copies:
            copy.wait_send()

    def expand():
        return (iota((rows, plane), 0) // CAP == iota((rows, plane), 1)).astype(f32).astype(bf16)

    def chosen(table):
        v = jnp.dot(expand(), table, preferred_element_type=f32)
        return jnp.where(v == (iota(v.shape, 0) % CAP + 1).astype(f32), 1.0, 0.0)

    def select(b, d, first, last):
        width = parts[d][1]

        def pick(m, carry):
            i = (m + side - 1) % side
            sel = chosen(vr[d][b, i]).astype(bf16)
            out = jnp.dot(sel, ag[d][b, i], preferred_element_type=f32)
            out = out.reshape(side, side, 2, CAP, width).astype(bf16)
            if up[d]:
                p2r[d][b, :, :, i, 0] = out[0]
            else:
                p2r[d][b, :, :, 0, i] = out[0]
            for j in every:
                p2s[d][b, j, :, :, i] = out[j]
            return carry

        lax.fori_loop(first, last, pick, 0)

    def ffn(b):
        def chunk(ox, carry):
            rec = xr[b, ox].astype(f32).reshape(rows, hidden).astype(bf16)
            act_a = jnp.dot(rec, w1[...], preferred_element_type=f32)
            act_b = jnp.dot(rec, w3[...], preferred_element_type=f32)
            inner = (act_a * jax.nn.sigmoid(act_a) * act_b).astype(bf16)
            g = gr[ox].reshape(plane, 1, LANES)
            g = jnp.broadcast_to(g, (plane, CAP, LANES)).reshape(rows, LANES)
            mine = iota(g.shape, 1) == b * CAP + iota(g.shape, 0) % CAP
            g = jnp.sum(jnp.where(mine, g, 0.0), axis=1, keepdims=True)
            out = jnp.dot(inner, w2[...], preferred_element_type=f32) * g
            xr[b, ox] = out.reshape(side, side, 2, CAP, hidden).astype(bf16)
            for c in range(2):
                pl.when(ox + c > 0)(back_one(b, 1, ox, c).start)
            return carry

        lax.fori_loop(0, side, chunk, 0)

    def tables(b):
        for d in range(3):
            def one(i, carry, d=d):
                sel = chosen(vr[d][b, i])
                sel_t = sel.T.astype(bf16)
                same = jnp.dot(sel.astype(bf16), sel_t, preferred_element_type=f32)
                r, c = iota(same.shape, 0), iota(same.shape, 1)
                same = jnp.where(r // (2 * CAP) == c // (2 * CAP), same, 0.0)
                earlier = jnp.sum(jnp.where(c < r, same, 0.0), axis=1, keepdims=True)
                fold = jnp.where(earlier > 0.0, 0.0, same).astype(bf16)
                for k in range(rows // tokens):
                    ag[d][0, i, :, k * rows:(k + 1) * rows] = fold[k * tokens:(k + 1) * tokens]
                ag[d][1, i, :, 0:rows] = sel_t
                return carry

            lax.fori_loop(0, side, one, 0)

    def partial(b, d, i):
        width = parts[d][1]
        z = r2[d][back_near(d, b, i)].astype(f32).reshape(rows, width).astype(bf16)
        fold = jnp.concatenate([ag[d][0, i, :, k * rows:(k + 1) * rows] for k in range(rows // tokens)], axis=0)
        part = jnp.dot(fold, z, preferred_element_type=f32).astype(bf16)
        return jnp.dot(ag[d][1, i, :, 0:rows], part, preferred_element_type=f32)

    narrow_first, wide_first = (0, 1, 2), (0, 1, 2)

    def both(body):
        def step(b, carry):
            body(b)
            return carry

        lax.fori_loop(0, 2, step, 0)

    def gather_rest(b):
        for d in narrow_first:
            arrived(gather_near(b, d))
            start(gather_relay(b, d))
        for d in narrow_first:
            arrived(gather_tables(b, d))
            select(b, d, 0, side - 1)

    def pick_rows(b):
        for d in narrow_first:
            arrived(gather_relay(b, d))
            select(b, d, side - 1, side)
            start(second(b, d))

        @pl.when(b == 0)
        def _():
            arrived(gate_first())
            start(gate_second())
            gb[:, 0] = ga[:, 0:far]

    def last_hop(b):
        for d in narrow_first:
            arrived(second(b, d))
            left(second(b, d))
        start(mixed([third(b, d) for d in narrow_first]))
        for d in narrow_first:
            xr[final(d, b, 0, 0)] = p2r[d][b, 0, 0]

        @pl.when(b == 0)
        def _():
            arrived(gate_second())
            start(gate_third())
            gr[:, :, 0] = gb[:, :, 0]

    def experts(b):
        for d in narrow_first:
            arrived(third(b, d))
        pl.when(b == 0)(lambda: arrived(gate_third()))
        ffn(b)
        start(mixed([back_third(b, d) for d in (2, 0)]))
        for d in narrow_first:
            p2s[d][b, :, 0, 0] = xr[final(d, b, 0, 0)]

    def return_second(b):
        for d in narrow_first:
            arrived(back_third(b, d))
        start(mixed([back_second(b, d) for d in narrow_first]))
        for d in narrow_first:
            r2[d][b, 0] = p2s[d][back_mid(d, b, 0)]

    def return_first(b):
        for d, (lo, width) in [(d, parts[d]) for d in wide_first]:
            arrived(back_second(b, d))

            def one(i, carry, d=d):
                ps[d][b, i - 1] = partial(b, d, i)
                return carry

            lax.fori_loop(1, side, one, 0)
            start(back_relay(b, d) + back_first(b, d))
            total[b, :, lo:lo + width] = partial(b, d, 0)
        pl.when(b == 0)(lambda: tables(1))

    def pass_on(b):
        half = tokens // 2
        for d in wide_first:
            arrived(back_relay(b, d))
            if ring:
                ps[d][b, 0, 0:half] += rel[d][b, 0]
                ps[d][b, 2, half:tokens] += rel[d][b, 1]
            start(back_last(b, d))

    def result(b):
        return pltpu.make_async_copy(rounded.at[b], y.at[b], ysem.at[b])

    def finish(b):
        for d, (lo, width) in [(d, parts[d]) for d in wide_first]:
            arrived(back_first(b, d) + back_last(b, d))
            out = total[b, :, lo:lo + width] + pr[d][b, 0]
            out = out + pr[d][b, 1] if ring else out
            rounded[b, :, lo:lo + width] = out.astype(bf16)
        result(b).start()

    def drain(b):
        for d in range(3):
            left(gather_tables(b, d) + third(b, d) + back_third(b, d) + back_second(b, d))
            left(back_relay(b, d) + back_first(b, d) + back_last(b, d))

    pl.semaphore_wait(barrier, peers)
    for copy in own[0]:
        copy.wait()
    start(mixed([gather_near(0, d) for d in narrow_first]))
    weights = [pltpu.make_async_copy(src, dst, wsem.at[k])
               for k, (src, dst) in enumerate(((w1_hbm.at[0], w1), (w3_hbm.at[0], w3), (w2_hbm.at[0], w2)))]
    for copy in weights:
        copy.start()


    for copy in routes:
        copy.wait()

    later = (iota((tokens, tokens), 0) < iota((tokens, tokens), 1)).astype(f32).astype(bf16)
    expert = expert_at(iota((n, 1), 0), 0)
    gate_rows = jnp.zeros((n, LANES), f32)
    lane = iota((n, LANES), 1)
    perms = [(expert_at(iota((n, 1), 0), d) == expert_at(iota((1, n), 1), 0)).astype(f32).astype(bf16) for d in (1, 2)]
    for b, (ids, gates) in enumerate(((ids1, gt1), (ids2, gt2))):
        member = jnp.zeros((n, tokens), f32)
        gate = jnp.zeros((n, tokens), f32)
        for j in range(ids.shape[0]):
            hit = ids[j:j + 1, :] == expert
            member = jnp.where(hit, 1.0, member)
            gate = jnp.where(hit, gates[j:j + 1, :], gate)
        before = jnp.dot(member.astype(bf16), later, preferred_element_type=f32)
        table = jnp.where(member > 0.0, before + 1.0, 0.0)
        short = table.astype(bf16)
        for d in range(3):
            vt[d][b] = jnp.dot(perms[d - 1], short, preferred_element_type=f32).astype(bf16) if d else short
            vr[d][b, 0] = vt[d][b, 0:plane, :]
        for k in range(CAP):
            col = jnp.sum(jnp.where(table == k + 1.0, gate, 0.0), axis=1, keepdims=True)
            gate_rows = jnp.where(lane == b * CAP + k, col, gate_rows)
    gs[...] = gate_rows[:, None, :]
    start(mixed([gather_tables(0, d) for d in narrow_first]))
    start(gate_first())
    ga[0] = gs[0:plane]
    for copy in own[1]:
        copy.wait()
    start(mixed([gather_near(1, d) + gather_tables(1, d) for d in narrow_first]))
    both(gather_rest)
    both(pick_rows)
    both(last_hop)
    for copy in weights:
        copy.wait()
    both(experts)
    both(lambda b: [left(gather_near(b, d) + gather_relay(b, d)) for d in range(3)])
    tables(0)
    both(return_second)
    both(return_first)
    both(pass_on)
    both(finish)
    left(gate_first() + gate_second() + gate_third())
    both(drain)
    for b in range(2):
        result(b).wait()


def copy_kernel(y, y1, y2, buf, sem):
    pieces = buf.shape[0] // 2
    size = buf.shape[1]
    moves = []
    for k in range(pieces):
        for b, dst in enumerate((y1, y2)):
            slot = 2 * k + b
            part = pl.ds(k * size, size)
            moves.append((pltpu.make_async_copy(y.at[b, part], buf.at[slot], sem.at[0, slot]),
                          pltpu.make_async_copy(buf.at[slot], dst.at[part], sem.at[1, slot])))
    for come, _ in moves:
        come.start()
    for come, go in moves:
        come.wait()
        go.start()
    for _, go in moves:
        go.wait()


def hand_on(y, pieces=2):
    hbm = pl.BlockSpec(memory_space=pl.ANY)
    _, tokens, hidden = y.shape
    shape = jax.ShapeDtypeStruct((tokens, hidden), jnp.bfloat16)
    if tokens // pieces % 16:
        pieces = 1
    return pl.pallas_call(
        copy_kernel, out_shape=(shape, shape), in_specs=[hbm], out_specs=(hbm, hbm),
        scratch_shapes=[pltpu.VMEM((2 * pieces, tokens // pieces, hidden), y.dtype),
                        pltpu.SemaphoreType.DMA((2, 2 * pieces))])(y)


def solution(mesh):
    n_grp = mesh.shape['grp']
    side = round(n_grp ** (1 / 3))
    n = side ** 3 * 2
    plane = n // side
    tok_spec = P(('dp', 'grp', 'ing'), None)
    w_spec = P(('grp', 'ing'), None, None)

    def body(x1, ids1, g1, x2, ids2, g2, w1, w3, w2):
        tokens, hidden = x1.shape
        ff = w1.shape[2]
        top_k = ids1.shape[1]
        hbm = pl.BlockSpec(memory_space=pl.ANY)
        out = jax.ShapeDtypeStruct((2, tokens, hidden), jnp.bfloat16)
        widths = [w for _, w in lane_parts(hidden)]

        def per_part(*shape):
            return [pltpu.VMEM((*shape, w), jnp.bfloat16) for w in widths]

        def wide(*shape):
            return [pltpu.VMEM((*shape, w), jnp.float32) for w in widths]

        def per_dim(*shape):
            return [pltpu.VMEM(shape, jnp.bfloat16) for _ in widths]

        rows = plane * CAP

        def gate(*shape):
            return pltpu.VMEM((*shape, 1, LANES), jnp.float32)

        y = pl.pallas_call(
            functools.partial(moe_kernel, side),
            out_shape=out,
            in_specs=[hbm] * 9,
            out_specs=hbm,
            scratch_shapes=[per_part(2, side, tokens),
                            per_part(2, side, side, 2, side, CAP),
                            per_part(2, side, 2, side, side, CAP),
                            [pltpu.VMEM((2, side, *((side, side, 2) if d < 2 else (side, 2, side)), CAP, w), jnp.bfloat16)
                             for d, w in enumerate(widths)],
                            wide(2, side - 1, tokens), wide(2, 2, tokens), wide(2, 2, tokens // 2),
                            per_dim(2, n, tokens),
                            per_dim(2, side, plane, tokens),
                            pltpu.VMEM((2, side, side, side, 2, CAP, hidden), jnp.bfloat16),
                            gate(n), gate(side, plane), gate(side, side, 2 * side), gate(side, side, 2 * side),
                            pltpu.VMEM((hidden, ff), jnp.bfloat16),
                            pltpu.VMEM((hidden, ff), jnp.bfloat16),
                            pltpu.VMEM((ff, hidden), jnp.bfloat16),
                            pltpu.VMEM((2, tokens, hidden), jnp.float32),
                            pltpu.VMEM((2, tokens, hidden), jnp.bfloat16),
                            *[pltpu.VMEM((top_k, tokens), t) for t in (ids1.dtype, ids2.dtype, g1.dtype, g2.dtype)],
                            pltpu.SemaphoreType.DMA((4,)), pltpu.SemaphoreType.DMA((2, 3)), pltpu.SemaphoreType.DMA((2,)),
                            pltpu.SemaphoreType.DMA((3,)), pltpu.SemaphoreType.DMA((2, 3, 2 * side)),
                            [pltpu.SemaphoreType.DMA((2, 2, 3, k * side)) for k in (1, 1, 1, 2, 2, 1, 3)]],
            compiler_params=pltpu.CompilerParams(collective_id=0, has_side_effects=True,
                                                 vmem_limit_bytes=67_000_000),
        )(x1, x2, ids1.T, ids2.T, g1.T, g2.T, w1, w3, w2)
        return hand_on(y)

    return jax.shard_map(body, mesh=mesh, in_specs=(tok_spec,) * 6 + (w_spec,) * 3,
                         out_specs=(tok_spec, tok_spec), check_vma=False)
```
